256 devices in a mesh: gx: 16 (over x, y), gy: 8 (over z), gz: 2 (over core).
Axes of the slice: x: 4, y: 4, z: 8, core: 2. Of those that a mesh axis runs over, the one named last changes fastest.
Arguments:
- membrane: float32 [256, 128, 512], P('gx', 'gy', 'gz'), may hold values from 0 to 0.95
- recovery: float32 [256, 128, 512], P('gx', 'gy', 'gz'), may hold values from 0 to 2
- extracellular: float32 [256, 128, 512], P('gx', 'gy', 'gz'), may hold values from -6 to 6
- fiber_scale: float32 [256, 128, 512], P('gx', 'gy', 'gz'), may hold values from 0.5 to 2
- labels: int32 [32, 16, 64], P('gx', 'gy', 'gz'), may hold values from 0 to 2
Outputs:
- membrane_next: float32 [256, 128, 512], P('gx', 'gy', 'gz')
- recovery_next: float32 [256, 128, 512], P('gx', 'gy', 'gz')
- extracellular_next: float32 [256, 128, 512], P('gx', 'gy', 'gz')
The draws below stay inside these ranges and needn't reach their ends.
All inputs are finite; a program needn't handle non-finite values.
Results may differ from the reference program's by a relative error of at most 0.0003.
Values sent between devices are 32-bit elements; how exact they have to be, the bound alone decides.
No kernel may reach another device: no remote copies, remote signals or barrier semaphores. Data moves between devices by JAX's collectives and lax.ppermute only.
A program may use at most 128 MiB of HBM per device.

```python
import math
import jax
import jax.numpy as jnp
from jax import lax

LEVELS = 4
SMOOTH_SWEEPS = 1
COARSE_SWEEPS = 8
NX = 256
NY = 128
NZ = 512


def draw_membrane(key, part):
    shape = (NX, NY, NZ)
    along_x = lax.broadcasted_iota(jnp.int32, shape, 0)
    along_y = lax.broadcasted_iota(jnp.int32, shape, 1)
    raised = (along_x < NX // 2) != (along_y < NY // 4)
    levels = jnp.where(raised, 0.85, 0.1).astype(jnp.float32)
    spread = 0.1
    noise = jax.random.uniform(key, shape, jnp.float32, -spread, spread)
    return (levels + noise).astype(jnp.float32)


def touch_ends(values, key, least, top_value):
    extent = values.shape
    place = [jax.random.randint(jax.random.fold_in(key, axis), (), 0, extent[axis]) for axis in range(len(extent))]
    values = values.at[tuple(place)].set(least)
    longest = extent.index(max(extent))
    place[longest] = (place[longest] + 1) % extent[longest]
    return values.at[tuple(place)].set(top_value)


def level_of(key, extent, split, least, largest):
    gain = 1.0
    for axis_at, shards_of in split:
        heights = jax.random.uniform(jax.random.fold_in(jax.random.fold_in(key, 6), axis_at), (shards_of,), jnp.float32, least / len(split), largest / len(split))
        gain = gain * jnp.repeat(jnp.exp(heights), extent[axis_at] // shards_of).reshape((-1,) + (1,) * (len(extent) - 1 - axis_at))
    return gain


def gaussian(own_key, extent, scale, bound, shards=(), kind=jnp.bfloat16):
    values = scale * jax.random.normal(own_key, extent, jnp.float32)
    if shards:
        values = values * level_of(own_key, extent, shards, -0.22, 0.18)
    return jnp.clip(values, -bound, bound).astype(kind)


def setup_inputs(seed: int = 0) -> dict:
    arg_keys = jax.random.split(jax.random.key(seed), 6)
    return {
        "membrane": draw_membrane(jax.random.fold_in(arg_keys[5], 71), 0),
        "recovery": jnp.clip(2.0 * jax.random.uniform(arg_keys[1], (NX, NY, NZ), jnp.float32) ** level_of(arg_keys[1], (NX, NY, NZ), ((0, 16), (1, 8), (2, 2)), -0.2, 0.2), 0.0, 2.0),
        "extracellular": gaussian(arg_keys[2], (NX, NY, NZ), 1.0, 6.0, ((0, 16), (1, 8), (2, 2)), jnp.float32),
        "fiber_scale": jnp.clip(jnp.exp(math.log(2.0) - 1.3862944 * jax.random.uniform(arg_keys[3], (NX, NY, NZ), jnp.float32) ** level_of(arg_keys[3], (NX, NY, NZ), ((0, 16), (1, 8), (2, 2)), -0.2, 0.2)), 0.5, 2.0),
        "labels": touch_ends(jax.random.randint(arg_keys[4], (NX // 8, NY // 8, NZ // 8), 0, 3), jax.random.fold_in(arg_keys[4], 1), 0, 2).astype(jnp.int32),
    }


TIME_STEP = 0.05
ionic_gain = 8.0
ionic_onset = 0.15
recovery_rate = 0.01
DIRECTIONS = ((0, -1), (0, 1), (1, -1), (1, 1), (2, -1), (2, 1))


def lookup(labels):
    inner = jnp.where(labels == 1, 1.0, jnp.where(labels == 2, 0.3, 0.0)).astype(jnp.float32)
    outer = jnp.where(labels == 0, 3.0, 1.0).astype(jnp.float32)
    return inner, outer


def expand(blocks, factor):
    sa, sb, sc = blocks.shape
    big = jnp.broadcast_to(blocks[:, None, :, None, :, None], (sa, factor, sb, factor, sc, factor))
    return big.reshape(sa * factor, sb * factor, sc * factor)


def restrict(values):
    shape = values.shape
    lead = shape[:-3]
    folded = values.reshape(lead + (shape[-3] // 2, 2, shape[-2] // 2, 2, shape[-1] // 2, 2))
    return jnp.mean(folded, axis=(-5, -3, -1))


def neighbour(padded, axis_index, side):
    pieces = [slice(1, padded.shape[0] - 1), slice(1, padded.shape[1] - 1), slice(1, padded.shape[2] - 1)]
    pieces[axis_index] = slice(1 + side, padded.shape[axis_index] - 1 + side)
    return padded[tuple(pieces)]


def widen(field):
    return jnp.pad(field, 1)


def widen_stack(coef):
    return jnp.pad(coef, ((0, 0), (1, 1), (1, 1), (1, 1)))


def couplings(pcoef):
    centre_in = neighbour(pcoef[0], 0, 0)
    centre_out = neighbour(pcoef[1], 0, 0)
    result = []
    for axis_index, side in DIRECTIONS:
        result.append(jnp.minimum(centre_in, neighbour(pcoef[0], axis_index, side))
                      + 0.5 * (centre_out + neighbour(pcoef[1], axis_index, side)))
    return result


def offdiag(padded_field, coupling):
    total = jnp.zeros(coupling[0].shape, jnp.float32)
    for index, (axis_index, side) in enumerate(DIRECTIONS):
        total = total + coupling[index] * neighbour(padded_field, axis_index, side)
    return total


def intra(padded_field, pcoef):
    centre_in = neighbour(pcoef[0], 0, 0)
    centre_val = neighbour(padded_field, 0, 0)
    total = jnp.zeros(centre_val.shape, jnp.float32)
    for axis_index, side in DIRECTIONS:
        weight = jnp.minimum(centre_in, neighbour(pcoef[0], axis_index, side))
        total = total + weight * (neighbour(padded_field, axis_index, side) - centre_val)
    return total


def parity_of(shape):
    total = lax.broadcasted_iota(jnp.int32, shape, 0) + lax.broadcasted_iota(jnp.int32, shape, 1)
    total = total + lax.broadcasted_iota(jnp.int32, shape, 2)
    return total % 2


def sweeps(field, rhs, coupling, diagonal, parity, count):
    for sweep_index in range(count):
        for colour in (0, 1):
            updated = (rhs + offdiag(widen(field), coupling)) / diagonal
            field = jnp.where(parity == colour, updated, field)
    return field


def cycle(level_index, field, rhs, padded_coefs):
    coupling = couplings(padded_coefs[level_index])
    diagonal = sum(coupling)
    parity = parity_of(rhs.shape)
    if level_index == LEVELS - 1:
        return sweeps(jnp.zeros_like(rhs), rhs, coupling, diagonal, parity, COARSE_SWEEPS)
    field = sweeps(field, rhs, coupling, diagonal, parity, SMOOTH_SWEEPS)
    remainder = rhs - (diagonal * field - offdiag(widen(field), coupling))
    coarse_rhs = 4.0 * restrict(remainder)
    correction = cycle(level_index + 1, jnp.zeros_like(coarse_rhs), coarse_rhs, padded_coefs)
    field = field + expand(correction, 2)
    return sweeps(field, rhs, coupling, diagonal, parity, SMOOTH_SWEEPS)


def reference(membrane, recovery, extracellular, fiber_scale, labels):
    lab_in, lab_out = lookup(labels)
    tissue = (expand(labels, 8) != 0).astype(jnp.float32)
    inner = expand(lab_in, 8) * fiber_scale
    outer = expand(lab_out, 8)
    coef = jnp.stack([inner, outer])
    padded_coefs = []
    for level_index in range(LEVELS):
        padded_coefs.append(widen_stack(coef))
        if level_index + 1 < LEVELS:
            coef = restrict(coef)
    drive = intra(widen(membrane + extracellular), padded_coefs[0])
    ionic = ionic_gain * membrane * (membrane - ionic_onset) * (membrane - 1.0) + membrane * recovery
    membrane_next = membrane + TIME_STEP * (drive - tissue * ionic)
    recovery_next = recovery + TIME_STEP * recovery_rate * (-recovery - ionic_gain * membrane * (membrane - ionic_onset - 1.0))
    rhs = intra(widen(membrane_next), padded_coefs[0])
    extracellular_next = cycle(0, extracellular, rhs, padded_coefs)
    return membrane_next, recovery_next, extracellular_next
```

```python
import jax
import jax.numpy as jnp
from jax import lax
from jax.experimental import pallas as pl
from jax.experimental.pallas import tpu as pltpu
from jax.sharding import PartitionSpec as P

TIME_STEP = 0.05
IONIC_GAIN = 8.0
IONIC_ONSET = 0.15
RECOVERY_RATE = 0.01
COARSE_SWEEPS = 8

F32 = jnp.float32
BX, BY, BZ = 16, 16, 256
H = 5
X0, Y0, Z0 = BX + 2 * H, 32, 2 * BZ
X1, Y1, Z1 = BX // 2 + 2 * H, 24, BZ
Z2 = BZ // 2
PAD = 4
VMEM = pl.BlockSpec(memory_space=pltpu.VMEM)
SMEM = pl.BlockSpec(memory_space=pltpu.SMEM)
PARAMS = pltpu.CompilerParams(vmem_limit_bytes=60 * 1024 * 1024)


def iota(shape, dim):
    return lax.broadcasted_iota(jnp.int32, shape, dim)


def up(x, axis):
    return pltpu.roll(x, x.shape[axis] - 1, axis)


def down(x, axis):
    return pltpu.roll(x, 1, axis)


def pair_matrix(rows, cols, value):
    return jnp.where(iota((rows, cols), 0) // 2 == iota((rows, cols), 1), value, 0.0).astype(F32)


def copy_matrix(rows, cols):
    return jnp.where(iota((rows, cols), 1) // 2 == iota((rows, cols), 0), 1.0, 0.0).astype(F32)


def dot(a, b):
    return jnp.dot(a, b, precision=lax.Precision.HIGHEST, preferred_element_type=F32)


def sum_rows(buf, x):
    rows, cols = x.shape
    sums = []
    for c in range(cols // 128):
        buf[c, 0:rows, :] = x[:, 128 * c : 128 * c + 128]
        sums.append(buf[c, pl.ds(0, rows // 2, 2), :] + buf[c, pl.ds(1, rows // 2, 2), :])
    return sums[0] if len(sums) == 1 else jnp.concatenate(sums, axis=1)


def twice_rows(buf, x):
    rows, cols = x.shape
    for c in range(cols // 128):
        for k in (0, 1):
            buf[c, pl.ds(k, rows, 2), :] = x[:, 128 * c : 128 * c + 128]


def columns(buf, start, rows, cols):
    parts = [buf[c, pl.ds(start, rows), :] for c in range(cols // 128)]
    return parts[0] if len(parts) == 1 else jnp.concatenate(parts, axis=1)


def loop(start, stop, step, body):
    def run(index, carry):
        body(start + index * step)
        return carry

    lax.fori_loop(0, (stop - start) // step, run, 0)


def faces(inner, outer, ax, ay, az, diag, inv, mx, my, mz, step):
    n, ys, zs = inner.shape
    shape = (step, ys, zs)
    row, lane = iota(shape, 1), iota(shape, 2)

    def x_face(i):
        here, there = pl.ds(i, step), pl.ds(i + 1, step)
        low = jnp.minimum(inner[here], inner[there])
        if mx is not None:
            mx[here] = low
        ax[here] = low + 0.5 * (outer[here] + outer[there])

    def first():
        low = jnp.minimum(inner[0:1], inner[1:2])
        if mx is not None:
            mx[0:1] = low
        ax[0:1] = low + 0.5 * (outer[0:1] + outer[1:2])

    first()

    def body(i):
        x_face(i)
        here = pl.ds(i, step)
        c_in, c_out = inner[here], outer[here]
        half = 0.5 * c_out
        low = jnp.where(row < ys - 1, jnp.minimum(c_in, up(c_in, 1)), 0.0)
        full = low + half + jnp.where(row < ys - 1, up(half, 1), 0.0)
        if my is not None:
            my[here] = low
        ay[here] = jnp.where(row < ys - 1, full, 0.0)
        total = full + jnp.where(row > 0, down(full, 1), half)
        low = jnp.where(lane < zs - 1, jnp.minimum(c_in, up(c_in, 2)), 0.0)
        full = low + half + jnp.where(lane < zs - 1, up(half, 2), 0.0)
        if mz is not None:
            mz[here] = low
        az[here] = jnp.where(lane < zs - 1, full, 0.0)
        total = total + full + jnp.where(lane > 0, down(full, 2), half)
        total = total + ax[here] + ax[pl.ds(i - 1, step)]
        if diag is not None:
            diag[here] = total
        inv[here] = jnp.where(c_out > 0.0, 1.0 / jnp.where(c_out > 0.0, total, 1.0), 0.0)

    loop(1, n - 1, step, body)


def offdiag(v, ax, ay, az, i, step):
    here, after, before = pl.ds(i, step), pl.ds(i + 1, step), pl.ds(i - 1, step)
    c = v[here]
    total = ax[here] * v[after] + ax[before] * v[before]
    cy, cz = ay[here], az[here]
    total = total + cy * up(c, 1) + down(cy * c, 1)
    return c, total + cz * up(c, 2) + down(cz * c, 2)


def half_sweep(v, b, ax, ay, az, inv, colour, offset, start, stop, step):
    shape = (step,) + tuple(v.shape[1:])
    place = iota(shape, 0) + iota(shape, 1) + iota(shape, 2)

    def body(i):
        here = pl.ds(i, step)
        c, total = offdiag(v, ax, ay, az, i, step)
        mine = ((place + (i + offset)) & 1) == colour
        v[here] = jnp.where(mine, (b[here] + total) * inv[here], c)

    loop(start, stop, step, body)


def first_half(v, b, inv, offset, start, stop, step):
    shape = (step,) + tuple(v.shape[1:])
    place = iota(shape, 0) + iota(shape, 1) + iota(shape, 2)

    def body(i):
        here = pl.ds(i, step)
        mine = ((place + (i + offset)) & 1) == 0
        v[here] = jnp.where(mine, b[here] * inv[here], 0.0)

    loop(start, stop, step, body)


def prep_kernel(m, r, u, f, labels, own, xup, xdn, yup, ydn, rnext):
    spread = jnp.where(iota((BZ // 8, BZ), 1) // 8 == iota((BZ // 8, BZ), 0), 1.0, 0.0).astype(F32)
    for bx in range(BX // 8):
        wide = jnp.dot(labels[bx].astype(F32), spread, preferred_element_type=F32)
        kind = jnp.concatenate(
            [jnp.broadcast_to(wide[by : by + 1], (8, BZ)) for by in range(BY // 8)], axis=0
        )
        factor = jnp.where(kind > 1.5, 0.3, jnp.where(kind > 0.5, 1.0, 0.0)).astype(F32)
        for x in range(8 * bx, 8 * bx + 8):
            own[2, x] = factor * f[x]
            mm, rr = m[x], r[x]
            own[0, x] = mm
            own[1, x] = u[x]
            own[3, x] = rr
            rnext[x] = rr + TIME_STEP * RECOVERY_RATE * (
                -rr - IONIC_GAIN * mm * (mm - IONIC_ONSET - 1.0)
            )
    for q in range(4):
        xup[q] = own[q, BX - H : BX]
        xdn[q] = own[q, 0:H]
        yup[q] = own[q, :, BY - 8 : BY, :]
        ydn[q] = own[q, :, 0:8, :]


def fine_kernel(
    place, own, own_z, xlo, xlo_z, xhi, xhi_z, ylo, ylo_z, yhi, yhi_z, clo, clo_z, chi, chi_z,
    mnext, v, rhs, inner, packed,
    m, r, s, outer, mx, my, mz, ax, ay, az, diag, inv, fold, fold2,
):
    core = place[2]
    has_xl = (place[0] > 0).astype(F32)
    has_xh = (place[0] < place[3] - 1).astype(F32)
    has_yl = (place[1] > 0).astype(F32)
    has_yh = (place[1] < place[4] - 1).astype(F32)
    for buf in (m, v, inner, r):
        buf[0:H, 0:8, :] = jnp.zeros((H, 8, Z0), F32)
    for side in (0, 1):
        lanes = pl.ds(pl.multiple_of((core if side == 0 else 1 - core) * BZ, BZ), BZ)
        o, xl, xh, yl, yh, cl, ch = (
            (own, xlo, xhi, ylo, yhi, clo, chi)
            if side == 0
            else (own_z, xlo_z, xhi_z, ylo_z, yhi_z, clo_z, chi_z)
        )
        for q, buf in enumerate((m, v, inner, r)):
            def body(x, q=q, buf=buf):
                buf[x + H, 8:24, lanes] = o[q, x]
                buf[x + H, 0:8, lanes] = yl[q, x] * has_yl
                buf[x + H, 24:32, lanes] = yh[q, x] * has_yh

            loop(0, BX, 1, body)

            def edge(x, q=q, buf=buf):
                buf[x, 8:24, lanes] = xl[q, x] * has_xl
                buf[x + BX + H, 8:24, lanes] = xh[q, x] * has_xh
                buf[x, 0:8, lanes] = cl[q, x] * (has_xl * has_yl)
                buf[x, 24:32, lanes] = ch[q, x] * (has_xl * has_yh)
                buf[x + BX + H, 0:8, lanes] = cl[q, x + H] * (has_xh * has_yl)
                buf[x + BX + H, 24:32, lanes] = ch[q, x + H] * (has_xh * has_yh)

            loop(0, H, 1, edge)
    row = iota((1, Y0, Z0), 1)
    in_y = jnp.where(row < 8, has_yl, jnp.where(row < 24, 1.0, has_yh))

    def body(x):
        in_x = jnp.where(x < H, has_xl, jnp.where(x < BX + H, 1.0, has_xh))
        here = pl.ds(x, 1)
        outer[here] = jnp.where(inner[here] > 0.0, 1.0, 3.0 * in_x * in_y)
        s[here] = m[here] + v[here]

    loop(0, X0, 1, body)
    faces(inner, outer, ax, ay, az, diag, inv, mx, my, mz, 1)

    def intra(w, i):
        here, after, before = pl.ds(i, 1), pl.ds(i + 1, 1), pl.ds(i - 1, 1)
        c = w[here]
        total = mx[here] * (w[after] - c) + mx[before] * (w[before] - c)
        flow = my[here] * (up(c, 1) - c)
        total = total + flow - down(flow, 1)
        flow = mz[here] * (up(c, 2) - c)
        return total + flow - down(flow, 2)

    def body(x):
        here = pl.ds(x, 1)
        mm = m[here]
        ionic = IONIC_GAIN * mm * (mm - IONIC_ONSET) * (mm - 1.0) + mm * r[here]
        ionic = jnp.where(inner[here] > 0.0, ionic, 0.0)
        r[here] = mm + TIME_STEP * (intra(s, x) - ionic)

    loop(1, X0 - 1, 1, body)
    lanes = pl.ds(pl.multiple_of(core * BZ, BZ), BZ)
    mnext[...] = r[H : BX + H, 8:24, lanes]

    def body(x):
        rhs[pl.ds(x, 1)] = intra(r, x)

    loop(2, X0 - 2, 1, body)
    half_sweep(v, rhs, ax, ay, az, inv, 0, 1, 2, X0 - 2, 1)
    half_sweep(v, rhs, ax, ay, az, inv, 1, 1, 3, X0 - 3, 1)

    def body(p):
        total = None
        for i in (2 * p + H, 2 * p + H + 1):
            c, off = offdiag(v, ax, ay, az, i, 1)
            here = pl.ds(i, 1)
            res = rhs[here] - (diag[here] * c - off)
            total = res if total is None else total + res
        fold[pl.ds(p, 1)] = total[:, 8:24, :]
        fold[pl.ds(p + 8, 1)] = (
            inner[pl.ds(2 * p + H, 1), 8:24, :] + inner[pl.ds(2 * p + H + 1, 1), 8:24, :]
        )

    loop(0, BX // 2, 1, body)
    half = BX // 2 * BY
    pairs = pair_matrix(Z0, Z1, 0.5)
    both = sum_rows(fold2, dot(fold[...].reshape(2 * half, Z0), pairs))
    packed[0] = both[: half // 2].reshape(8, 8, Z1)
    packed[1] = 0.25 * both[half // 2 :].reshape(8, 8, Z1)


def middle_kernel(
    place, low, own, high, v, b, inner, send, outer, ax, ay, az, diag, inv, fold, fold2
):
    core = place[2]
    has_xl = (place[0] > 0).astype(F32)
    has_xh = (place[0] < place[3] - 1).astype(F32)
    has_yl = (place[1] > 0).astype(F32)
    has_yh = (place[1] < place[4] - 1).astype(F32)
    row = iota((1, Y1, Z1), 1)
    in_y = jnp.where(row < 8, has_yl, jnp.where(row < 16, 1.0, has_yh))
    for q, buf in enumerate((b, inner)):
        buf[0:H] = low[q] * (in_y * has_xl)
        buf[H : H + 8] = own[q] * in_y
        buf[H + 8 :] = high[q] * (in_y * has_xh)
    for x in range(X1):
        in_x = has_xl if x < H else (has_xh if x >= H + 8 else 1.0)
        here = slice(x, x + 1)
        outer[here] = jnp.where(inner[here] > 0.0, 1.0, 3.0 * in_x * in_y)
    faces(inner, outer, ax, ay, az, diag, inv, None, None, None, 2)
    v[0:1] = jnp.zeros((1, Y1, Z1), F32)
    v[X1 - 1 :] = jnp.zeros((1, Y1, Z1), F32)
    first_half(v, b, inv, 1, 1, X1 - 1, 2)
    half_sweep(v, b, ax, ay, az, inv, 1, 1, 1, X1 - 1, 2)
    for p in range(4):
        i = 2 * p + H
        c, off = offdiag(v, ax, ay, az, i, 2)
        here = slice(i, i + 2)
        res = (b[here] - (diag[here] * c - off))[:, 8:16, :]
        mean = inner[here][:, 8:16, :]
        fold[8 * p : 8 * p + 8] = res[0] + res[1]
        fold[32 + 8 * p : 40 + 8 * p] = 0.25 * (mean[0] + mean[1])
    both = sum_rows(fold2, dot(fold[...], pair_matrix(Z1, Z2, 0.5)))
    first = core == 0
    piece = jnp.concatenate(
        [
            jnp.where(first, both[0:8], both[8:16]),
            jnp.where(first, both[16:24], both[24:32]),
        ],
        axis=0,
    )

    def body(d):
        send[d] = piece

    loop(0, send.shape[0], 1, body)


def up_kernel(
    place, got, got_z, v1, b1, in1, v0, b0, in0, out,
    b2, in2, out2, ax2, ay2, az2, diag2, inv2, v2,
    b3, in3, out3, ax3, ay3, az3, inv3, v3,
    out1, ax1, ay1, az1, inv1, out0, ax0, ay0, az0, inv0, fold2, fold1, fold0,
    *, nx, ny,
):
    core = place[2]
    has_xl = (place[0] > 0).astype(F32)
    has_xh = (place[0] < nx - 1).astype(F32)
    has_yl = (place[1] > 0).astype(F32)
    has_yh = (place[1] < ny - 1).astype(F32)
    n2, y2 = 4 * nx, 4 * ny
    n3, y3 = 2 * nx, 2 * ny
    for buf in (b2, in2, out2, v2):
        buf[0:PAD] = jnp.zeros((PAD, y2, Z2), F32)
        buf[PAD + n2 :] = jnp.zeros((PAD, y2, Z2), F32)

    def body(gx):
        for side in (0, 1):
            src = got if side == 0 else got_z
            half = core if side == 0 else 1 - core
            for i in (0, 1):
                x = PAD + 4 * gx + 2 * half + i
                for gy in range(ny):
                    b2[x, 4 * gy : 4 * gy + 4, :] = src[gx * ny + gy, 4 * i : 4 * i + 4, :]
                    in2[x, 4 * gy : 4 * gy + 4, :] = src[gx * ny + gy, 8 + 4 * i : 12 + 4 * i, :]

    loop(0, nx, 1, body)

    def body(i):
        here = pl.ds(i, 4)
        out2[here] = jnp.where(in2[here] > 0.0, 1.0, 3.0)

    loop(PAD, PAD + n2, 4, body)
    core2 = slice(PAD - 1, PAD + n2 + 1)
    at = lambda ref: ref.at[pl.ds(PAD - 1, n2 + 2)]
    faces(at(in2), at(out2), at(ax2), at(ay2), at(az2), at(diag2), at(inv2), None, None, None, 4)
    first_half(v2, b2, inv2, 0, PAD, PAD + n2, 4)
    half_sweep(v2, b2, ax2, ay2, az2, inv2, 1, 0, PAD, PAD + n2, 4)

    def body(p):
        i = PAD + 4 * p
        c, off = offdiag(v2, ax2, ay2, az2, i, 4)
        here = pl.ds(i, 4)
        res = b2[here] - (diag2[here] * c - off)
        mean = in2[here]
        for k in (0, 1):
            fold2[0, pl.ds(2 * p + k, 1)] = res[2 * k : 2 * k + 1] + res[2 * k + 1 : 2 * k + 2]
            fold2[1, pl.ds(2 * p + k, 1)] = 0.25 * (
                mean[2 * k : 2 * k + 1] + mean[2 * k + 1 : 2 * k + 2]
            )

    loop(0, nx, 1, body)
    pairs = pair_matrix(Z2, Z2, 0.5)
    rows = n3 * y2
    for q in (0, 1):
        both = sum_rows(fold1, dot(fold2[q].reshape(rows, Z2), pairs))
        (b3, in3)[q][1 : n3 + 1] = both.reshape(n3, y3, Z2)
    for buf in (in3, out3, v3):
        buf[0:1] = jnp.zeros((1, y3, Z2), F32)
        buf[n3 + 1 :] = jnp.zeros((1, y3, Z2), F32)
    lane = iota((n3, y3, Z2), 2)
    out3[1 : n3 + 1] = jnp.where(
        lane < Z2 // 2, jnp.where(in3[1 : n3 + 1] > 0.0, 1.0, 3.0), 0.0
    )
    step3 = 8 if n3 % 8 == 0 else n3
    faces(in3, out3, ax3, ay3, az3, None, inv3, None, None, None, step3)
    first_half(v3, b3, inv3, 1, 1, n3 + 1, step3)
    half_sweep(v3, b3, ax3, ay3, az3, inv3, 1, 1, 1, n3 + 1, step3)

    def sweep(k):
        half_sweep(v3, b3, ax3, ay3, az3, inv3, 0, 1, 1, n3 + 1, step3)
        half_sweep(v3, b3, ax3, ay3, az3, inv3, 1, 1, 1, n3 + 1, step3)

    loop(0, COARSE_SWEEPS - 1, 1, sweep)
    wide = dot(v3[1 : n3 + 1].reshape(n3 * y3, Z2), copy_matrix(Z2, Z2))
    twice_rows(fold1, wide)

    def body(p):
        e = columns(fold1, pl.multiple_of(p * y2, y2), y2, Z2)
        for k in (0, 1):
            v2[PAD + 2 * p + k] = v2[PAD + 2 * p + k] + e

    loop(0, n3, 1, body)
    half_sweep(v2, b2, ax2, ay2, az2, inv2, 0, 0, PAD, PAD + n2, 4)
    half_sweep(v2, b2, ax2, ay2, az2, inv2, 1, 0, PAD, PAD + n2, 4)
    row = iota((1, Y1, Z1), 1)
    in_y = jnp.where(row < 8, has_yl, jnp.where(row < 16, 1.0, has_yh))
    for x in range(X1):
        in_x = has_xl if x < H else (has_xh if x >= H + 8 else 1.0)
        here = slice(x, x + 1)
        out1[here] = jnp.where(in1[here] > 0.0, 1.0, 3.0 * in_x * in_y)
    faces(in1, out1, ax1, ay1, az1, None, inv1, None, None, None, 2)
    shift = lax.rem(4 - 4 * place[1] + 2 * y2, y2)
    part = pltpu.roll(v2[pl.ds(PAD + 4 * place[0] - 2, 8)], shift, 1)[:, 0:16, :]
    wide = dot(part.reshape(128, Z2), copy_matrix(Z2, Z1))
    twice_rows(fold1, wide)
    for x in range(1, X1 - 1):
        k = (x - 1) // 2
        e = columns(fold1, 32 * k, Y1, Z1)
        v1[x] = jnp.where(out1[x] > 0.0, v1[x] + e, 0.0)
    half_sweep(v1, b1, ax1, ay1, az1, inv1, 0, 1, 1, X1 - 1, 2)
    half_sweep(v1, b1, ax1, ay1, az1, inv1, 1, 1, 1, X1 - 1, 2)
    row = iota((1, Y0, Z0), 1)
    in_y = jnp.where(row < 8, has_yl, jnp.where(row < 24, 1.0, has_yh))

    def body(x):
        in_x = jnp.where(x < H, has_xl, jnp.where(x < BX + H, 1.0, has_xh))
        here = pl.ds(x, 1)
        out0[here] = jnp.where(in0[here] > 0.0, 1.0, 3.0 * in_x * in_y)

    loop(2, X0 - 2, 1, body)
    at = lambda ref: ref.at[pl.ds(2, X0 - 4)]
    faces(at(in0), at(out0), at(ax0), at(ay0), at(az0), None, at(inv0), None, None, None, 1)
    part = v1[4:14, 4:20, :]
    wide = dot(part.reshape(160, Z1), copy_matrix(Z1, Z0))
    twice_rows(fold0, wide)

    def body(p):
        e = columns(fold0, pl.multiple_of(p * 32, 32), 32, Z0)
        for k in (0, 1):
            x = 3 + 2 * p + k
            v0[x] = jnp.where(out0[x] > 0.0, v0[x] + e, 0.0)

    loop(0, 10, 1, body)
    half_sweep(v0, b0, ax0, ay0, az0, inv0, 0, 1, H - 1, X0 - H + 1, 1)
    half_sweep(v0, b0, ax0, ay0, az0, inv0, 1, 1, H, X0 - H, 1)
    lanes = pl.ds(pl.multiple_of(core * BZ, BZ), BZ)
    out[...] = v0[H : BX + H, 8:24, lanes]


def shape(*dims):
    return jax.ShapeDtypeStruct(dims, F32)


def scratch(*dims):
    return pltpu.VMEM(dims, F32)


def ring(x, axis, step):
    n = lax.axis_size(axis)
    return lax.ppermute(x, axis, [(i, (i + step) % n) for i in range(n)])


def swap(x):
    return lax.ppermute(x, "gz", [(0, 1), (1, 0)])


def on_device(membrane, recovery, extracellular, fiber_scale, labels):
    nx, ny = lax.axis_size("gx"), lax.axis_size("gy")
    place = jnp.stack(
        [lax.axis_index("gx"), lax.axis_index("gy"), lax.axis_index("gz"), nx, ny]
    ).astype(jnp.int32)
    own, xup, xdn, yup, ydn, rnext = pl.pallas_call(
        prep_kernel,
        out_shape=(
            shape(4, BX, BY, BZ),
            shape(4, H, BY, BZ),
            shape(4, H, BY, BZ),
            shape(4, BX, 8, BZ),
            shape(4, BX, 8, BZ),
            shape(BX, BY, BZ),
        ),
        in_specs=[VMEM] * 5,
        out_specs=(VMEM,) * 6,
        compiler_params=PARAMS,
        name="prep",
    )(membrane, recovery, extracellular, fiber_scale, labels)
    xlo, xhi = ring(xup, "gx", 1), ring(xdn, "gx", -1)
    ylo, yhi = ring(yup, "gy", 1), ring(ydn, "gy", -1)
    clo = ring(jnp.concatenate([xlo[:, :, 8:16], xhi[:, :, 8:16]], axis=1), "gy", 1)
    chi = ring(jnp.concatenate([xlo[:, :, 0:8], xhi[:, :, 0:8]], axis=1), "gy", -1)
    halos = []
    for piece in (own, xlo, xhi, ylo, yhi, clo, chi):
        halos += [piece, swap(piece)]
    fine = (X0, Y0, Z0)
    mnext, v0, b0, in0, packed = pl.pallas_call(
        fine_kernel,
        out_shape=(
            shape(BX, BY, BZ), shape(*fine), shape(*fine), shape(*fine), shape(2, 8, 8, Z1),
        ),
        in_specs=[SMEM] + [VMEM] * 14,
        out_specs=(VMEM,) * 5,
        scratch_shapes=[scratch(*fine)] * 12 + [scratch(16, BY, Z0), scratch(2, 256, 128)],
        compiler_params=PARAMS,
        name="fine",
    )(place, *halos)
    wide = jnp.concatenate([ring(packed, "gy", 1), packed, ring(packed, "gy", -1)], axis=2)
    low, high = ring(wide[:, 8 - H :], "gx", 1), ring(wide[:, :H], "gx", -1)
    mid = (X1, Y1, Z1)
    v1, b1, in1, send = pl.pallas_call(
        middle_kernel,
        out_shape=(shape(*mid), shape(*mid), shape(*mid), shape(nx * ny, 16, Z2)),
        in_specs=[SMEM] + [VMEM] * 3,
        out_specs=(VMEM,) * 4,
        scratch_shapes=[scratch(*mid)] * 6 + [scratch(64, Z1), scratch(1, 64, 128)],
        compiler_params=PARAMS,
        name="middle",
    )(place, low, wide, high)
    got = lax.all_to_all(send, ("gx", "gy"), 0, 0, tiled=True)
    got_z = swap(got)
    grid2 = (4 * nx + 2 * PAD, 4 * ny, Z2)
    grid3 = (2 * nx + 2, 2 * ny, Z2)
    enext = pl.pallas_call(
        lambda *refs: up_kernel(*refs, nx=nx, ny=ny),
        out_shape=shape(BX, BY, BZ),
        in_specs=[SMEM] + [VMEM] * 8,
        out_specs=VMEM,
        scratch_shapes=[scratch(*grid2)] * 9
        + [scratch(*grid3)] * 8
        + [scratch(*mid)] * 5
        + [scratch(*fine)] * 5
        + [
            scratch(2, 2 * nx, 4 * ny, Z2),
            scratch(2, max(8 * nx * ny, 256), 128),
            scratch(4, 320, 128),
        ],
        compiler_params=PARAMS,
        name="up",
    )(place, got, got_z, v1, b1, in1, v0, b0, in0)
    return mnext, rnext, enext


def solution(mesh):
    spec = P("gx", "gy", "gz")
    return jax.shard_map(
        on_device, mesh=mesh, in_specs=(spec,) * 5, out_specs=(spec,) * 3, check_vma=False
    )
```

```python
import jax
import jax.numpy as jnp
from jax import lax
from jax.experimental import pallas as pl
from jax.experimental.pallas import tpu as pltpu
from jax.sharding import PartitionSpec as P

TIME_STEP = 0.05
IONIC_GAIN = 8.0
IONIC_ONSET = 0.15
RECOVERY_RATE = 0.01
COARSE_SWEEPS = 8

F32 = jnp.float32
BX, BY, BZ = 16, 16, 256
H = 3
K0, Y0, Z0 = BX // 2 + 2 * H, 32, 384
K1, Y1, Z1 = BX // 4 + 2 * H, 24, BZ
Z2 = BZ // 2
VMEM = pl.BlockSpec(memory_space=pltpu.VMEM)
HBM = pl.BlockSpec(memory_space=pltpu.HBM)


def params(mib):
    return pltpu.CompilerParams(vmem_limit_bytes=mib * 1024 * 1024)


def iota(shape, dim):
    return lax.broadcasted_iota(jnp.int32, shape, dim)


def first_is_red(shape):
    return ((iota(shape, len(shape) - 2) + iota(shape, len(shape) - 1)) & 1) == 0


def up(x, axis):
    return pltpu.roll(x, x.shape[axis] - 1, axis)


def down(x, axis):
    return pltpu.roll(x, 1, axis)


def pair_matrix(rows, cols, value, shift=0):
    return jnp.where(
        iota((rows, cols), 0) // 2 + shift == iota((rows, cols), 1), value, 0.0
    ).astype(F32)


def copy_matrix(rows, cols, shift=0):
    return jnp.where(
        iota((rows, cols), 1) // 2 + shift == iota((rows, cols), 0), 1.0, 0.0
    ).astype(F32)


def dot(a, b):
    return jnp.dot(a, b, precision=lax.Precision.HIGHEST, preferred_element_type=F32)


def sum_rows(buf, x):
    rows, cols = x.shape
    sums = []
    for c in range(cols // 128):
        buf[c, 0:rows, :] = x[:, 128 * c : 128 * c + 128]
        sums.append(buf[c, pl.ds(0, rows // 2, 2), :] + buf[c, pl.ds(1, rows // 2, 2), :])
    return sums[0] if len(sums) == 1 else jnp.concatenate(sums, axis=1)


def twice_rows(buf, x):
    rows, cols = x.shape
    for c in range(cols // 128):
        for k in (0, 1):
            buf[c, pl.ds(k, rows, 2), :] = x[:, 128 * c : 128 * c + 128]


def columns(buf, start, rows, cols):
    parts = [buf[c, pl.ds(start, rows), :] for c in range(cols // 128)]
    return parts[0] if len(parts) == 1 else jnp.concatenate(parts, axis=1)


def loop(start, stop, step, body):
    def run(index, carry):
        body(start + index * step)
        return carry

    lax.fori_loop(0, (stop - start) // step, run, 0)


def far(other, k, step, red, first):
    before, after = other[pl.ds(k - 1, step)], other[pl.ds(k + 1, step)]
    return jnp.where(first, before, after) if red else jnp.where(first, after, before)


def faces(inner, outer, near, fars, ys, zs, diag, inv, least, start, stop, step):
    rows, lanes = inner[0].shape[1:]
    shape = (step, rows, lanes)
    row, lane = iota(shape, 1), iota(shape, 2)
    first = first_is_red(shape)

    def body(k):
        here = pl.ds(k, step)
        low = jnp.minimum(inner[0][here], inner[1][here])
        if least is not None:
            least[0][here] = low
        halves = [0.5 * outer[c][here] for c in (0, 1)]
        pair = low + halves[0] + halves[1]
        near[here] = pair
        totals = [pair, pair]
        for axis, out, keep, place, size in (
            (1, ys, None if least is None else least[2], row, rows),
            (2, zs, None if least is None else least[3], lane, lanes),
        ):
            full = []
            for c in (0, 1):
                o = 1 - c
                mine = inner[c][here]
                low = jnp.where(place < size - 1, jnp.minimum(mine, up(inner[o][here], axis)), 0.0)
                if keep is not None:
                    keep[c][here] = low
                both = low + halves[c] + jnp.where(place < size - 1, up(halves[o], axis), 0.0)
                full.append(both)
                out[c][here] = jnp.where(place < size - 1, both, 0.0)
            for c in (0, 1):
                below = jnp.where(place > 0, down(full[1 - c], axis), halves[c])
                totals[c] = totals[c] + full[c] + below
        for c in (0, 1):
            o = 1 - c
            low = jnp.minimum(inner[c][here], far(inner[o], k, step, c == 0, first))
            if least is not None:
                least[1][c][here] = low
            both = low + halves[c] + 0.5 * far(outer[o], k, step, c == 0, first)
            fars[c][here] = both
            total = totals[c] + both
            if c == 0 and diag is not None:
                diag[here] = total
            inside = outer[c][here] > 0.0
            inv[c][here] = jnp.where(inside, 1.0 / jnp.where(inside, total, 1.0), 0.0)

    loop(start, stop, step, body)


def gathered(v, c, near, fars, ys, zs, k, step, first):
    here = pl.ds(k, step)
    o = 1 - c
    other = v[o][here]
    total = near[here] * other + fars[c][here] * far(v[o], k, step, c == 0, first)
    total = total + ys[c][here] * up(other, 1) + down(ys[o][here] * other, 1)
    return total + zs[c][here] * up(other, 2) + down(zs[o][here] * other, 2)


def half_sweep(v, b, c, coef, inv, start, stop, step):
    first = first_is_red((step,) + tuple(v[0].shape[1:]))

    def body(k):
        here = pl.ds(k, step)
        v[c][here] = (b[c][here] + gathered(v, c, *coef, k, step, first)) * inv[c][here]

    loop(start, stop, step, body)


def from_zero(v, b, coef, inv, start, stop, step):
    count = v[0].shape[0]
    for c in (0, 1):
        v[c][0:1] = jnp.zeros_like(v[c][0:1])
        v[c][count - 1 :] = jnp.zeros_like(v[c][0:1])

    def body(k):
        here = pl.ds(k, step)
        v[0][here] = b[0][here] * inv[0][here]

    loop(start, stop, step, body)
    half_sweep(v, b, 1, coef, inv, start, stop, step)


def put(bufs, k, rows, lanes, a, b):
    some = a if b is None else b
    a = jnp.zeros_like(some) if a is None else a
    b = jnp.zeros_like(some) if b is None else b
    first = first_is_red(some.shape)
    bufs[0][k, rows, lanes] = jnp.where(first, a, b)
    bufs[1][k, rows, lanes] = jnp.where(first, b, a)


def colours(x):
    n = x.shape[0] // 2
    first = first_is_red(x.shape[1:])
    pairs = [(x[2 * p], x[2 * p + 1]) for p in range(n)]
    return (
        jnp.stack([jnp.where(first, a, b) for a, b in pairs]),
        jnp.stack([jnp.where(first, b, a) for a, b in pairs]),
    )


def where_am_i():
    return lax.axis_index("gx"), lax.axis_index("gy"), lax.axis_index("gz")


def flags():
    gx, gy, _ = where_am_i()
    return (
        (gx > 0).astype(F32),
        (gx < lax.axis_size("gx") - 1).astype(F32),
        (gy > 0).astype(F32),
        (gy < lax.axis_size("gy") - 1).astype(F32),
    )


def fetch(pairs, sems):
    copies = [pltpu.make_async_copy(src, dst, sems.at[i]) for i, (src, dst) in enumerate(pairs)]
    for copy in copies:
        copy.start()
    return copies


def outside(shape, own_rows, k, own, has):
    row = iota(shape, len(shape) - 2)
    in_y = jnp.where(row < 8, has[2], jnp.where(row < 8 + own_rows, 1.0, has[3]))
    return in_y * jnp.where(k < H, has[0], jnp.where(k < H + own, 1.0, has[1]))


def block_of(i):
    rows, lanes = 8 * ((i % 4) // 2), 128 * (i % 2)
    return i // 4, slice(rows, rows + 8), slice(lanes, lanes + 128)


def block_of24(i):
    tile, half = (i % 6) // 2, i % 2
    return i // 6, slice(8 * tile, 8 * tile + 8), slice(128 * half, 128 * half + 128)


def prep_kernel(
    m_in, r_in, u_in, f_in, labels_in, own, xup, xdn, yup, ydn, m, r, u, f, labels, fold, sems
):
    copies = fetch(
        [(labels_in, labels), (m_in, m), (u_in, u), (r_in, r), (f_in, f)], sems
    )
    for copy in copies:
        copy.wait()
    spread = jnp.where(iota((BZ // 8, BZ), 1) // 8 == iota((BZ // 8, BZ), 0), 1.0, 0.0).astype(F32)
    for bx in range(BX // 8):
        wide = jnp.dot(labels[bx].astype(F32), spread, preferred_element_type=F32)
        kind = jnp.concatenate(
            [jnp.broadcast_to(wide[by : by + 1], (8, BZ)) for by in range(BY // 8)], axis=0
        )
        factor = jnp.where(kind > 1.5, 0.3, jnp.where(kind > 0.5, 1.0, 0.0)).astype(F32)
        for x in range(8 * bx, 8 * bx + 8):
            mm, rr, uu = m[x], r[x], u[x]
            inner = factor * f[x]
            own[x] = mm + uu
            own[BX + x] = inner
            ionic = IONIC_GAIN * mm * (mm - IONIC_ONSET) * (mm - 1.0) + mm * rr
            own[2 * BX + x] = mm - jnp.where(kind > 0.5, TIME_STEP * ionic, 0.0)
            own[3 * BX + x] = uu
    sums = jnp.concatenate(
        [own[BX + 2 * p] + own[BX + 2 * p + 1] for p in range(BX // 2)], axis=0
    )
    mean = sum_rows(fold, dot(sums, pair_matrix(BZ, BZ // 2, 0.125)))
    for i in range(8):
        slab, rows, lanes = block_of(i)
        own[4 * BX + slab, rows, lanes] = mean[8 * i : 8 * i + 8]
        slab, rows, lanes = block_of24(i)
        yup[BX + slab, rows, lanes] = mean[8 * i : 8 * i + 8]
        ydn[BX + slab, rows, lanes] = mean[8 * i : 8 * i + 8]
    for i in range(5):
        slab, rows, lanes = block_of(i)
        xup[18 + slab, rows, lanes] = mean[8 * (3 + i) : 8 * (4 + i)]
        xdn[18 + slab, rows, lanes] = mean[8 * i : 8 * i + 8]
    base = 0
    for q, depth in enumerate((5, 5, 4, 4)):
        xup[base : base + depth] = own[BX * (q + 1) - depth : BX * (q + 1)]
        xdn[base : base + depth] = own[BX * q : BX * q + depth]
        base += depth
    row = iota((8, BZ), 0)
    for x in range(BX):
        for q in (0, 1):
            yup[x, 8 * q : 8 * q + 8] = own[BX * q + x, 8:16]
            ydn[x, 8 * q : 8 * q + 8] = own[BX * q + x, 0:8]
        w, v = own[2 * BX + x], own[3 * BX + x]
        yup[x, 16:24] = merge(True, w[8:16], v[8:16])
        ydn[x, 16:24] = merge(False, w[0:8], v[0:8])


def merge(high, a, b):
    row = iota(a.shape, 0)
    return jnp.where(row >= 4, a, pltpu.roll(b, 4, 0)) if high else jnp.where(
        row < 4, a, pltpu.roll(b, 4, 0)
    )


def corner_kernel(xlo, xhi, cup, cdn):
    for high, out in ((True, cup), (False, cdn)):
        rows = slice(8, 16) if high else slice(0, 8)
        for side, src in ((0, xlo), (1, xhi)):
            at = lambda base, depth, d: src[base + (depth - d if side == 0 else d - 1), rows]
            s, n, w, u = (
                lambda d: at(0, 5, d),
                lambda d: at(5, 5, d),
                lambda d: at(10, 4, d),
                lambda d: at(14, 4, d),
            )
            tiles = [
                merge(high, s(1), s(2)),
                merge(high, s(3), s(4)),
                merge(high, n(1), n(2)),
                merge(high, n(3), n(4)),
                merge(high, w(1), w(2)),
                merge(high, u(1), u(2)),
                merge(high, w(3), u(3)),
            ]
            for t, tile in enumerate(tiles):
                out[10 * side + t] = tile

            def coarse(d):
                slab, block_rows, lanes = block_of(5 - d if side == 0 else d - 1)
                return src[18 + slab, block_rows, lanes]

            for d in range(1, 6):
                tile, lanes = 10 * side + 7 + (d - 1) // 2, 128 * ((d - 1) % 2)
                out[tile, :, lanes : lanes + 128] = coarse(d)


def fine_kernel(*refs):
    pieces, refs = refs[:14], refs[14:]
    mnext, rhs1, refs = refs[0], refs[1], refs[2:]
    mean1, refs = refs[0:2], refs[2:]
    v, b, near, fars, ys, zs, inv, refs = (
        refs[0:2], refs[2:4], refs[4], refs[5:7], refs[7:9], refs[9:11], refs[11:13], refs[13:],
    )
    inner, outer, s, w, refs = refs[0:2], refs[2:4], refs[4:6], refs[6:8], refs[8:]
    low_near, low_far, low_y, low_z, diag, fold, fold2 = (
        refs[0], refs[1:3], refs[3:5], refs[5:7], refs[7], refs[8], refs[9],
    )
    mout, sems = refs[10], refs[11]
    core = lax.axis_index("gz")
    has = flags()
    fields = (s, inner, w, v)
    for side in (0, 1):
        own, xlo, xhi, ylo, yhi, clo, chi = pieces[side::2]
        wide = BZ if side == 0 else 128
        src = pl.ds(0 if side == 0 else pl.multiple_of(core * 128, 128), wide)
        dst = pl.ds(pl.multiple_of(core * 128 if side == 0 else (1 - core) * 256, 128), wide)
        mid, low, high = slice(8, 24), slice(0, 8), slice(24, 32)

        def body(p, own=own, ylo=ylo, yhi=yhi, src=src, dst=dst):
            k = p + H
            for q, bufs in enumerate(fields):
                put(bufs, k, mid, dst, own[BX * q + 2 * p, :, src], own[BX * q + 2 * p + 1, :, src])
            for rows, ref, flag in ((low, ylo, has[2]), (high, yhi, has[3])):
                for q in (0, 1):
                    part = slice(8 * q, 8 * q + 8)
                    put(
                        fields[q], k, rows, dst,
                        ref[2 * p, part, src] * flag, ref[2 * p + 1, part, src] * flag,
                    )
                a, c = (ref[2 * p + i, 16:24, src] * flag for i in (0, 1))
                put(w, k, rows, dst, a, c)
                put(v, k, rows, dst, pltpu.roll(a, 4, 0), pltpu.roll(c, 4, 0))

        loop(0, BX // 2, 1, body)
        for x_side, ref, flag in ((0, xlo, has[0]), (1, xhi, has[1])):
            base = 0
            order = (5, 4, 3, 2, 1) if x_side == 0 else (1, 2, 3, 4, 5)
            for q, depth in enumerate((5, 5, 4, 4)):
                slabs = {d: ref[base + i, :, src] * flag for i, d in enumerate(
                    [d for d in order if d <= depth])}
                base += depth
                for j in range(H):
                    near_d, far_d = 2 * j + 1, 2 * j + 2
                    pair = (slabs.get(near_d), slabs.get(far_d))
                    k = H - 1 - j if x_side == 0 else K0 - H + j
                    if x_side == 0:
                        pair = pair[::-1]
                    if pair[0] is None and pair[1] is None:
                        pair = (jnp.zeros((16, wide), F32), None)
                    put(fields[q], k, mid, dst, *pair)
            for rows, cref, yflag in ((low, clo, has[2]), (high, chi, has[3])):
                both = flag * yflag
                tile = [cref[10 * x_side + t, :, src] * both for t in range(7)]
                turned = [pltpu.roll(t, 4, 0) for t in tile]
                zero = jnp.zeros((8, wide), F32)
                by_field = (
                    (tile[0], turned[0], tile[1], turned[1]),
                    (tile[2], turned[2], tile[3], turned[3]),
                    (tile[4], turned[4], tile[6], zero),
                    (tile[5], turned[5], turned[6], zero),
                )
                for q in range(4):
                    slabs = by_field[q] + (zero, zero)
                    for j in range(H):
                        pair = (slabs[2 * j], slabs[2 * j + 1])
                        k = H - 1 - j if x_side == 0 else K0 - H + j
                        put(fields[q], k, rows, dst, *(pair[::-1] if x_side == 0 else pair))
        dst = pl.ds(pl.multiple_of((core if side == 0 else 1 - core) * 128, 128), 128)
        for p in range(4):
            def of_own(i):
                slab, rows, lanes = block_of(i)
                return own[4 * BX + slab, rows, lanes]

            put(mean1, p + H, slice(8, 16), dst, of_own(2 * p), of_own(2 * p + 1))
            for rows, ref, flag in ((slice(0, 8), ylo, has[2]), (slice(16, 24), yhi, has[3])):
                def of_y(i):
                    slab, part, lanes = block_of24(i)
                    return ref[BX + slab, part, lanes] * flag

                put(mean1, p + H, rows, dst, of_y(2 * p), of_y(2 * p + 1))
        for x_side, ref, flag in ((0, xlo, has[0]), (1, xhi, has[1])):
            def of_x(d):
                slab, part, lanes = block_of(5 - d if x_side == 0 else d - 1)
                return ref[18 + slab, part, lanes] * flag

            zero = jnp.zeros((8, 128), F32)
            mids = [of_x(d) for d in (1, 2, 3, 4, 5)] + [zero]
            columns_of = [(slice(8, 16), mids)]
            for rows, cref, yflag in ((slice(0, 8), clo, has[2]), (slice(16, 24), chi, has[3])):
                t = [
                    cref[10 * x_side + 7 + i // 2, :, 128 * (i % 2) : 128 * (i % 2) + 128]
                    * (flag * yflag)
                    for i in range(5)
                ]
                columns_of.append((rows, t + [zero]))
            for rows, slabs in columns_of:
                for j in range(H):
                    pair = (slabs[2 * j], slabs[2 * j + 1])
                    k = H - 1 - j if x_side == 0 else K1 - H + j
                    put(mean1, k, rows, dst, *(pair[::-1] if x_side == 0 else pair))

    def body(k):
        here = pl.ds(k, 1)
        inside = outside((1, Y0, Z0), 16, k, BX // 2, has)
        for c in (0, 1):
            outer[c][here] = jnp.where(inner[c][here] > 0.0, 1.0, 3.0 * inside)

    loop(0, K0, 1, body)
    faces(
        inner, outer, near, fars, ys, zs, diag, inv, (low_near, low_far, low_y, low_z), 1, K0 - 1, 1
    )
    first = first_is_red((1, Y0, Z0))

    def intra(x, k):
        here = pl.ds(k, 1)
        a = [x[0][here], x[1][here]]
        flow = low_near[here] * (a[1] - a[0])
        total = [flow, -flow]
        for c in (0, 1):
            total[c] = total[c] + low_far[c][here] * (far(x[1 - c], k, 1, c == 0, first) - a[c])
        for axis, low in ((1, low_y), (2, low_z)):
            flows = [low[c][here] * (up(a[1 - c], axis) - a[c]) for c in (0, 1)]
            for c in (0, 1):
                total[c] = total[c] + flows[c] - down(flows[1 - c], axis)
        return total

    def body(k):
        here = pl.ds(k, 1)
        drive = intra(s, k)
        for c in (0, 1):
            w[c][here] = w[c][here] + TIME_STEP * drive[c]

    loop(1, K0 - 1, 1, body)
    lanes = pl.ds(pl.multiple_of(core * 128, 128), BZ)
    half_first = first_is_red((BY, BZ))

    def body(p):
        a, c = w[0][p + H, 8:24, lanes], w[1][p + H, 8:24, lanes]
        mout[2 * p] = jnp.where(half_first, a, c)
        mout[2 * p + 1] = jnp.where(half_first, c, a)

    loop(0, BX // 2, 1, body)
    copies = fetch([(mout, mnext)], sems)

    def body(k):
        here = pl.ds(k, 1)
        both = intra(w, k)
        for c in (0, 1):
            b[c][here] = both[c]

    loop(1, K0 - 1, 1, body)
    coef = (near, fars, ys, zs)
    half_sweep(v, b, 0, coef, inv, 1, K0 - 1, 1)
    half_sweep(v, b, 1, coef, inv, 2, K0 - 2, 1)

    def body(p):
        here = pl.ds(p + H, 1)
        res = b[0][here] - (diag[here] * v[0][here] - gathered(v, 0, *coef, p + H, 1, first))
        fold[pl.ds(p, 1)] = res[:, 8:24, :]

    loop(0, BX // 2, 1, body)
    half = BX // 2 * BY
    pairs = pair_matrix(Z0, Z1, 0.5, core * 64)
    coarse = sum_rows(fold2, dot(fold[...].reshape(half, Z0), pairs)).reshape(8, 8, Z1)
    red, black = colours(coarse)
    rhs1[0] = red
    rhs1[1] = black
    copies[0].wait()


def middle_faces_kernel(m_in, r_in, *refs):
    inner, refs = refs[0:2], refs[2:]
    rnext, near, fars, ys, zs, diag, inv, outer = (
        refs[0], refs[1], refs[2:4], refs[4:6], refs[6:8], refs[8], refs[9:11], refs[11:13],
    )
    m, r, sems = refs[13:]
    copies = fetch([(m_in, m), (r_in, r)], sems)
    has = flags()
    for k in range(K1):
        inside = outside((Y1, Z1), 8, k, 4, has)
        for c in (0, 1):
            outer[c][k] = jnp.where(inner[c][k] > 0.0, 1.0, 3.0 * inside)
    for copy in copies:
        copy.wait()
    for x in range(BX):
        mm, rr = m[x], r[x]
        r[x] = rr + TIME_STEP * RECOVERY_RATE * (
            -rr - IONIC_GAIN * mm * (mm - IONIC_ONSET - 1.0)
        )
    copies = fetch([(r, rnext)], sems)
    faces(inner, outer, near, fars, ys, zs, diag, inv, None, 1, K1 - 1, 2)
    copies[0].wait()


def join_kernel(low, own, high, wide, xup, xdn):
    for c in (0, 1):
        for p in range(4):
            for i, ref in enumerate((low, own, high)):
                rows = slice(8 * i, 8 * i + 8)
                wide[c, p, rows] = ref[c, p]
                if p < 2:
                    xdn[c, p, rows] = ref[c, p]
                else:
                    xup[c, p - 2, rows] = ref[c, p]


def spread_kernel(got, send):
    whole = got[...]
    for d in range(send.shape[0]):
        send[d] = whole


def middle_kernel(low, own, high, *refs):
    inner, refs = refs[0:2], refs[2:]
    near, fars, ys, zs, diag, inv, refs = (
        refs[0], refs[1:3], refs[3:5], refs[5:7], refs[7], refs[8:10], refs[10:],
    )
    v, b, send, fold, fold2 = refs[0:2], refs[2:4], refs[4], refs[5], refs[6]
    core = lax.axis_index("gz")
    has = flags()
    for c in (0, 1):
        b[c][0:1] = jnp.zeros((1, Y1, Z1), F32)
        b[c][K1 - 1 :] = jnp.zeros((1, Y1, Z1), F32)
        for k in range(1, K1 - 1):
            src = low[c, k - 1] if k < H else (own[c, k - H] if k < H + 4 else high[c, k - H - 4])
            b[c][k] = src * outside((Y1, Z1), 8, k, 4, has)
    coef = (near, fars, ys, zs)
    from_zero(v, b, coef, inv, 1, K1 - 1, 2)
    first = first_is_red((2, Y1, Z1))
    for p in (0, 2):
        here = slice(p + H, p + H + 2)
        res = b[0][here] - (diag[here] * v[0][here] - gathered(v, 0, *coef, p + H, 2, first))
        res = res[:, 8:16, :]
        fold[8 * p : 8 * p + 16] = res.reshape(16, Z1)
        total = (inner[0][here] + inner[1][here])[:, 8:16, :]
        fold[32 + 8 * p : 48 + 8 * p] = 0.25 * total.reshape(16, Z1)
    both = sum_rows(fold2, dot(fold[...], pair_matrix(Z1, Z2, 0.5)))
    lane = iota((8, Z2), 1)
    out = []
    for q in (0, 1):
        red, black = colours(both[16 * q : 16 * q + 16].reshape(4, 4, Z2))
        red, black = red.reshape(8, Z2), black.reshape(8, Z2)
        lower = jnp.where(lane < 64, red, pltpu.roll(black, 64, 1))
        upper = jnp.where(lane < 64, pltpu.roll(red, 64, 1), black)
        out.append(jnp.where(core == 0, lower, upper))
    piece = jnp.concatenate(out, axis=0)
    for d in range(send.shape[0]):
        send[d] = piece


def up_kernel(got, got_z, *refs, nx, ny):
    level1, refs = refs[:13], refs[13:]
    level0, refs = refs[:13], refs[13:]
    out, refs = refs[0], refs[1:]

    def split(r):
        return r[0:2], r[2:4], (r[4], r[5:7], r[7:9], r[9:11]), r[11:13]

    v1, b1, coef1, inv1 = split(level1)
    v0, b0, coef0, inv0 = split(level0)
    n2, y2 = 2 * nx, 4 * ny
    n3, y3 = nx, 2 * ny
    v2, b2, coef2, inv2 = split(refs[:13])
    in2, out2, diag2, refs = refs[13:15], refs[15:17], refs[17], refs[18:]
    v3, b3, coef3, inv3 = split(refs[:13])
    in3, out3, refs = refs[13:15], refs[15:17], refs[17:]
    parts, fold2, fold1, fold0 = refs[0:2], refs[2], refs[3], refs[4]
    gx_me, gy_me, core = where_am_i()
    lane = iota((2, y2, Z2), 2)

    def body(gx):
        for side in (0, 1):
            src = got if side == 0 else got_z
            for gy in range(ny):
                d = gx * ny + gy
                for q in (0, 1):
                    for p in (0, 1):
                        row = 8 * q + 4 * p
                        parts[side][2 * q + p, 4 * gy : 4 * gy + 4, :] = src[d, row : row + 4, :]
        for q, bufs in ((0, b2), (1, in2)):
            mine, other = parts[0][2 * q : 2 * q + 2], parts[1][2 * q : 2 * q + 2]
            h0 = jnp.where(core == 0, mine, other)
            h1 = jnp.where(core == 0, other, mine)
            here = pl.ds(1 + 2 * gx, 2)
            bufs[0][here] = jnp.where(lane < 64, h0, pltpu.roll(h1, 64, 2))
            bufs[1][here] = jnp.where(lane < 64, pltpu.roll(h0, 64, 2), h1)
            if q == 1:
                for c in (0, 1):
                    out2[c][here] = jnp.where(in2[c][here] > 0.0, 1.0, 3.0)

    loop(0, nx, 1, body)
    for bufs, count in ((in2, n2), (out2, n2), (in3, n3), (out3, n3)):
        for c in (0, 1):
            bufs[c][0:1] = jnp.zeros_like(bufs[c][0:1])
            bufs[c][count + 1 :] = jnp.zeros_like(bufs[c][0:1])
    faces(in2, out2, *coef2, diag2, inv2, None, 1, n2 + 1, 2)
    from_zero(v2, b2, coef2, inv2, 1, n2 + 1, 4)
    first = first_is_red((4, y2, Z2))

    def body(k):
        here, there = pl.ds(k, 4), pl.ds(k - 1, 4)
        res = b2[0][here] - (diag2[here] * v2[0][here] - gathered(v2, 0, *coef2, k, 4, first))
        fold2[0, pl.ds(pl.multiple_of((k - 1) * y2, 4 * y2), 4 * y2), :] = res.reshape(4 * y2, Z2)
        total = 0.25 * (in2[0][here] + in2[1][here])
        fold2[1, pl.ds(pl.multiple_of((k - 1) * y2, 4 * y2), 4 * y2), :] = total.reshape(4 * y2, Z2)

    loop(1, n2 + 1, 4, body)
    pairs = pair_matrix(Z2, Z2, 0.5)
    rows = n2 * y3
    first3 = first_is_red((1, y3, Z2))
    lane3 = iota((1, y3, Z2), 2)
    for q in (0, 1):
        sums = fold2[q, pl.ds(0, rows, 2), :] + fold2[q, pl.ds(1, rows, 2), :]
        fold1[0, 0:rows, :] = dot(sums, pairs)
        bufs = (b3, in3)[q]

        def body(p):
            a = fold1[0, pl.ds(pl.multiple_of(2 * p * y3, y3), y3), :][None]
            c = fold1[0, pl.ds(pl.multiple_of((2 * p + 1) * y3, y3), y3), :][None]
            here = pl.ds(p + 1, 1)
            bufs[0][here] = jnp.where(first3, a, c)
            bufs[1][here] = jnp.where(first3, c, a)
            if q == 1:
                for colour in (0, 1):
                    value = jnp.where(in3[colour][here] > 0.0, 1.0, 3.0)
                    out3[colour][here] = jnp.where(lane3 < Z2 // 2, value, 0.0)

        loop(0, n3, 1, body)
    step3 = 8 if n3 % 8 == 0 else n3
    faces(in3, out3, *coef3, None, inv3, None, 1, n3 + 1, step3)
    from_zero(v3, b3, coef3, inv3, 1, n3 + 1, step3)

    def sweep(i):
        half_sweep(v3, b3, 0, coef3, inv3, 1, n3 + 1, step3)
        half_sweep(v3, b3, 1, coef3, inv3, 1, n3 + 1, step3)

    loop(0, COARSE_SWEEPS - 1, 1, sweep)
    for p in range(n3):
        a, c = v3[0][p + 1 : p + 2], v3[1][p + 1 : p + 2]
        fold2[0, 2 * p * y3 : (2 * p + 1) * y3, :] = jnp.where(first3, a, c)[0]
        fold2[0, (2 * p + 1) * y3 : (2 * p + 2) * y3, :] = jnp.where(first3, c, a)[0]
    twice_rows(fold1, dot(fold2[0, 0:rows, :], copy_matrix(Z2, Z2)))

    def body(k):
        here = pl.ds(k, 4)
        start = pl.multiple_of((k - 1) * y2, 4 * y2)
        e = fold1[0, pl.ds(start, 4 * y2), :].reshape(4, y2, Z2)
        for c in (0, 1):
            v2[c][here] = v2[c][here] + e

    loop(1, n2 + 1, 4, body)
    half_sweep(v2, b2, 0, coef2, inv2, 1, n2 + 1, 4)
    half_sweep(v2, b2, 1, coef2, inv2, 1, n2 + 1, 4)
    shift = lax.rem(4 - 4 * gy_me + 2 * y2, y2)
    first1 = first_is_red((y2, Z2))
    cells = []
    for j in range(4):
        a, c = v2[0][2 * gx_me + j], v2[1][2 * gx_me + j]
        for cell in (jnp.where(first1, a, c), jnp.where(first1, c, a)):
            cells.append(pltpu.roll(cell, shift, 0)[0:16])
    twice_rows(fold1, dot(jnp.concatenate(cells, axis=0), copy_matrix(Z2, Z1)))
    for k in range(1, K1 - 1):
        e = columns(fold1, 32 * (k - 1), Y1, Z1)
        for c in (0, 1):
            v1[c][k] = jnp.where(inv1[c][k] > 0.0, v1[c][k] + e, 0.0)
    half_sweep(v1, b1, 0, coef1, inv1, 1, K1 - 1, 2)
    half_sweep(v1, b1, 1, coef1, inv1, 1, K1 - 1, 2)
    first0 = first_is_red((Y1, Z1))
    cells = []
    for k in range(H - 1, K1 - H + 1):
        a, c = v1[0][k], v1[1][k]
        cells += [jnp.where(first0, a, c), jnp.where(first0, c, a)]
    cells = [cell[4:20] for cell in cells[1:-1]]
    twice_rows(fold0, dot(jnp.concatenate(cells, axis=0), copy_matrix(Z1, Z0, core * 64)))

    def body(p):
        e = columns(fold0, pl.multiple_of(p * 32, 32), 32, Z0)[None]
        here = pl.ds(p + H - 1, 1)
        for c in (0, 1):
            v0[c][here] = jnp.where(inv0[c][here] > 0.0, v0[c][here] + e, 0.0)

    loop(0, BX // 2 + 2, 1, body)
    half_sweep(v0, b0, 0, coef0, inv0, H - 1, K0 - H + 1, 1)
    half_sweep(v0, b0, 1, coef0, inv0, H, K0 - H, 1)
    lanes = pl.ds(pl.multiple_of(core * 128, 128), BZ)
    half_first = first_is_red((BY, BZ))

    def body(p):
        a, c = v0[0][p + H, 8:24, lanes], v0[1][p + H, 8:24, lanes]
        out[2 * p] = jnp.where(half_first, a, c)
        out[2 * p + 1] = jnp.where(half_first, c, a)

    loop(0, BX // 2, 1, body)


def shape(*dims):
    return jax.ShapeDtypeStruct(dims, F32)


def scratch(*dims):
    return pltpu.VMEM(dims, F32)


def ring(x, axis, step):
    n = lax.axis_size(axis)
    return lax.ppermute(x, axis, [(i, (i + step) % n) for i in range(n)])


def swap(x):
    return lax.ppermute(x, "gz", [(0, 1), (1, 0)])


def call(kernel, name, mib, outs, scratches, *args, hbm_in=0, hbm_out=0):
    return pl.pallas_call(
        kernel,
        out_shape=tuple(shape(*o) for o in outs),
        in_specs=[HBM] * hbm_in + [VMEM] * (len(args) - hbm_in),
        out_specs=(HBM,) * hbm_out + (VMEM,) * (len(outs) - hbm_out),
        scratch_shapes=[scratch(*s) if isinstance(s, tuple) else s for s in scratches],
        compiler_params=params(mib),
        name=name,
    )(*args)


def on_device(membrane, recovery, extracellular, fiber_scale, labels):
    nx, ny = lax.axis_size("gx"), lax.axis_size("gy")
    block = (BX, BY, BZ)
    held = [
        pltpu.with_memory_space_constraint(x, pltpu.HBM)
        for x in (membrane, recovery, extracellular, fiber_scale, labels)
    ]
    own, xup, xdn, yup, ydn = call(
        prep_kernel, "prep", 6,
        [(4 * BX + 2, BY, BZ)] + [(20, BY, BZ)] * 2 + [(BX + 2, 24, BZ)] * 2,
        [block] * 4
        + [pltpu.VMEM(labels.shape, jnp.int32), (1, 128, 128), pltpu.SemaphoreType.DMA((5,))],
        *held, hbm_in=5,
    )
    xlo, xhi = ring(xup, "gx", 1), ring(xdn, "gx", -1)
    ylo, yhi = ring(yup, "gy", 1), ring(ydn, "gy", -1)
    cup, cdn = call(corner_kernel, "corner", 4, [(20, 8, BZ)] * 2, [], xlo, xhi)
    clo, chi = ring(cup, "gy", 1), ring(cdn, "gy", -1)
    halos = []
    for piece in (own, xlo, xhi, ylo, yhi, clo, chi):
        halos += [piece, swap(piece)]
    fine = (K0, Y0, Z0)
    mid = (K1, Y1, Z1)
    mnext, rhs1, in1r, in1b, *level0 = call(
        fine_kernel, "fine", 20,
        [block, (2, 4, 8, Z1)] + [mid] * 2 + [fine] * 13,
        [fine] * 16
        + [(8, BY, Z0), (2, 128, 128), block, pltpu.SemaphoreType.DMA((1,))],
        *halos, hbm_out=1,
    )
    rnext, *coef1 = call(
        middle_faces_kernel, "middle_faces", 4, [block] + [mid] * 10,
        [mid] * 2 + [block] * 2 + [pltpu.SemaphoreType.DMA((2,))],
        held[0], held[1], in1r, in1b, hbm_in=2, hbm_out=1,
    )
    part = (2, 2, Y1, Z1)
    wide, xup, xdn = call(
        join_kernel, "join", 4, [(2, 4, Y1, Z1), part, part], [],
        ring(rhs1, "gy", 1), rhs1, ring(rhs1, "gy", -1),
    )
    low, high = ring(xup, "gx", 1), ring(xdn, "gx", -1)
    v1r, v1b, b1r, b1b, send = call(
        middle_kernel, "middle", 4,
        [mid] * 4 + [(ny, 16, Z2)],
        [(64, Z1), (1, 64, 128)],
        low, wide, high, in1r, in1b, *coef1,
    )
    got = lax.all_to_all(send, "gy", 0, 0, tiled=True)
    (send,) = call(spread_kernel, "spread", 4, [(nx, ny, 16, Z2)], [], got)
    got = lax.all_to_all(send, "gx", 0, 0, tiled=True).reshape(nx * ny, 16, Z2)
    grid2, grid3 = (2 * nx + 2, 4 * ny, Z2), (nx + 2, 2 * ny, Z2)
    level1 = [v1r, v1b, b1r, b1b, *coef1[:7], *coef1[8:]]
    (enext,) = call(
        lambda *refs: up_kernel(*refs, nx=nx, ny=ny), "up", 24,
        [block],
        [grid2] * 18 + [grid3] * 17
        + [(4, 4 * ny, Z2)] * 2
        + [(2, 8 * nx * ny, Z2), (2, max(8 * nx * ny, 256), Z2), (3, 320, 128)],
        got, swap(got), *level1, *level0,
    )
    return mnext, rnext, enext


def solution(mesh):
    spec = P("gx", "gy", "gz")
    return jax.shard_map(
        on_device, mesh=mesh, in_specs=(spec,) * 5, out_specs=(spec,) * 3, check_vma=False
    )
```

```python
import jax
import jax.numpy as jnp
from jax import lax
from jax.experimental import pallas as pl
from jax.experimental.pallas import tpu as pltpu
from jax.sharding import PartitionSpec as P

TIME_STEP = 0.05
IONIC_GAIN = 8.0
IONIC_ONSET = 0.15
RECOVERY_RATE = 0.01
COARSE_SWEEPS = 8

F32 = jnp.float32
BX, BY, BZ = 16, 16, 256
H = 3
SF, SI, SH, SHB, S1, S2, SU, S22, S3 = 3, 4, 4, 5, 8, 8, 8, 16, 16
K0, Y0, Z0 = BX // 2 + 2 * H, 32, 384
K1, Y1, Z1 = BX // 4 + 2 * H, 24, BZ
Z2 = BZ // 2
VMEM = pl.BlockSpec(memory_space=pltpu.VMEM)
HBM = pl.BlockSpec(memory_space=pltpu.HBM)


def params(mib):
    return pltpu.CompilerParams(vmem_limit_bytes=mib * 1024 * 1024)


def iota(shape, dim):
    return lax.broadcasted_iota(jnp.int32, shape, dim)


def first_is_red(shape):
    return ((iota(shape, len(shape) - 2) + iota(shape, len(shape) - 1)) & 1) == 0


def up(x, axis):
    return pltpu.roll(x, x.shape[axis] - 1, axis)


def down(x, axis):
    return pltpu.roll(x, 1, axis)


def pair_matrix(rows, cols, value, shift=0):
    return jnp.where(
        iota((rows, cols), 0) // 2 + shift == iota((rows, cols), 1), value, 0.0
    ).astype(F32)


def copy_matrix(rows, cols, shift=0):
    return jnp.where(
        iota((rows, cols), 1) // 2 + shift == iota((rows, cols), 0), 1.0, 0.0
    ).astype(F32)


def dot(a, b):
    b = b.astype(jnp.bfloat16)
    high = a.astype(jnp.bfloat16)
    rest = a - high.astype(F32)
    mid = rest.astype(jnp.bfloat16)
    low = (rest - mid.astype(F32)).astype(jnp.bfloat16)
    parts = [jnp.dot(p, b, preferred_element_type=F32) for p in (low, mid, high)]
    return parts[0] + parts[1] + parts[2]


def sum_rows(buf, x):
    rows, cols = x.shape
    sums = []
    for c in range(cols // 128):
        buf[c, 0:rows, :] = x[:, 128 * c : 128 * c + 128]
        sums.append(buf[c, pl.ds(0, rows // 2, 2), :] + buf[c, pl.ds(1, rows // 2, 2), :])
    return sums[0] if len(sums) == 1 else jnp.concatenate(sums, axis=1)


def twice_rows(buf, x):
    rows, cols = x.shape
    for c in range(cols // 128):
        for k in (0, 1):
            buf[c, pl.ds(k, rows, 2), :] = x[:, 128 * c : 128 * c + 128]


def columns(buf, start, rows, cols):
    parts = [buf[c, pl.ds(start, rows), :] for c in range(cols // 128)]
    return parts[0] if len(parts) == 1 else jnp.concatenate(parts, axis=1)


def loop(start, stop, step, body):
    if not isinstance(start, int) or stop - start == step:
        body(start)
        return

    def run(index, carry):
        body(start + index * step)
        return carry

    lax.fori_loop(0, (stop - start) // step, run, 0)


def far(other, k, step, red, first):
    before, after = other[pl.ds(k - 1, step)], other[pl.ds(k + 1, step)]
    return jnp.where(first, before, after) if red else jnp.where(first, after, before)


def faces(inner, outer, near, fars, ys, zs, diag, inv, least, start, stop, step):
    rows, lanes = inner[0].shape[1:]
    shape = (step, rows, lanes)
    row, lane = iota(shape, 1), iota(shape, 2)
    first = first_is_red(shape)

    def body(k):
        here = pl.ds(k, step)
        low = jnp.minimum(inner[0][here], inner[1][here])
        if least is not None:
            least[0][here] = low
        halves = [0.5 * outer[c][here] for c in (0, 1)]
        pair = low + halves[0] + halves[1]
        near[here] = pair
        totals = [pair, pair]
        for axis, out, keep, place, size in (
            (1, ys, None if least is None else least[2], row, rows),
            (2, zs, None if least is None else least[3], lane, lanes),
        ):
            full = []
            for c in (0, 1):
                o = 1 - c
                mine = inner[c][here]
                low = jnp.where(place < size - 1, jnp.minimum(mine, up(inner[o][here], axis)), 0.0)
                if keep is not None:
                    keep[c][here] = low
                both = low + halves[c] + jnp.where(place < size - 1, up(halves[o], axis), 0.0)
                full.append(both)
                out[c][here] = jnp.where(place < size - 1, both, 0.0)
            for c in (0, 1):
                below = jnp.where(place > 0, down(full[1 - c], axis), halves[c])
                totals[c] = totals[c] + full[c] + below
        for c in (0, 1):
            o = 1 - c
            low = jnp.minimum(inner[c][here], far(inner[o], k, step, c == 0, first))
            if least is not None:
                least[1][c][here] = low
            both = low + halves[c] + 0.5 * far(outer[o], k, step, c == 0, first)
            fars[c][here] = both
            total = totals[c] + both
            if c == 0 and diag is not None:
                diag[here] = total
            inside = outer[c][here] > 0.0
            inv[c][here] = jnp.where(inside, 1.0 / jnp.where(inside, total, 1.0), 0.0)

    loop(start, stop, step, body)


def gathered(v, c, near, fars, ys, zs, k, step, first):
    here = pl.ds(k, step)
    o = 1 - c
    other = v[o][here]
    total = near[here] * other + fars[c][here] * far(v[o], k, step, c == 0, first)
    total = total + ys[c][here] * up(other, 1) + down(ys[o][here] * other, 1)
    return total + zs[c][here] * up(other, 2) + down(zs[o][here] * other, 2)


def half_sweep(v, b, c, coef, inv, start, stop, step):
    first = first_is_red((step,) + tuple(v[0].shape[1:]))

    def body(k):
        here = pl.ds(k, step)
        v[c][here] = (b[c][here] + gathered(v, c, *coef, k, step, first)) * inv[c][here]

    loop(start, stop, step, body)


def from_zero(v, b, coef, inv, start, stop, step):
    count = v[0].shape[0]
    for c in (0, 1):
        v[c][0:1] = jnp.zeros_like(v[c][0:1])
        v[c][count - 1 :] = jnp.zeros_like(v[c][0:1])

    def body(k):
        here = pl.ds(k, step)
        v[0][here] = b[0][here] * inv[0][here]

    loop(start, stop, step, body)
    half_sweep(v, b, 1, coef, inv, start, stop, step)


def put(bufs, k, rows, lanes, a, b):
    some = a if b is None else b
    a = jnp.zeros_like(some) if a is None else a
    b = jnp.zeros_like(some) if b is None else b
    first = first_is_red(some.shape)
    bufs[0][k, rows, lanes] = jnp.where(first, a, b)
    bufs[1][k, rows, lanes] = jnp.where(first, b, a)


def colours(x):
    n = x.shape[0] // 2
    first = first_is_red(x.shape[1:])
    pairs = [(x[2 * p], x[2 * p + 1]) for p in range(n)]
    return (
        jnp.stack([jnp.where(first, a, b) for a, b in pairs]),
        jnp.stack([jnp.where(first, b, a) for a, b in pairs]),
    )


def where_am_i():
    return lax.axis_index("gx"), lax.axis_index("gy"), lax.axis_index("gz")


def flags():
    gx, gy, _ = where_am_i()
    return (
        (gx > 0).astype(F32),
        (gx < lax.axis_size("gx") - 1).astype(F32),
        (gy > 0).astype(F32),
        (gy < lax.axis_size("gy") - 1).astype(F32),
    )


def fetch(pairs, sems):
    copies = [pltpu.make_async_copy(src, dst, sems.at[i]) for i, (src, dst) in enumerate(pairs)]
    for copy in copies:
        copy.start()
    return copies


def outside(shape, own_rows, k, own, has):
    row = iota(shape, len(shape) - 2)
    in_y = jnp.where(row < 8, has[2], jnp.where(row < 8 + own_rows, 1.0, has[3]))
    return in_y * jnp.where(k < H, has[0], jnp.where(k < H + own, 1.0, has[1]))


def block_of(i):
    rows, lanes = 8 * ((i % 4) // 2), 128 * (i % 2)
    return i // 4, slice(rows, rows + 8), slice(lanes, lanes + 128)


def block_of24(i):
    tile, half = (i % 6) // 2, i % 2
    return i // 6, slice(8 * tile, 8 * tile + 8), slice(128 * half, 128 * half + 128)


def prep_kernel(
    m_in, r_in, u_in, f_in, labels_in, own, xup, xdn, yup, ydn, m, r, u, f, labels, fold, sems
):
    copies = fetch(
        [(labels_in, labels), (m_in, m), (u_in, u), (r_in, r), (f_in, f)], sems
    )
    for copy in copies:
        copy.wait()
    spread = jnp.where(iota((BZ // 8, BZ), 1) // 8 == iota((BZ // 8, BZ), 0), 1.0, 0.0).astype(F32)
    for bx in range(BX // 8):
        wide = jnp.dot(labels[bx].astype(F32), spread, preferred_element_type=F32)
        kind = jnp.concatenate(
            [jnp.broadcast_to(wide[by : by + 1], (8, BZ)) for by in range(BY // 8)], axis=0
        )
        factor = jnp.where(kind > 1.5, 0.3, jnp.where(kind > 0.5, 1.0, 0.0)).astype(F32)
        for x in range(8 * bx, 8 * bx + 8):
            mm, rr, uu = m[x], r[x], u[x]
            inner = factor * f[x]
            own[x] = mm + uu
            own[BX + x] = inner
            ionic = IONIC_GAIN * mm * (mm - IONIC_ONSET) * (mm - 1.0) + mm * rr
            own[2 * BX + x] = mm - jnp.where(kind > 0.5, TIME_STEP * ionic, 0.0)
            own[3 * BX + x] = uu
    sums = jnp.concatenate(
        [own[BX + 2 * p] + own[BX + 2 * p + 1] for p in range(BX // 2)], axis=0
    )
    mean = sum_rows(fold, dot(sums, pair_matrix(BZ, BZ // 2, 0.125)))
    for i in range(8):
        slab, rows, lanes = block_of(i)
        own[4 * BX + slab, rows, lanes] = mean[8 * i : 8 * i + 8]
        slab, rows, lanes = block_of24(i)
        yup[BX + slab, rows, lanes] = mean[8 * i : 8 * i + 8]
        ydn[BX + slab, rows, lanes] = mean[8 * i : 8 * i + 8]
    for i in range(5):
        slab, rows, lanes = block_of(i)
        xup[18 + slab, rows, lanes] = mean[8 * (3 + i) : 8 * (4 + i)]
        xdn[18 + slab, rows, lanes] = mean[8 * i : 8 * i + 8]
    base = 0
    for q, depth in enumerate((5, 5, 4, 4)):
        xup[base : base + depth] = own[BX * (q + 1) - depth : BX * (q + 1)]
        xdn[base : base + depth] = own[BX * q : BX * q + depth]
        base += depth
    row = iota((8, BZ), 0)
    for x in range(BX):
        for q in (0, 1):
            yup[x, 8 * q : 8 * q + 8] = own[BX * q + x, 8:16]
            ydn[x, 8 * q : 8 * q + 8] = own[BX * q + x, 0:8]
        w, v = own[2 * BX + x], own[3 * BX + x]
        yup[x, 16:24] = merge(True, w[8:16], v[8:16])
        ydn[x, 16:24] = merge(False, w[0:8], v[0:8])


def merge(high, a, b):
    row = iota(a.shape, 0)
    return jnp.where(row >= 4, a, pltpu.roll(b, 4, 0)) if high else jnp.where(
        row < 4, a, pltpu.roll(b, 4, 0)
    )


def corner_kernel(xlo, xhi, cup, cdn):
    for high, out in ((True, cup), (False, cdn)):
        rows = slice(8, 16) if high else slice(0, 8)
        for side, src in ((0, xlo), (1, xhi)):
            at = lambda base, depth, d: src[base + (depth - d if side == 0 else d - 1), rows]
            s, n, w, u = (
                lambda d: at(0, 5, d),
                lambda d: at(5, 5, d),
                lambda d: at(10, 4, d),
                lambda d: at(14, 4, d),
            )
            tiles = [
                merge(high, s(1), s(2)),
                merge(high, s(3), s(4)),
                merge(high, n(1), n(2)),
                merge(high, n(3), n(4)),
                merge(high, w(1), w(2)),
                merge(high, u(1), u(2)),
                merge(high, w(3), u(3)),
            ]
            for t, tile in enumerate(tiles):
                out[10 * side + t] = tile

            def coarse(d):
                slab, block_rows, lanes = block_of(5 - d if side == 0 else d - 1)
                return src[18 + slab, block_rows, lanes]

            for d in range(1, 6):
                tile, lanes = 10 * side + 7 + (d - 1) // 2, 128 * ((d - 1) % 2)
                out[tile, :, lanes : lanes + 128] = coarse(d)


def fine_kernel(*refs):
    pieces, refs = refs[:14], refs[14:]
    mnext, rhs1, refs = refs[0], refs[1], refs[2:]
    mean1, refs = refs[0:2], refs[2:]
    v, b, near, fars, ys, zs, inv, refs = (
        refs[0:2], refs[2:4], refs[4], refs[5:7], refs[7:9], refs[9:11], refs[11:13], refs[13:],
    )
    inner, outer, s, w, refs = refs[0:2], refs[2:4], refs[4:6], refs[6:8], refs[8:]
    low_near, low_far, low_y, low_z, diag, fold, fold2 = (
        refs[0], refs[1:3], refs[3:5], refs[5:7], refs[7], refs[8], refs[9],
    )
    mout, sems = refs[10], refs[11]
    core = lax.axis_index("gz")
    has = flags()
    fields = (s, inner, w, v)
    for side in (0, 1):
        own, xlo, xhi, ylo, yhi, clo, chi = pieces[side::2]
        wide = BZ if side == 0 else 128
        src = pl.ds(0 if side == 0 else pl.multiple_of(core * 128, 128), wide)
        dst = pl.ds(pl.multiple_of(core * 128 if side == 0 else (1 - core) * 256, 128), wide)
        mid, low, high = slice(8, 24), slice(0, 8), slice(24, 32)

        def body(p, own=own, ylo=ylo, yhi=yhi, src=src, dst=dst):
            k = p + H
            for q, bufs in enumerate(fields):
                put(bufs, k, mid, dst, own[BX * q + 2 * p, :, src], own[BX * q + 2 * p + 1, :, src])
            for rows, ref, flag in ((low, ylo, has[2]), (high, yhi, has[3])):
                for q in (0, 1):
                    part = slice(8 * q, 8 * q + 8)
                    put(
                        fields[q], k, rows, dst,
                        ref[2 * p, part, src] * flag, ref[2 * p + 1, part, src] * flag,
                    )
                a, c = (ref[2 * p + i, 16:24, src] * flag for i in (0, 1))
                put(w, k, rows, dst, a, c)
                put(v, k, rows, dst, pltpu.roll(a, 4, 0), pltpu.roll(c, 4, 0))

        loop(0, BX // 2, 1, body)
        for x_side, ref, flag in ((0, xlo, has[0]), (1, xhi, has[1])):
            base = 0
            order = (5, 4, 3, 2, 1) if x_side == 0 else (1, 2, 3, 4, 5)
            for q, depth in enumerate((5, 5, 4, 4)):
                slabs = {d: ref[base + i, :, src] * flag for i, d in enumerate(
                    [d for d in order if d <= depth])}
                base += depth
                for j in range(H):
                    near_d, far_d = 2 * j + 1, 2 * j + 2
                    pair = (slabs.get(near_d), slabs.get(far_d))
                    k = H - 1 - j if x_side == 0 else K0 - H + j
                    if x_side == 0:
                        pair = pair[::-1]
                    if pair[0] is None and pair[1] is None:
                        pair = (jnp.zeros((16, wide), F32), None)
                    put(fields[q], k, mid, dst, *pair)
            for rows, cref, yflag in ((low, clo, has[2]), (high, chi, has[3])):
                both = flag * yflag
                tile = [cref[10 * x_side + t, :, src] * both for t in range(7)]
                turned = [pltpu.roll(t, 4, 0) for t in tile]
                zero = jnp.zeros((8, wide), F32)
                by_field = (
                    (tile[0], turned[0], tile[1], turned[1]),
                    (tile[2], turned[2], tile[3], turned[3]),
                    (tile[4], turned[4], tile[6], zero),
                    (tile[5], turned[5], turned[6], zero),
                )
                for q in range(4):
                    slabs = by_field[q] + (zero, zero)
                    for j in range(H):
                        pair = (slabs[2 * j], slabs[2 * j + 1])
                        k = H - 1 - j if x_side == 0 else K0 - H + j
                        put(fields[q], k, rows, dst, *(pair[::-1] if x_side == 0 else pair))
        dst = pl.ds(pl.multiple_of((core if side == 0 else 1 - core) * 128, 128), 128)
        for p in range(4):
            def of_own(i):
                slab, rows, lanes = block_of(i)
                return own[4 * BX + slab, rows, lanes]

            put(mean1, p + H, slice(8, 16), dst, of_own(2 * p), of_own(2 * p + 1))
            for rows, ref, flag in ((slice(0, 8), ylo, has[2]), (slice(16, 24), yhi, has[3])):
                def of_y(i):
                    slab, part, lanes = block_of24(i)
                    return ref[BX + slab, part, lanes] * flag

                put(mean1, p + H, rows, dst, of_y(2 * p), of_y(2 * p + 1))
        for x_side, ref, flag in ((0, xlo, has[0]), (1, xhi, has[1])):
            def of_x(d):
                slab, part, lanes = block_of(5 - d if x_side == 0 else d - 1)
                return ref[18 + slab, part, lanes] * flag

            zero = jnp.zeros((8, 128), F32)
            mids = [of_x(d) for d in (1, 2, 3, 4, 5)] + [zero]
            columns_of = [(slice(8, 16), mids)]
            for rows, cref, yflag in ((slice(0, 8), clo, has[2]), (slice(16, 24), chi, has[3])):
                t = [
                    cref[10 * x_side + 7 + i // 2, :, 128 * (i % 2) : 128 * (i % 2) + 128]
                    * (flag * yflag)
                    for i in range(5)
                ]
                columns_of.append((rows, t + [zero]))
            for rows, slabs in columns_of:
                for j in range(H):
                    pair = (slabs[2 * j], slabs[2 * j + 1])
                    k = H - 1 - j if x_side == 0 else K1 - H + j
                    put(mean1, k, rows, dst, *(pair[::-1] if x_side == 0 else pair))

    def body(k):
        here = pl.ds(k, 1)
        inside = outside((1, Y0, Z0), 16, k, BX // 2, has)
        for c in (0, 1):
            outer[c][here] = jnp.where(inner[c][here] > 0.0, 1.0, 3.0 * inside)

    loop(0, K0, 1, body)
    faces(
        inner, outer, near, fars, ys, zs, diag, inv, (low_near, low_far, low_y, low_z), 1, K0 - 1, SF
    )
    first = first_is_red((SI, Y0, Z0))

    def intra(x, k):
        here = pl.ds(k, SI)
        a = [x[0][here], x[1][here]]
        flow = low_near[here] * (a[1] - a[0])
        total = [flow, -flow]
        for c in (0, 1):
            total[c] = total[c] + low_far[c][here] * (far(x[1 - c], k, SI, c == 0, first) - a[c])
        for axis, low in ((1, low_y), (2, low_z)):
            flows = [low[c][here] * (up(a[1 - c], axis) - a[c]) for c in (0, 1)]
            for c in (0, 1):
                total[c] = total[c] + flows[c] - down(flows[1 - c], axis)
        return total

    def body(k):
        here = pl.ds(k, SI)
        drive = intra(s, k)
        for c in (0, 1):
            w[c][here] = w[c][here] + TIME_STEP * drive[c]

    loop(1, K0 - 1, SI, body)
    lanes = pl.ds(pl.multiple_of(core * 128, 128), BZ)
    half_first = first_is_red((BY, BZ))

    def body(p):
        a, c = w[0][p + H, 8:24, lanes], w[1][p + H, 8:24, lanes]
        mout[2 * p] = jnp.where(half_first, a, c)
        mout[2 * p + 1] = jnp.where(half_first, c, a)

    loop(0, BX // 2, 1, body)
    copies = fetch([(mout, mnext)], sems)

    def body(k):
        here = pl.ds(k, SI)
        both = intra(w, k)
        for c in (0, 1):
            b[c][here] = both[c]

    loop(1, K0 - 1, SI, body)
    coef = (near, fars, ys, zs)
    half_sweep(v, b, 0, coef, inv, 1, K0 - 1, SH)
    half_sweep(v, b, 1, coef, inv, 2, K0 - 2, SHB)
    first = first_is_red((SH, Y0, Z0))

    def body(p):
        here = pl.ds(p + H, SH)
        res = b[0][here] - (diag[here] * v[0][here] - gathered(v, 0, *coef, p + H, SH, first))
        fold[pl.ds(p, SH)] = res[:, 8:24, :]

    loop(0, BX // 2, SH, body)
    half = BX // 2 * BY
    pairs = pair_matrix(Z0, Z1, 0.5, core * 64)
    coarse = sum_rows(fold2, dot(fold[...].reshape(half, Z0), pairs)).reshape(8, 8, Z1)
    red, black = colours(coarse)
    rhs1[0] = red
    rhs1[1] = black
    copies[0].wait()


def middle_faces_kernel(m_in, r_in, *refs):
    inner, refs = refs[0:2], refs[2:]
    rnext, near, fars, ys, zs, diag, inv, outer = (
        refs[0], refs[1], refs[2:4], refs[4:6], refs[6:8], refs[8], refs[9:11], refs[11:13],
    )
    m, r, sems = refs[13:]
    copies = fetch([(m_in, m), (r_in, r)], sems)
    has = flags()
    for k in range(K1):
        inside = outside((Y1, Z1), 8, k, 4, has)
        for c in (0, 1):
            outer[c][k] = jnp.where(inner[c][k] > 0.0, 1.0, 3.0 * inside)
    for copy in copies:
        copy.wait()
    for x in range(BX):
        mm, rr = m[x], r[x]
        r[x] = rr + TIME_STEP * RECOVERY_RATE * (
            -rr - IONIC_GAIN * mm * (mm - IONIC_ONSET - 1.0)
        )
    copies = fetch([(r, rnext)], sems)
    faces(inner, outer, near, fars, ys, zs, diag, inv, None, 1, K1 - 1, S1)
    copies[0].wait()


def join_kernel(low, own, high, wide, xup, xdn):
    for c in (0, 1):
        for p in range(4):
            for i, ref in enumerate((low, own, high)):
                rows = slice(8 * i, 8 * i + 8)
                wide[c, p, rows] = ref[c, p]
                if p < 2:
                    xdn[c, p, rows] = ref[c, p]
                else:
                    xup[c, p - 2, rows] = ref[c, p]


def spread_kernel(got, send):
    whole = got[...]
    for d in range(send.shape[0]):
        send[d] = whole


def middle_kernel(low, own, high, seed, *refs):
    near, fars, ys, zs, diag, inv, refs = (
        refs[0], refs[1:3], refs[3:5], refs[5:7], refs[7], refs[8:10], refs[10:],
    )
    v, b, send, fold, fold2 = refs[0:2], refs[2:4], refs[4], refs[5], refs[6]
    core = lax.axis_index("gz")
    has = flags()
    for c in (0, 1):
        b[c][0:1] = jnp.zeros((1, Y1, Z1), F32)
        b[c][K1 - 1 :] = jnp.zeros((1, Y1, Z1), F32)
        for k in range(1, K1 - 1):
            src = low[c, k - 1] if k < H else (own[c, k - H] if k < H + 4 else high[c, k - H - 4])
            b[c][k] = src * outside((Y1, Z1), 8, k, 4, has)
    coef = (near, fars, ys, zs)
    from_zero(v, b, coef, inv, 1, K1 - 1, S1)
    first = first_is_red((2, Y1, Z1))
    for p in (0, 2):
        here = slice(p + H, p + H + 2)
        res = b[0][here] - (diag[here] * v[0][here] - gathered(v, 0, *coef, p + H, 2, first))
        fold[8 * p : 8 * p + 16] = res[:, 8:16, :].reshape(16, Z1)
    both = sum_rows(fold2, dot(fold[...], pair_matrix(Z1, Z2, 0.5)))
    red, black = colours(both.reshape(4, 4, Z2))
    red, black = red.reshape(8, Z2), black.reshape(8, Z2)
    mine = (iota((8, Z2), 1) < 64) == (core == 0)
    piece = in_order(jnp.where(mine, red, pltpu.roll(black, 64, 1)))
    for d in range(send.shape[0]):
        send[d, 0:8] = piece
        send[d, 8:16] = seed[...]


def in_order(piece):
    odd = (iota(piece.shape, 0) * 0 + lax.axis_index("gy")) & 1
    return jnp.where(odd == 1, pltpu.roll(piece, 4, 0), piece)


def seed_kernel(own, send, fold):
    sums = []
    for p in range(4):
        total = None
        for i in (2 * p, 2 * p + 1):
            slab, rows, lanes = block_of(i)
            block = own[4 * BX + slab, rows, lanes]
            total = block if total is None else total + block
        sums.append(total)
    both = sum_rows(fold, dot(jnp.concatenate(sums, axis=0), pair_matrix(Z2, Z2, 0.125)))
    red, black = colours(both.reshape(4, 4, Z2))
    red, black = red.reshape(8, Z2), black.reshape(8, Z2)
    core = lax.axis_index("gz")
    lane = iota((8, Z2), 1) + core * 0
    lower = jnp.where(lane < 64, red, pltpu.roll(black, 64, 1))
    upper = jnp.where(lane < 64, black, pltpu.roll(red, 64, 1))
    send[...] = in_order(jnp.where(core == 0, lower, upper))


def unpack(got, got_z, part, bufs, nx, ny):
    core = lax.axis_index("gz")
    mine = (iota((8, Z2), 1) < 64) == (core == 0)
    upper = iota((8, Z2), 0) < 4

    def body(start):
      for gx in [start + i for i in range(min(SU, nx))]:
        for t in range(ny // 2):
            d = gx * ny + 2 * t
            tiles = []
            for src in (got, got_z):
                even, odd = src[d, part : part + 8], src[d + 1, part : part + 8]
                tiles.append(
                    (
                        jnp.where(upper, even, odd),
                        pltpu.roll(jnp.where(upper, odd, even), 4, 0),
                    )
                )
            for p in (0, 1):
                a, c = tiles[0][p], tiles[1][p]
                rows = slice(8 * t, 8 * t + 8)
                bufs[0][1 + 2 * gx + p, rows, :] = jnp.where(mine, a, c)
                bufs[1][1 + 2 * gx + p, rows, :] = pltpu.roll(jnp.where(mine, c, a), 64, 1)

    loop(0, nx, min(SU, nx), body)


def coarse_kernel(got, got_z, *refs, nx, ny):
    n2, y2, n3, y3 = 2 * nx, 4 * ny, nx, 2 * ny
    coef2, refs = (refs[0], refs[1:3], refs[3:5], refs[5:7], refs[7], refs[8:10]), refs[10:]
    coef3, refs = (refs[0], refs[1:3], refs[3:5], refs[5:7], None, refs[7:9]), refs[9:]
    in2, out2, in3, out3, fold2, fold1 = (
        refs[0:2], refs[2:4], refs[4:6], refs[6:8], refs[8], refs[9],
    )
    unpack(got, got_z, 8, in2, nx, ny)

    def body(k):
        here = pl.ds(k, 4)
        for c in (0, 1):
            out2[c][here] = jnp.where(in2[c][here] > 0.0, 1.0, 3.0)
        total = 0.25 * (in2[0][here] + in2[1][here])
        fold2[pl.ds(pl.multiple_of((k - 1) * y2, 4 * y2), 4 * y2), :] = total.reshape(4 * y2, Z2)

    loop(1, n2 + 1, 4, body)
    for bufs, count in ((in2, n2), (out2, n2), (in3, n3), (out3, n3)):
        for c in (0, 1):
            bufs[c][0:1] = jnp.zeros_like(bufs[c][0:1])
            bufs[c][count + 1 :] = jnp.zeros_like(bufs[c][0:1])
    faces(in2, out2, *coef2, None, 1, n2 + 1, min(S2, n2))
    restrict(fold2, fold1, in3, n3, y3)
    lane = iota((n3, y3, Z2), 2)
    for c in (0, 1):
        value = jnp.where(in3[c][1 : n3 + 1] > 0.0, 1.0, 3.0)
        out3[c][1 : n3 + 1] = jnp.where(lane < Z2 // 2, value, 0.0)
    faces(in3, out3, *coef3, None, 1, n3 + 1, min(S3, n3))


def restrict(fold2, fold1, bufs, n3, y3):
    rows = 2 * n3 * y3
    sums = fold2[pl.ds(0, rows, 2), :] + fold2[pl.ds(1, rows, 2), :]
    fold1[0, 0:rows, :] = dot(sums, pair_matrix(Z2, Z2, 0.5))
    first = first_is_red((1, y3, Z2))

    def body(p):
        a = fold1[0, pl.ds(pl.multiple_of(2 * p * y3, y3), y3), :][None]
        c = fold1[0, pl.ds(pl.multiple_of((2 * p + 1) * y3, y3), y3), :][None]
        here = pl.ds(p + 1, 1)
        bufs[0][here] = jnp.where(first, a, c)
        bufs[1][here] = jnp.where(first, c, a)

    loop(0, n3, 1, body)


def up_kernel(got, got_z, *refs, nx, ny):
    level1, refs = refs[:13], refs[13:]
    level0, refs = refs[:13], refs[13:]
    coef2, diag2, inv2, refs = (
        (refs[0], refs[1:3], refs[3:5], refs[5:7]), refs[7], refs[8:10], refs[10:],
    )
    coef3, inv3, refs = (refs[0], refs[1:3], refs[3:5], refs[5:7]), refs[7:9], refs[9:]
    out, refs = refs[0], refs[1:]

    def split(r):
        return r[0:2], r[2:4], (r[4], r[5:7], r[7:9], r[9:11]), r[11:13]

    v1, b1, coef1, inv1 = split(level1)
    v0, b0, coef0, inv0 = split(level0)
    n2, y2 = 2 * nx, 4 * ny
    n3, y3 = nx, 2 * ny
    v2, b2, v3, b3 = refs[0:2], refs[2:4], refs[4:6], refs[6:8]
    fold2, fold1, fold0 = refs[8], refs[9], refs[10]
    gx_me, gy_me, core = where_am_i()
    unpack(got, got_z, 0, b2, nx, ny)
    step2 = min(S22, n2)
    from_zero(v2, b2, coef2, inv2, 1, n2 + 1, step2)
    first = first_is_red((step2, y2, Z2))

    def body(k):
        here = pl.ds(k, step2)
        res = b2[0][here] - (diag2[here] * v2[0][here] - gathered(v2, 0, *coef2, k, step2, first))
        start = pl.multiple_of((k - 1) * y2, step2 * y2)
        fold2[pl.ds(start, step2 * y2), :] = res.reshape(step2 * y2, Z2)

    loop(1, n2 + 1, step2, body)
    restrict(fold2, fold1, b3, n3, y3)
    from_zero(v3, b3, coef3, inv3, 1, n3 + 1, n3)

    def sweep(i):
        half_sweep(v3, b3, 0, coef3, inv3, 1, n3 + 1, n3)
        half_sweep(v3, b3, 1, coef3, inv3, 1, n3 + 1, n3)

    loop(0, COARSE_SWEEPS - 1, 1, sweep)
    near2 = min(8, n2)
    base = jnp.clip(2 * gx_me - 2, 0, n2 - near2)
    first3 = first_is_red((y3, Z2))
    for p in range(near2 // 2):
        a, c = v3[0][base // 2 + p + 1], v3[1][base // 2 + p + 1]
        fold2[2 * p * y3 : (2 * p + 1) * y3, :] = jnp.where(first3, a, c)
        fold2[(2 * p + 1) * y3 : (2 * p + 2) * y3, :] = jnp.where(first3, c, a)
    twice_rows(fold1, dot(fold2[0 : near2 * y3, :], copy_matrix(Z2, Z2)))
    for k in range(0, near2, 4):
        e = fold1[0, k * y2 : (k + 4) * y2, :].reshape(4, y2, Z2)
        here = pl.ds(base + 1 + k, 4)
        for c in (0, 1):
            v2[c][here] = v2[c][here] + e
    half_sweep(v2, b2, 0, coef2, inv2, base + 1, base + 1 + near2, near2)
    half_sweep(v2, b2, 1, coef2, inv2, base + 1, base + 1 + near2, near2)
    shift = lax.rem(4 - 4 * gy_me + 2 * y2, y2)
    first1 = first_is_red((y2, Z2))
    cells = []
    for j in range(4):
        a, c = v2[0][2 * gx_me + j], v2[1][2 * gx_me + j]
        for cell in (jnp.where(first1, a, c), jnp.where(first1, c, a)):
            cells.append(pltpu.roll(cell, shift, 0)[0:16])
    twice_rows(fold1, dot(jnp.concatenate(cells, axis=0), copy_matrix(Z2, Z1)))
    for k in range(1, K1 - 1):
        e = columns(fold1, 32 * (k - 1), Y1, Z1)
        for c in (0, 1):
            v1[c][k] = jnp.where(inv1[c][k] > 0.0, v1[c][k] + e, 0.0)
    half_sweep(v1, b1, 0, coef1, inv1, 1, K1 - 1, S1)
    half_sweep(v1, b1, 1, coef1, inv1, 1, K1 - 1, S1)
    first0 = first_is_red((Y1, Z1))
    cells = []
    for k in range(H - 1, K1 - H + 1):
        a, c = v1[0][k], v1[1][k]
        cells += [jnp.where(first0, a, c), jnp.where(first0, c, a)]
    cells = [cell[4:20] for cell in cells[1:-1]]
    twice_rows(fold0, dot(jnp.concatenate(cells, axis=0), copy_matrix(Z1, Z0, core * 64)))

    def body(p):
        e = columns(fold0, pl.multiple_of(p * 32, 32), 32, Z0)[None]
        here = pl.ds(p + H - 1, 1)
        for c in (0, 1):
            v0[c][here] = jnp.where(inv0[c][here] > 0.0, v0[c][here] + e, 0.0)

    loop(0, BX // 2 + 2, 1, body)
    half_sweep(v0, b0, 0, coef0, inv0, H - 1, K0 - H + 1, SHB)
    half_sweep(v0, b0, 1, coef0, inv0, H, K0 - H, SH)
    lanes = pl.ds(pl.multiple_of(core * 128, 128), BZ)
    half_first = first_is_red((BY, BZ))

    def body(p):
        a, c = v0[0][p + H, 8:24, lanes], v0[1][p + H, 8:24, lanes]
        out[2 * p] = jnp.where(half_first, a, c)
        out[2 * p + 1] = jnp.where(half_first, c, a)

    loop(0, BX // 2, 1, body)


def shape(*dims):
    return jax.ShapeDtypeStruct(dims, F32)


def scratch(*dims):
    return pltpu.VMEM(dims, F32)


def ring(x, axis, step):
    n = lax.axis_size(axis)
    return lax.ppermute(x, axis, [(i, (i + step) % n) for i in range(n)])


def swap(x):
    return lax.ppermute(x, "gz", [(0, 1), (1, 0)])


def gather(send, nx, ny):
    got = lax.all_to_all(send, "gy", 0, 0, tiled=True)
    (send,) = call(spread_kernel, "spread", 4, [(nx,) + got.shape], [], got)
    return lax.all_to_all(send, "gx", 0, 0, tiled=True).reshape((nx * ny,) + got.shape[1:])


def call(kernel, name, mib, outs, scratches, *args, hbm_in=0, hbm_out=0):
    return pl.pallas_call(
        kernel,
        out_shape=tuple(shape(*o) for o in outs),
        in_specs=[HBM] * hbm_in + [VMEM] * (len(args) - hbm_in),
        out_specs=(HBM,) * hbm_out + (VMEM,) * (len(outs) - hbm_out),
        scratch_shapes=[scratch(*s) if isinstance(s, tuple) else s for s in scratches],
        compiler_params=params(mib),
        name=name,
    )(*args)


def on_device(membrane, recovery, extracellular, fiber_scale, labels):
    nx, ny = lax.axis_size("gx"), lax.axis_size("gy")
    block = (BX, BY, BZ)
    held = [
        pltpu.with_memory_space_constraint(x, pltpu.HBM)
        for x in (membrane, recovery, extracellular, fiber_scale, labels)
    ]
    own, xup, xdn, yup, ydn = call(
        prep_kernel, "prep", 6,
        [(4 * BX + 2, BY, BZ)] + [(20, BY, BZ)] * 2 + [(BX + 2, 24, BZ)] * 2,
        [block] * 4
        + [pltpu.VMEM(labels.shape, jnp.int32), (1, 128, 128), pltpu.SemaphoreType.DMA((5,))],
        *held, hbm_in=5,
    )
    xlo, xhi = ring(xup, "gx", 1), ring(xdn, "gx", -1)
    ylo, yhi = ring(yup, "gy", 1), ring(ydn, "gy", -1)
    cup, cdn = call(corner_kernel, "corner", 4, [(20, 8, BZ)] * 2, [], xlo, xhi)
    clo, chi = ring(cup, "gy", 1), ring(cdn, "gy", -1)
    halos = []
    for piece in (own, xlo, xhi, ylo, yhi, clo, chi):
        halos += [piece, swap(piece)]
    (seed,) = call(seed_kernel, "seed", 4, [(8, Z2)], [(1, 32, 128)], own)
    fine = (K0, Y0, Z0)
    mid = (K1, Y1, Z1)
    grid2, grid3 = (2 * nx + 2, 4 * ny, Z2), (nx + 2, 2 * ny, Z2)
    mnext, rhs1, in1r, in1b, *level0 = call(
        fine_kernel, "fine", 20,
        [block, (2, 4, 8, Z1)] + [mid] * 2 + [fine] * 13,
        [fine] * 16
        + [(8, BY, Z0), (2, 128, 128), block, pltpu.SemaphoreType.DMA((1,))],
        *halos, hbm_out=1,
    )
    rnext, *coef1 = call(
        middle_faces_kernel, "middle_faces", 4, [block] + [mid] * 10,
        [mid] * 2 + [block] * 2 + [pltpu.SemaphoreType.DMA((2,))],
        held[0], held[1], in1r, in1b, hbm_in=2, hbm_out=1,
    )
    part = (2, 2, Y1, Z1)
    wide, xup, xdn = call(
        join_kernel, "join", 4, [(2, 4, Y1, Z1), part, part], [],
        ring(rhs1, "gy", 1), rhs1, ring(rhs1, "gy", -1),
    )
    low, high = ring(xup, "gx", 1), ring(xdn, "gx", -1)
    v1r, v1b, b1r, b1b, send = call(
        middle_kernel, "middle", 4,
        [mid] * 4 + [(ny, 16, Z2)],
        [(32, Z1), (1, 32, 128)],
        low, wide, high, seed, *coef1,
    )
    got = gather(send, nx, ny)
    got_z = swap(got)
    coarse = call(
        lambda *refs: coarse_kernel(*refs, nx=nx, ny=ny), "coarse", 8,
        [grid2] * 10 + [grid3] * 9,
        [grid2] * 4 + [grid3] * 4 + [(8 * nx * ny, Z2), (1, 4 * nx * ny, Z2)],
        got, got_z,
    )
    level1 = [v1r, v1b, b1r, b1b, *coef1[:7], *coef1[8:]]
    (enext,) = call(
        lambda *refs: up_kernel(*refs, nx=nx, ny=ny), "up", 10,
        [block],
        [grid2] * 4 + [grid3] * 4
        + [(8 * nx * ny, Z2), (2, max(4 * nx * ny, 256), Z2), (3, 320, 128)],
        got, got_z, *level1, *level0, *coarse,
    )
    return mnext, rnext, enext


def solution(mesh):
    spec = P("gx", "gy", "gz")
    return jax.shard_map(
        on_device, mesh=mesh, in_specs=(spec,) * 5, out_specs=(spec,) * 3, check_vma=False
    )
```

```python
import jax
import jax.numpy as jnp
from jax import lax
from jax.experimental import pallas as pl
from jax.experimental.pallas import tpu as pltpu
from jax.sharding import PartitionSpec as P

TIME_STEP = 0.05
IONIC_GAIN = 8.0
IONIC_ONSET = 0.15
RECOVERY_RATE = 0.01
COARSE_SWEEPS = 8

F32 = jnp.float32
BX, BY, BZ = 16, 16, 256
H = 3
SF, SI, SH, SHB, S1, S2, SU, S22, S3 = 3, 4, 4, 5, 8, 8, 8, 16, 16
AT_IN, AT_W, AT_U, AT_MEAN = BX, 2 * BX, 3 * BX, 3 * BX + BX // 2
K0, Y0, Z0 = BX // 2 + 2 * H, 32, 384
K1, Y1, Z1 = BX // 4 + 2 * H, 24, BZ
Z2 = BZ // 2
VMEM = pl.BlockSpec(memory_space=pltpu.VMEM)
HBM = pl.BlockSpec(memory_space=pltpu.HBM)


def params(mib):
    return pltpu.CompilerParams(vmem_limit_bytes=mib * 1024 * 1024)


def iota(shape, dim):
    return lax.broadcasted_iota(jnp.int32, shape, dim)


def first_is_red(shape):
    return ((iota(shape, len(shape) - 2) + iota(shape, len(shape) - 1)) & 1) == 0


def up(x, axis):
    return pltpu.roll(x, x.shape[axis] - 1, axis)


def down(x, axis):
    return pltpu.roll(x, 1, axis)


def pair_matrix(rows, cols, value, shift=0):
    return jnp.where(
        iota((rows, cols), 0) // 2 + shift == iota((rows, cols), 1), value, 0.0
    ).astype(F32)


def copy_matrix(rows, cols, shift=0):
    return jnp.where(
        iota((rows, cols), 1) // 2 + shift == iota((rows, cols), 0), 1.0, 0.0
    ).astype(F32)


def dot(a, b):
    b = b.astype(jnp.bfloat16)
    high = a.astype(jnp.bfloat16)
    rest = a - high.astype(F32)
    mid = rest.astype(jnp.bfloat16)
    low = (rest - mid.astype(F32)).astype(jnp.bfloat16)
    parts = [jnp.dot(p, b, preferred_element_type=F32) for p in (low, mid, high)]
    return parts[0] + parts[1] + parts[2]


def sum_rows(buf, x):
    rows, cols = x.shape
    sums = []
    for c in range(cols // 128):
        buf[c, 0:rows, :] = x[:, 128 * c : 128 * c + 128]
        sums.append(buf[c, pl.ds(0, rows // 2, 2), :] + buf[c, pl.ds(1, rows // 2, 2), :])
    return sums[0] if len(sums) == 1 else jnp.concatenate(sums, axis=1)


def twice_rows(buf, x):
    rows, cols = x.shape
    for c in range(cols // 128):
        for k in (0, 1):
            buf[c, pl.ds(k, rows, 2), :] = x[:, 128 * c : 128 * c + 128]


def columns(buf, start, rows, cols):
    parts = [buf[c, pl.ds(start, rows), :] for c in range(cols // 128)]
    return parts[0] if len(parts) == 1 else jnp.concatenate(parts, axis=1)


def loop(start, stop, step, body):
    if not isinstance(start, int) or stop - start == step:
        body(start)
        return

    def run(index, carry):
        body(start + index * step)
        return carry

    lax.fori_loop(0, (stop - start) // step, run, 0)


def far(other, k, step, red, first):
    before, after = other[pl.ds(k - 1, step)], other[pl.ds(k + 1, step)]
    return jnp.where(first, before, after) if red else jnp.where(first, after, before)


def faces(inner, outer, near, fars, ys, zs, diag, inv, least, start, stop, step):
    rows, lanes = inner[0].shape[1:]
    shape = (step, rows, lanes)
    row, lane = iota(shape, 1), iota(shape, 2)
    first = first_is_red(shape)

    def body(k):
        here = pl.ds(k, step)
        low = jnp.minimum(inner[0][here], inner[1][here])
        if least is not None:
            least[0][here] = low
        halves = [0.5 * outer[c][here] for c in (0, 1)]
        pair = low + halves[0] + halves[1]
        near[here] = pair
        totals = [pair, pair]
        for axis, out, keep, place, size in (
            (1, ys, None if least is None else least[2], row, rows),
            (2, zs, None if least is None else least[3], lane, lanes),
        ):
            full = []
            for c in (0, 1):
                o = 1 - c
                mine = inner[c][here]
                low = jnp.where(place < size - 1, jnp.minimum(mine, up(inner[o][here], axis)), 0.0)
                if keep is not None:
                    keep[c][here] = low
                both = low + halves[c] + jnp.where(place < size - 1, up(halves[o], axis), 0.0)
                full.append(both)
                out[c][here] = jnp.where(place < size - 1, both, 0.0)
            for c in (0, 1):
                below = jnp.where(place > 0, down(full[1 - c], axis), halves[c])
                totals[c] = totals[c] + full[c] + below
        for c in (0, 1):
            o = 1 - c
            low = jnp.minimum(inner[c][here], far(inner[o], k, step, c == 0, first))
            if least is not None:
                least[1][c][here] = low
            both = low + halves[c] + 0.5 * far(outer[o], k, step, c == 0, first)
            fars[c][here] = both
            total = totals[c] + both
            if c == 0 and diag is not None:
                diag[here] = total
            inside = outer[c][here] > 0.0
            inv[c][here] = jnp.where(inside, 1.0 / jnp.where(inside, total, 1.0), 0.0)

    loop(start, stop, step, body)


def gathered(v, c, near, fars, ys, zs, k, step, first):
    here = pl.ds(k, step)
    o = 1 - c
    other = v[o][here]
    total = near[here] * other + fars[c][here] * far(v[o], k, step, c == 0, first)
    total = total + ys[c][here] * up(other, 1) + down(ys[o][here] * other, 1)
    return total + zs[c][here] * up(other, 2) + down(zs[o][here] * other, 2)


def half_sweep(v, b, c, coef, inv, start, stop, step):
    first = first_is_red((step,) + tuple(v[0].shape[1:]))

    def body(k):
        here = pl.ds(k, step)
        v[c][here] = (b[c][here] + gathered(v, c, *coef, k, step, first)) * inv[c][here]

    loop(start, stop, step, body)


def from_zero(v, b, coef, inv, start, stop, step):
    count = v[0].shape[0]
    for c in (0, 1):
        v[c][0:1] = jnp.zeros_like(v[c][0:1])
        v[c][count - 1 :] = jnp.zeros_like(v[c][0:1])

    def body(k):
        here = pl.ds(k, step)
        v[0][here] = b[0][here] * inv[0][here]

    loop(start, stop, step, body)
    half_sweep(v, b, 1, coef, inv, start, stop, step)


def put(bufs, k, rows, lanes, a, b):
    some = a if b is None else b
    a = jnp.zeros_like(some) if a is None else a
    b = jnp.zeros_like(some) if b is None else b
    first = first_is_red(some.shape)
    bufs[0][k, rows, lanes] = jnp.where(first, a, b)
    bufs[1][k, rows, lanes] = jnp.where(first, b, a)


def colours(x):
    n = x.shape[0] // 2
    first = first_is_red(x.shape[1:])
    pairs = [(x[2 * p], x[2 * p + 1]) for p in range(n)]
    return (
        jnp.stack([jnp.where(first, a, b) for a, b in pairs]),
        jnp.stack([jnp.where(first, b, a) for a, b in pairs]),
    )


def where_am_i():
    return lax.axis_index("gx"), lax.axis_index("gy"), lax.axis_index("gz")


def flags():
    gx, gy, _ = where_am_i()
    return (
        (gx > 0).astype(F32),
        (gx < lax.axis_size("gx") - 1).astype(F32),
        (gy > 0).astype(F32),
        (gy < lax.axis_size("gy") - 1).astype(F32),
    )


def fetch(pairs, sems):
    copies = [pltpu.make_async_copy(src, dst, sems.at[i]) for i, (src, dst) in enumerate(pairs)]
    for copy in copies:
        copy.start()
    return copies


def outside(shape, own_rows, k, own, has):
    row = iota(shape, len(shape) - 2)
    in_y = jnp.where(row < 8, has[2], jnp.where(row < 8 + own_rows, 1.0, has[3]))
    return in_y * jnp.where(k < H, has[0], jnp.where(k < H + own, 1.0, has[1]))


def block_of(i):
    rows, lanes = 8 * ((i % 4) // 2), 128 * (i % 2)
    return i // 4, slice(rows, rows + 8), slice(lanes, lanes + 128)


def prep_kernel(
    m_in, r_in, u_in, f_in, labels_in, own, xup, xdn, yup, ydn, m, r, u, f, labels, fold, sems
):
    copies = fetch(
        [(labels_in, labels), (m_in, m), (u_in, u), (r_in, r), (f_in, f)], sems
    )
    for copy in copies:
        copy.wait()
    spread = jnp.where(iota((BZ // 8, BZ), 1) // 8 == iota((BZ // 8, BZ), 0), 1.0, 0.0).astype(F32)
    for bx in range(BX // 8):
        wide = jnp.dot(labels[bx].astype(F32), spread, preferred_element_type=F32)
        kind = jnp.concatenate(
            [jnp.broadcast_to(wide[by : by + 1], (8, BZ)) for by in range(BY // 8)], axis=0
        )
        factor = jnp.where(kind > 1.5, 0.3, jnp.where(kind > 0.5, 1.0, 0.0)).astype(F32)
        for x in range(8 * bx, 8 * bx + 8):
            mm, rr, uu = m[x], r[x], u[x]
            inner = factor * f[x]
            own[x] = mm + uu
            own[AT_IN + x] = inner
            ionic = IONIC_GAIN * mm * (mm - IONIC_ONSET) * (mm - 1.0) + mm * rr
            own[AT_W + x] = mm - jnp.where(kind > 0.5, TIME_STEP * ionic, 0.0)
            if x % 2:
                first = first_is_red((BY, BZ))
                own[AT_U + x // 2] = jnp.where(first, uu, u[x - 1])
    sums = jnp.concatenate(
        [own[AT_IN + 2 * p] + own[AT_IN + 2 * p + 1] for p in range(BX // 2)], axis=0
    )
    mean = sum_rows(fold, dot(sums, pair_matrix(BZ, BZ // 2, 0.125)))
    for i in range(8):
        slab, rows, lanes = block_of(i)
        for ref, base in ((own, AT_MEAN), (yup, BX), (ydn, BX)):
            ref[base + slab, rows, lanes] = mean[8 * i : 8 * i + 8]
    for i in range(5):
        slab, rows, lanes = block_of(i)
        xup[16 + slab, rows, lanes] = mean[8 * (3 + i) : 8 * (4 + i)]
        xdn[16 + slab, rows, lanes] = mean[8 * i : 8 * i + 8]
    base = 0
    for start, count, depth in ((0, BX, 5), (AT_IN, BX, 5), (AT_W, BX, 4), (AT_U, BX // 2, 2)):
        xup[base : base + depth] = own[start + count - depth : start + count]
        xdn[base : base + depth] = own[start : start + depth]
        base += depth
    row = iota((8, BZ), 0)
    turn = lambda x, by: pltpu.roll(x, by % 8, 0)
    for p in range(BX // 2):
        for out, rows, keep, by, fourth in (
            (yup, slice(8, 16), row >= 3, 3, (4, 5, 6)),
            (ydn, slice(0, 8), row < 5, 5, (2, 3, 4)),
        ):
            s = [own[2 * p + i, rows] for i in (0, 1)]
            n = [own[AT_IN + 2 * p + i, rows] for i in (0, 1)]
            rest = [own[AT_W + 2 * p, rows], own[AT_W + 2 * p + 1, rows], own[AT_U + p, rows]]
            at = 0 if out is yup else 5
            last = jnp.where(
                row == at,
                turn(rest[0], fourth[0]),
                jnp.where(row == at + 1, turn(rest[1], fourth[1]), turn(rest[2], fourth[2])),
            )
            out[2 * p, 0:8] = jnp.where(keep, s[0], turn(rest[0], by))
            out[2 * p, 8:16] = jnp.where(keep, s[1], turn(rest[1], by))
            out[2 * p + 1, 0:8] = jnp.where(keep, n[0], turn(rest[2], by))
            out[2 * p + 1, 8:16] = jnp.where(keep, n[1], last)


def merge(high, a, b):
    row = iota(a.shape, 0)
    return jnp.where(row >= 4, a, pltpu.roll(b, 4, 0)) if high else jnp.where(
        row < 4, a, pltpu.roll(b, 4, 0)
    )


def corner_kernel(xlo, xhi, cup, cdn):
    for high, out in ((True, cup), (False, cdn)):
        rows = slice(8, 16) if high else slice(0, 8)
        for side, src in ((0, xlo), (1, xhi)):
            at = lambda base, depth, d: src[base + (depth - d if side == 0 else d - 1), rows]
            s, n, w = (
                lambda d: at(0, 5, d),
                lambda d: at(5, 5, d),
                lambda d: at(10, 4, d),
            )
            u = lambda d: at(14, 2, d)
            tiles = [
                merge(high, s(1), s(2)),
                merge(high, s(3), s(4)),
                merge(high, n(1), n(2)),
                merge(high, n(3), n(4)),
                merge(high, w(1), w(2)),
                merge(high, w(3), u(1)),
                u(2),
            ]
            for t, tile in enumerate(tiles):
                out[10 * side + t] = tile

            def coarse(d):
                slab, block_rows, lanes = block_of(5 - d if side == 0 else d - 1)
                return src[16 + slab, block_rows, lanes]

            for d in range(1, 6):
                tile, lanes = 10 * side + 7 + (d - 1) // 2, 128 * ((d - 1) % 2)
                out[tile, :, lanes : lanes + 128] = coarse(d)


def fine_kernel(*refs):
    pieces, refs = refs[:14], refs[14:]
    mnext, rhs1, rup, rdn, refs = refs[0], refs[1], refs[2], refs[3], refs[4:]
    mean1, refs = refs[0:2], refs[2:]
    v, b, near, fars, ys, zs, inv, refs = (
        refs[0:2], refs[2:4], refs[4], refs[5:7], refs[7:9], refs[9:11], refs[11:13], refs[13:],
    )
    inner, outer, s, w, refs = refs[0:2], refs[2:4], refs[4:6], refs[6:8], refs[8:]
    low_near, low_far, low_y, low_z, diag, fold, fold2 = (
        refs[0], refs[1:3], refs[3:5], refs[5:7], refs[7], refs[8], refs[9],
    )
    mout, sems = refs[10], refs[11]
    core = lax.axis_index("gz")
    has = flags()
    fields = (s, inner, w)
    for side in (0, 1):
        own, xlo, xhi, ylo, yhi, clo, chi = pieces[side::2]
        wide = BZ if side == 0 else 128
        src = pl.ds(0 if side == 0 else pl.multiple_of(core * 128, 128), wide)
        dst = pl.ds(pl.multiple_of(core * 128 if side == 0 else (1 - core) * 256, 128), wide)
        mid, low, high = slice(8, 24), slice(0, 8), slice(24, 32)

        def body(p, own=own, ylo=ylo, yhi=yhi, src=src, dst=dst):
            k = p + H
            for q, bufs in enumerate(fields):
                put(bufs, k, mid, dst, own[BX * q + 2 * p, :, src], own[BX * q + 2 * p + 1, :, src])
            v[1][k, mid, dst] = own[AT_U + p, :, src]
            row = iota((8, wide), 0)
            turn = lambda x, by: pltpu.roll(x, by, 0)
            for rows, ref, flag, keep, deep, by, fourth in (
                (low, ylo, has[2], row >= 3, row >= 5, 5, (4, 3, 2)),
                (high, yhi, has[3], row < 5, row < 3, 3, (6, 5, 4)),
            ):
                t = [
                    ref[2 * p + i // 2, 8 * (i % 2) : 8 * (i % 2) + 8, src] * flag for i in range(4)
                ]
                put(s, k, rows, dst, t[0], t[1])
                put(inner, k, rows, dst, jnp.where(keep, t[2], 0.0), jnp.where(keep, t[3], 0.0))
                rest = [
                    jnp.where(deep, turn(t[i], by), turn(t[3], fourth[i])) for i in (0, 1, 2)
                ]
                put(w, k, rows, dst, rest[0], rest[1])
                v[1][k, rows, dst] = rest[2]

        loop(0, BX // 2, 1, body)
        for x_side, ref, flag in ((0, xlo, has[0]), (1, xhi, has[1])):
            base = 0
            order = (5, 4, 3, 2, 1) if x_side == 0 else (1, 2, 3, 4, 5)
            for q, depth in enumerate((5, 5, 4)):
                slabs = {d: ref[base + i, :, src] * flag for i, d in enumerate(
                    [d for d in order if d <= depth])}
                base += depth
                for j in range(H):
                    near_d, far_d = 2 * j + 1, 2 * j + 2
                    pair = (slabs.get(near_d), slabs.get(far_d))
                    k = H - 1 - j if x_side == 0 else K0 - H + j
                    if x_side == 0:
                        pair = pair[::-1]
                    if pair[0] is None and pair[1] is None:
                        pair = (jnp.zeros((16, wide), F32), None)
                    put(fields[q], k, mid, dst, *pair)
            black = [ref[14, :, src] * flag, ref[15, :, src] * flag, jnp.zeros((16, wide), F32)]
            if x_side == 0:
                black[0], black[1] = black[1], black[0]
            for j in range(H):
                v[1][H - 1 - j if x_side == 0 else K0 - H + j, mid, dst] = black[j]
            for rows, cref, yflag in ((low, clo, has[2]), (high, chi, has[3])):
                both = flag * yflag
                tile = [cref[10 * x_side + t, :, src] * both for t in range(7)]
                turned = [pltpu.roll(t, 4, 0) for t in tile]
                zero = jnp.zeros((8, wide), F32)
                by_field = (
                    (tile[0], turned[0], tile[1], turned[1]),
                    (tile[2], turned[2], tile[3], turned[3]),
                    (tile[4], turned[4], tile[5], zero),
                )
                black = (turned[5], tile[6], zero)
                for j in range(H):
                    v[1][H - 1 - j if x_side == 0 else K0 - H + j, rows, dst] = black[j]
                for q in range(3):
                    slabs = by_field[q] + (zero, zero)
                    for j in range(H):
                        pair = (slabs[2 * j], slabs[2 * j + 1])
                        k = H - 1 - j if x_side == 0 else K0 - H + j
                        put(fields[q], k, rows, dst, *(pair[::-1] if x_side == 0 else pair))
        dst = pl.ds(pl.multiple_of((core if side == 0 else 1 - core) * 128, 128), 128)
        for p in range(4):
            def of_own(i):
                slab, rows, lanes = block_of(i)
                return own[AT_MEAN + slab, rows, lanes]

            put(mean1, p + H, slice(8, 16), dst, of_own(2 * p), of_own(2 * p + 1))
            for rows, ref, flag in ((slice(0, 8), ylo, has[2]), (slice(16, 24), yhi, has[3])):
                def of_y(i):
                    slab, part, lanes = block_of(i)
                    return ref[BX + slab, part, lanes] * flag

                put(mean1, p + H, rows, dst, of_y(2 * p), of_y(2 * p + 1))
        for x_side, ref, flag in ((0, xlo, has[0]), (1, xhi, has[1])):
            def of_x(d):
                slab, part, lanes = block_of(5 - d if x_side == 0 else d - 1)
                return ref[16 + slab, part, lanes] * flag

            zero = jnp.zeros((8, 128), F32)
            mids = [of_x(d) for d in (1, 2, 3, 4, 5)] + [zero]
            columns_of = [(slice(8, 16), mids)]
            for rows, cref, yflag in ((slice(0, 8), clo, has[2]), (slice(16, 24), chi, has[3])):
                t = [
                    cref[10 * x_side + 7 + i // 2, :, 128 * (i % 2) : 128 * (i % 2) + 128]
                    * (flag * yflag)
                    for i in range(5)
                ]
                columns_of.append((rows, t + [zero]))
            for rows, slabs in columns_of:
                for j in range(H):
                    pair = (slabs[2 * j], slabs[2 * j + 1])
                    k = H - 1 - j if x_side == 0 else K1 - H + j
                    put(mean1, k, rows, dst, *(pair[::-1] if x_side == 0 else pair))

    def body(k):
        here = pl.ds(k, 1)
        inside = outside((1, Y0, Z0), 16, k, BX // 2, has)
        for c in (0, 1):
            outer[c][here] = jnp.where(inner[c][here] > 0.0, 1.0, 3.0 * inside)

    loop(0, K0, 1, body)
    faces(
        inner, outer, near, fars, ys, zs, diag, inv, (low_near, low_far, low_y, low_z), 1, K0 - 1, SF
    )
    first = first_is_red((SI, Y0, Z0))

    def intra(x, k):
        here = pl.ds(k, SI)
        a = [x[0][here], x[1][here]]
        flow = low_near[here] * (a[1] - a[0])
        total = [flow, -flow]
        for c in (0, 1):
            total[c] = total[c] + low_far[c][here] * (far(x[1 - c], k, SI, c == 0, first) - a[c])
        for axis, low in ((1, low_y), (2, low_z)):
            flows = [low[c][here] * (up(a[1 - c], axis) - a[c]) for c in (0, 1)]
            for c in (0, 1):
                total[c] = total[c] + flows[c] - down(flows[1 - c], axis)
        return total

    def body(k):
        here = pl.ds(k, SI)
        drive = intra(s, k)
        for c in (0, 1):
            w[c][here] = w[c][here] + TIME_STEP * drive[c]

    loop(1, K0 - 1, SI, body)
    lanes = pl.ds(pl.multiple_of(core * 128, 128), BZ)
    half_first = first_is_red((BY, BZ))

    def body(p):
        a, c = w[0][p + H, 8:24, lanes], w[1][p + H, 8:24, lanes]
        mout[2 * p] = jnp.where(half_first, a, c)
        mout[2 * p + 1] = jnp.where(half_first, c, a)

    loop(0, BX // 2, 1, body)
    copies = fetch([(mout, mnext)], sems)

    def body(k):
        here = pl.ds(k, SI)
        both = intra(w, k)
        for c in (0, 1):
            b[c][here] = both[c]

    loop(1, K0 - 1, SI, body)
    coef = (near, fars, ys, zs)
    half_sweep(v, b, 0, coef, inv, 1, K0 - 1, SH)
    half_sweep(v, b, 1, coef, inv, 2, K0 - 2, SHB)
    first = first_is_red((SH, Y0, Z0))

    def body(p):
        here = pl.ds(p + H, SH)
        res = b[0][here] - (diag[here] * v[0][here] - gathered(v, 0, *coef, p + H, SH, first))
        fold[pl.ds(p, SH)] = res[:, 8:24, :]

    loop(0, BX // 2, SH, body)
    half = BX // 2 * BY
    pairs = pair_matrix(Z0, Z1, 0.5, core * 64)
    coarse = sum_rows(fold2, dot(fold[...].reshape(half, Z0), pairs)).reshape(8, 8, Z1)
    red, black = colours(coarse)
    for c, pairs in ((0, red), (1, black)):
        rhs1[c] = pairs
        for j in (0, 1):
            rup[c, j] = merge(True, pairs[2 * j], pairs[2 * j + 1])
            rdn[c, j] = merge(False, pairs[2 * j], pairs[2 * j + 1])
    copies[0].wait()


def middle_faces_kernel(m_in, r_in, *refs):
    inner, refs = refs[0:2], refs[2:]
    rnext, near, fars, ys, zs, diag, inv, outer = (
        refs[0], refs[1], refs[2:4], refs[4:6], refs[6:8], refs[8], refs[9:11], refs[11:13],
    )
    m, r, sems = refs[13:]
    copies = fetch([(m_in, m), (r_in, r)], sems)
    has = flags()
    for k in range(K1):
        inside = outside((Y1, Z1), 8, k, 4, has)
        for c in (0, 1):
            outer[c][k] = jnp.where(inner[c][k] > 0.0, 1.0, 3.0 * inside)
    for copy in copies:
        copy.wait()
    for x in range(BX):
        mm, rr = m[x], r[x]
        r[x] = rr + TIME_STEP * RECOVERY_RATE * (
            -rr - IONIC_GAIN * mm * (mm - IONIC_ONSET - 1.0)
        )
    copies = fetch([(r, rnext)], sems)
    faces(inner, outer, near, fars, ys, zs, diag, inv, None, 1, K1 - 1, S1)
    copies[0].wait()


def join_kernel(low, own, high, wide, xup, xdn):
    row = iota((8, Z1), 0)
    for c in (0, 1):
        for p in range(4):
            a, b = low[c, p // 2], high[c, p // 2]
            edge = jnp.where(row >= 4, a, b) if p % 2 == 0 else pltpu.roll(
                jnp.where(row < 4, a, b), 4, 0
            )
            for ref, q in ((wide, p), (xdn, p) if p < 2 else (xup, p - 2)):
                ref[c, q, 0:8] = edge
                ref[c, q, 8:16] = own[c, p]


def spread_kernel(got, send):
    whole = got[...]
    for d in range(send.shape[0]):
        send[d] = whole


def middle_kernel(low, own, high, seed, *refs):
    near, fars, ys, zs, diag, inv, refs = (
        refs[0], refs[1:3], refs[3:5], refs[5:7], refs[7], refs[8:10], refs[10:],
    )
    v, b, send, fold, fold2 = refs[0:2], refs[2:4], refs[4], refs[5], refs[6]
    core = lax.axis_index("gz")
    has = flags()
    for c in (0, 1):
        b[c][0:1] = jnp.zeros((1, Y1, Z1), F32)
        b[c][K1 - 1 :] = jnp.zeros((1, Y1, Z1), F32)
        for k in range(1, K1 - 1):
            src = low[c, k - 1] if k < H else (own[c, k - H] if k < H + 4 else high[c, k - H - 4])
            inside = outside((Y1, Z1), 8, k, 4, has)
            for rows, part in ((slice(0, 8), src[0:8]), (slice(8, 16), src[8:16]), (slice(16, 24), src[0:8])):
                b[c][k, rows] = part * inside[rows]
    coef = (near, fars, ys, zs)
    from_zero(v, b, coef, inv, 1, K1 - 1, S1)
    first = first_is_red((2, Y1, Z1))
    for p in (0, 2):
        here = slice(p + H, p + H + 2)
        res = b[0][here] - (diag[here] * v[0][here] - gathered(v, 0, *coef, p + H, 2, first))
        fold[8 * p : 8 * p + 16] = res[:, 8:16, :].reshape(16, Z1)
    both = sum_rows(fold2, dot(fold[...], pair_matrix(Z1, Z2, 0.5)))
    red, black = colours(both.reshape(4, 4, Z2))
    red, black = red.reshape(8, Z2), black.reshape(8, Z2)
    mine = (iota((8, Z2), 1) < 64) == (core == 0)
    piece = in_order(jnp.where(mine, red, pltpu.roll(black, 64, 1)))
    for d in range(send.shape[0]):
        send[d, 0:8] = piece
        send[d, 8:16] = seed[...]


def in_order(piece):
    odd = (iota(piece.shape, 0) * 0 + lax.axis_index("gy")) & 1
    return jnp.where(odd == 1, pltpu.roll(piece, 4, 0), piece)


def seed_kernel(own, send, fold):
    sums = []
    for p in range(4):
        total = None
        for i in (2 * p, 2 * p + 1):
            slab, rows, lanes = block_of(i)
            block = own[AT_MEAN + slab, rows, lanes]
            total = block if total is None else total + block
        sums.append(total)
    both = sum_rows(fold, dot(jnp.concatenate(sums, axis=0), pair_matrix(Z2, Z2, 0.125)))
    red, black = colours(both.reshape(4, 4, Z2))
    red, black = red.reshape(8, Z2), black.reshape(8, Z2)
    core = lax.axis_index("gz")
    lane = iota((8, Z2), 1) + core * 0
    lower = jnp.where(lane < 64, red, pltpu.roll(black, 64, 1))
    upper = jnp.where(lane < 64, black, pltpu.roll(red, 64, 1))
    send[...] = in_order(jnp.where(core == 0, lower, upper))


def unpack(got, got_z, part, bufs, nx, ny):
    core = lax.axis_index("gz")
    mine = (iota((8, Z2), 1) < 64) == (core == 0)
    upper = iota((8, Z2), 0) < 4

    def body(start):
      for gx in [start + i for i in range(min(SU, nx))]:
        for t in range(ny // 2):
            d = gx * ny + 2 * t
            tiles = []
            for src in (got, got_z):
                even, odd = src[d, part : part + 8], src[d + 1, part : part + 8]
                tiles.append(
                    (
                        jnp.where(upper, even, odd),
                        pltpu.roll(jnp.where(upper, odd, even), 4, 0),
                    )
                )
            for p in (0, 1):
                a, c = tiles[0][p], tiles[1][p]
                rows = slice(8 * t, 8 * t + 8)
                bufs[0][1 + 2 * gx + p, rows, :] = jnp.where(mine, a, c)
                bufs[1][1 + 2 * gx + p, rows, :] = pltpu.roll(jnp.where(mine, c, a), 64, 1)

    loop(0, nx, min(SU, nx), body)


def coarse_kernel(got, got_z, *refs, nx, ny):
    n2, y2, n3, y3 = 2 * nx, 4 * ny, nx, 2 * ny
    coef2, refs = (refs[0], refs[1:3], refs[3:5], refs[5:7], refs[7], refs[8:10]), refs[10:]
    coef3, refs = (refs[0], refs[1:3], refs[3:5], refs[5:7], None, refs[7:9]), refs[9:]
    in2, out2, in3, out3, fold2, fold1 = (
        refs[0:2], refs[2:4], refs[4:6], refs[6:8], refs[8], refs[9],
    )
    unpack(got, got_z, 8, in2, nx, ny)

    def body(k):
        here = pl.ds(k, 4)
        for c in (0, 1):
            out2[c][here] = jnp.where(in2[c][here] > 0.0, 1.0, 3.0)
        total = 0.25 * (in2[0][here] + in2[1][here])
        fold2[pl.ds(pl.multiple_of((k - 1) * y2, 4 * y2), 4 * y2), :] = total.reshape(4 * y2, Z2)

    loop(1, n2 + 1, 4, body)
    for bufs, count in ((in2, n2), (out2, n2), (in3, n3), (out3, n3)):
        for c in (0, 1):
            bufs[c][0:1] = jnp.zeros_like(bufs[c][0:1])
            bufs[c][count + 1 :] = jnp.zeros_like(bufs[c][0:1])
    faces(in2, out2, *coef2, None, 1, n2 + 1, min(S2, n2))
    restrict(fold2, fold1, in3, n3, y3)
    lane = iota((n3, y3, Z2), 2)
    for c in (0, 1):
        value = jnp.where(in3[c][1 : n3 + 1] > 0.0, 1.0, 3.0)
        out3[c][1 : n3 + 1] = jnp.where(lane < Z2 // 2, value, 0.0)
    faces(in3, out3, *coef3, None, 1, n3 + 1, min(S3, n3))


def restrict(fold2, fold1, bufs, n3, y3):
    rows = 2 * n3 * y3
    sums = fold2[pl.ds(0, rows, 2), :] + fold2[pl.ds(1, rows, 2), :]
    fold1[0, 0:rows, :] = dot(sums, pair_matrix(Z2, Z2, 0.5))
    first = first_is_red((1, y3, Z2))

    def body(p):
        a = fold1[0, pl.ds(pl.multiple_of(2 * p * y3, y3), y3), :][None]
        c = fold1[0, pl.ds(pl.multiple_of((2 * p + 1) * y3, y3), y3), :][None]
        here = pl.ds(p + 1, 1)
        bufs[0][here] = jnp.where(first, a, c)
        bufs[1][here] = jnp.where(first, c, a)

    loop(0, n3, 1, body)


def up_kernel(got, got_z, *refs, nx, ny):
    level1, refs = refs[:13], refs[13:]
    level0, refs = refs[:13], refs[13:]
    coef2, diag2, inv2, refs = (
        (refs[0], refs[1:3], refs[3:5], refs[5:7]), refs[7], refs[8:10], refs[10:],
    )
    coef3, inv3, refs = (refs[0], refs[1:3], refs[3:5], refs[5:7]), refs[7:9], refs[9:]
    out, refs = refs[0], refs[1:]

    def split(r):
        return r[0:2], r[2:4], (r[4], r[5:7], r[7:9], r[9:11]), r[11:13]

    v1, b1, coef1, inv1 = split(level1)
    v0, b0, coef0, inv0 = split(level0)
    n2, y2 = 2 * nx, 4 * ny
    n3, y3 = nx, 2 * ny
    v2, b2, v3, b3 = refs[0:2], refs[2:4], refs[4:6], refs[6:8]
    fold2, fold1, fold0 = refs[8], refs[9], refs[10]
    gx_me, gy_me, core = where_am_i()
    unpack(got, got_z, 0, b2, nx, ny)
    step2 = min(S22, n2)
    from_zero(v2, b2, coef2, inv2, 1, n2 + 1, step2)
    first = first_is_red((step2, y2, Z2))

    def body(k):
        here = pl.ds(k, step2)
        res = b2[0][here] - (diag2[here] * v2[0][here] - gathered(v2, 0, *coef2, k, step2, first))
        start = pl.multiple_of((k - 1) * y2, step2 * y2)
        fold2[pl.ds(start, step2 * y2), :] = res.reshape(step2 * y2, Z2)

    loop(1, n2 + 1, step2, body)
    restrict(fold2, fold1, b3, n3, y3)
    from_zero(v3, b3, coef3, inv3, 1, n3 + 1, n3)

    def sweep(i):
        half_sweep(v3, b3, 0, coef3, inv3, 1, n3 + 1, n3)
        half_sweep(v3, b3, 1, coef3, inv3, 1, n3 + 1, n3)

    loop(0, COARSE_SWEEPS - 1, 1, sweep)
    near2 = min(8, n2)
    base = jnp.clip(2 * gx_me - 2, 0, n2 - near2)
    first3 = first_is_red((y3, Z2))
    for p in range(near2 // 2):
        a, c = v3[0][base // 2 + p + 1], v3[1][base // 2 + p + 1]
        fold2[2 * p * y3 : (2 * p + 1) * y3, :] = jnp.where(first3, a, c)
        fold2[(2 * p + 1) * y3 : (2 * p + 2) * y3, :] = jnp.where(first3, c, a)
    twice_rows(fold1, dot(fold2[0 : near2 * y3, :], copy_matrix(Z2, Z2)))
    for k in range(0, near2, 4):
        e = fold1[0, k * y2 : (k + 4) * y2, :].reshape(4, y2, Z2)
        here = pl.ds(base + 1 + k, 4)
        v2[1][here] = v2[1][here] + e
    half_sweep(v2, b2, 0, coef2, inv2, base + 1, base + 1 + near2, near2)
    half_sweep(v2, b2, 1, coef2, inv2, base + 1, base + 1 + near2, near2)
    shift = lax.rem(4 - 4 * gy_me + 2 * y2, y2)
    first1 = first_is_red((y2, Z2))
    cells = []
    for j in range(4):
        a, c = v2[0][2 * gx_me + j], v2[1][2 * gx_me + j]
        for cell in (jnp.where(first1, a, c), jnp.where(first1, c, a)):
            cells.append(pltpu.roll(cell, shift, 0)[0:16])
    twice_rows(fold1, dot(jnp.concatenate(cells, axis=0), copy_matrix(Z2, Z1)))
    for k in range(1, K1 - 1):
        e = columns(fold1, 32 * (k - 1), Y1, Z1)
        v1[1][k] = jnp.where(inv1[1][k] > 0.0, v1[1][k] + e, 0.0)
    half_sweep(v1, b1, 0, coef1, inv1, 1, K1 - 1, S1)
    half_sweep(v1, b1, 1, coef1, inv1, 1, K1 - 1, S1)
    first0 = first_is_red((Y1, Z1))
    cells = []
    for k in range(H - 1, K1 - H + 1):
        a, c = v1[0][k], v1[1][k]
        cells += [jnp.where(first0, a, c), jnp.where(first0, c, a)]
    cells = [cell[4:20] for cell in cells[1:-1]]
    twice_rows(fold0, dot(jnp.concatenate(cells, axis=0), copy_matrix(Z1, Z0, core * 64)))

    def body(p):
        e = columns(fold0, pl.multiple_of(p * 32, 32), 32, Z0)[None]
        here = pl.ds(p + H - 1, 1)
        v0[1][here] = jnp.where(inv0[1][here] > 0.0, v0[1][here] + e, 0.0)

    loop(0, BX // 2 + 2, 1, body)
    half_sweep(v0, b0, 0, coef0, inv0, H - 1, K0 - H + 1, SHB)
    half_sweep(v0, b0, 1, coef0, inv0, H, K0 - H, SH)
    lanes = pl.ds(pl.multiple_of(core * 128, 128), BZ)
    half_first = first_is_red((BY, BZ))

    def body(p):
        a, c = v0[0][p + H, 8:24, lanes], v0[1][p + H, 8:24, lanes]
        out[2 * p] = jnp.where(half_first, a, c)
        out[2 * p + 1] = jnp.where(half_first, c, a)

    loop(0, BX // 2, 1, body)


def shape(*dims):
    return jax.ShapeDtypeStruct(dims, F32)


def scratch(*dims):
    return pltpu.VMEM(dims, F32)


def ring(x, axis, step):
    n = lax.axis_size(axis)
    return lax.ppermute(x, axis, [(i, (i + step) % n) for i in range(n)])


def swap(x):
    return lax.ppermute(x, "gz", [(0, 1), (1, 0)])


def gather(send, nx, ny):
    got = lax.all_to_all(send, "gy", 0, 0, tiled=True)
    (send,) = call(spread_kernel, "spread", 4, [(nx,) + got.shape], [], got)
    return lax.all_to_all(send, "gx", 0, 0, tiled=True).reshape((nx * ny,) + got.shape[1:])


def call(kernel, name, mib, outs, scratches, *args, hbm_in=0, hbm_out=0):
    return pl.pallas_call(
        kernel,
        out_shape=tuple(shape(*o) for o in outs),
        in_specs=[HBM] * hbm_in + [VMEM] * (len(args) - hbm_in),
        out_specs=(HBM,) * hbm_out + (VMEM,) * (len(outs) - hbm_out),
        scratch_shapes=[scratch(*s) if isinstance(s, tuple) else s for s in scratches],
        compiler_params=params(mib),
        name=name,
    )(*args)


def on_device(membrane, recovery, extracellular, fiber_scale, labels):
    nx, ny = lax.axis_size("gx"), lax.axis_size("gy")
    block = (BX, BY, BZ)
    held = [
        pltpu.with_memory_space_constraint(x, pltpu.HBM)
        for x in (membrane, recovery, extracellular, fiber_scale, labels)
    ]
    own, xup, xdn, yup, ydn = call(
        prep_kernel, "prep", 6,
        [(AT_MEAN + 2, BY, BZ)] + [(18, BY, BZ)] * 4,
        [block] * 4
        + [pltpu.VMEM(labels.shape, jnp.int32), (1, 128, 128), pltpu.SemaphoreType.DMA((5,))],
        *held, hbm_in=5,
    )
    xlo, xhi = ring(xup, "gx", 1), ring(xdn, "gx", -1)
    ylo, yhi = ring(yup, "gy", 1), ring(ydn, "gy", -1)
    cup, cdn = call(corner_kernel, "corner", 4, [(20, 8, BZ)] * 2, [], xlo, xhi)
    clo, chi = lax.optimization_barrier((ring(cup, "gy", 1), ring(cdn, "gy", -1)))
    halos = []
    for piece in (own, xlo, xhi, ylo, yhi, clo, chi):
        halos += [piece, swap(piece)]
    (seed,) = call(seed_kernel, "seed", 4, [(8, Z2)], [(1, 32, 128)], own)
    fine = (K0, Y0, Z0)
    mid = (K1, Y1, Z1)
    grid2, grid3 = (2 * nx + 2, 4 * ny, Z2), (nx + 2, 2 * ny, Z2)
    mnext, rhs1, rup, rdn, in1r, in1b, *level0 = call(
        fine_kernel, "fine", 20,
        [block, (2, 4, 8, Z1), (2, 2, 8, Z1), (2, 2, 8, Z1)] + [mid] * 2 + [fine] * 13,
        [fine] * 16
        + [(8, BY, Z0), (2, 128, 128), block, pltpu.SemaphoreType.DMA((1,))],
        *halos, hbm_out=1,
    )
    rnext, *coef1 = call(
        middle_faces_kernel, "middle_faces", 4, [block] + [mid] * 10,
        [mid] * 2 + [block] * 2 + [pltpu.SemaphoreType.DMA((2,))],
        held[0], held[1], in1r, in1b, hbm_in=2, hbm_out=1,
    )
    part = (2, 2, 16, Z1)
    wide, xup, xdn = call(
        join_kernel, "join", 4, [(2, 4, 16, Z1), part, part], [],
        ring(rup, "gy", 1), rhs1, ring(rdn, "gy", -1),
    )
    low, high = ring(xup, "gx", 1), ring(xdn, "gx", -1)
    v1r, v1b, b1r, b1b, send = call(
        middle_kernel, "middle", 4,
        [mid] * 4 + [(ny, 16, Z2)],
        [(32, Z1), (1, 32, 128)],
        low, wide, high, seed, *coef1,
    )
    got = gather(send, nx, ny)
    got_z = swap(got)
    coarse = call(
        lambda *refs: coarse_kernel(*refs, nx=nx, ny=ny), "coarse", 8,
        [grid2] * 10 + [grid3] * 9,
        [grid2] * 4 + [grid3] * 4 + [(8 * nx * ny, Z2), (1, 4 * nx * ny, Z2)],
        got, got_z,
    )
    level1 = [v1r, v1b, b1r, b1b, *coef1[:7], *coef1[8:]]
    (enext,) = call(
        lambda *refs: up_kernel(*refs, nx=nx, ny=ny), "up", 10,
        [block],
        [grid2] * 4 + [grid3] * 4
        + [(8 * nx * ny, Z2), (2, max(4 * nx * ny, 256), Z2), (3, 320, 128)],
        got, got_z, *level1, *level0, *coarse,
    )
    return mnext, rnext, enext


def solution(mesh):
    spec = P("gx", "gy", "gz")
    return jax.shard_map(
        on_device, mesh=mesh, in_specs=(spec,) * 5, out_specs=(spec,) * 3, check_vma=False
    )
```

```python
import jax
import jax.numpy as jnp
from jax import lax
from jax.experimental import pallas as pl
from jax.experimental.pallas import tpu as pltpu
from jax.sharding import PartitionSpec as P

TIME_STEP = 0.05
IONIC_GAIN = 8.0
IONIC_ONSET = 0.15
RECOVERY_RATE = 0.01
COARSE_SWEEPS = 8

F32 = jnp.float32
BX, BY, BZ = 16, 16, 256
H = 3
SF, SI, SH, SHB, S1, S2, SU, S22, S3 = 3, 4, 4, 5, 8, 8, 8, 16, 16
AT_IN, AT_W, AT_U, AT_MEAN = BX, 2 * BX, 3 * BX, 3 * BX + BX // 2
K0, Y0, Z0 = BX // 2 + 2 * H, 32, 384
K1, Y1, Z1 = BX // 4 + 2 * H, 24, BZ
Z2 = BZ // 2
VMEM = pl.BlockSpec(memory_space=pltpu.VMEM)
HBM = pl.BlockSpec(memory_space=pltpu.HBM)


def params(mib):
    return pltpu.CompilerParams(vmem_limit_bytes=mib * 1024 * 1024)


def iota(shape, dim):
    return lax.broadcasted_iota(jnp.int32, shape, dim)


def first_is_red(shape):
    return ((iota(shape, len(shape) - 2) + iota(shape, len(shape) - 1)) & 1) == 0


def up(x, axis):
    return pltpu.roll(x, x.shape[axis] - 1, axis)


def down(x, axis):
    return pltpu.roll(x, 1, axis)


def pair_matrix(rows, cols, value, shift=0):
    return jnp.where(
        iota((rows, cols), 0) // 2 + shift == iota((rows, cols), 1), value, 0.0
    ).astype(F32)


def copy_matrix(rows, cols, shift=0):
    return jnp.where(
        iota((rows, cols), 1) // 2 + shift == iota((rows, cols), 0), 1.0, 0.0
    ).astype(F32)


def dot(a, b):
    b = b.astype(jnp.bfloat16)
    high = a.astype(jnp.bfloat16)
    rest = a - high.astype(F32)
    mid = rest.astype(jnp.bfloat16)
    low = (rest - mid.astype(F32)).astype(jnp.bfloat16)
    parts = [jnp.dot(p, b, preferred_element_type=F32) for p in (low, mid, high)]
    return parts[0] + parts[1] + parts[2]


def sum_rows(buf, x):
    rows, cols = x.shape
    sums = []
    for c in range(cols // 128):
        buf[c, 0:rows, :] = x[:, 128 * c : 128 * c + 128]
        sums.append(buf[c, pl.ds(0, rows // 2, 2), :] + buf[c, pl.ds(1, rows // 2, 2), :])
    return sums[0] if len(sums) == 1 else jnp.concatenate(sums, axis=1)


def twice_rows(buf, x):
    rows, cols = x.shape
    for c in range(cols // 128):
        for k in (0, 1):
            buf[c, pl.ds(k, rows, 2), :] = x[:, 128 * c : 128 * c + 128]


def columns(buf, start, rows, cols):
    parts = [buf[c, pl.ds(start, rows), :] for c in range(cols // 128)]
    return parts[0] if len(parts) == 1 else jnp.concatenate(parts, axis=1)


def loop(start, stop, step, body):
    if not isinstance(start, int) or stop - start == step:
        body(start)
        return

    def run(index, carry):
        body(start + index * step)
        return carry

    lax.fori_loop(0, (stop - start) // step, run, 0)


def far(other, k, step, red, first):
    before, after = other[pl.ds(k - 1, step)], other[pl.ds(k + 1, step)]
    return jnp.where(first, before, after) if red else jnp.where(first, after, before)


def faces(inner, outer, near, fars, ys, zs, diag, inv, least, start, stop, step):
    rows, lanes = inner[0].shape[1:]
    shape = (step, rows, lanes)
    row, lane = iota(shape, 1), iota(shape, 2)
    first = first_is_red(shape)

    def body(k):
        here = pl.ds(k, step)
        low = jnp.minimum(inner[0][here], inner[1][here])
        if least is not None:
            least[0][here] = low
        halves = [0.5 * outer[c][here] for c in (0, 1)]
        pair = low + halves[0] + halves[1]
        near[here] = pair
        totals = [pair, pair]
        for axis, out, keep, place, size in (
            (1, ys, None if least is None else least[2], row, rows),
            (2, zs, None if least is None else least[3], lane, lanes),
        ):
            full = []
            for c in (0, 1):
                o = 1 - c
                mine = inner[c][here]
                low = jnp.where(place < size - 1, jnp.minimum(mine, up(inner[o][here], axis)), 0.0)
                if keep is not None:
                    keep[c][here] = low
                both = low + halves[c] + jnp.where(place < size - 1, up(halves[o], axis), 0.0)
                full.append(both)
                out[c][here] = jnp.where(place < size - 1, both, 0.0)
            for c in (0, 1):
                below = jnp.where(place > 0, down(full[1 - c], axis), halves[c])
                totals[c] = totals[c] + full[c] + below
        for c in (0, 1):
            o = 1 - c
            low = jnp.minimum(inner[c][here], far(inner[o], k, step, c == 0, first))
            if least is not None:
                least[1][c][here] = low
            both = low + halves[c] + 0.5 * far(outer[o], k, step, c == 0, first)
            fars[c][here] = both
            total = totals[c] + both
            if c == 0 and diag is not None:
                diag[here] = total
            inside = outer[c][here] > 0.0
            inv[c][here] = jnp.where(inside, 1.0 / jnp.where(inside, total, 1.0), 0.0)

    loop(start, stop, step, body)


def gathered(v, c, near, fars, ys, zs, k, step, first):
    here = pl.ds(k, step)
    o = 1 - c
    other = v[o][here]
    total = near[here] * other + fars[c][here] * far(v[o], k, step, c == 0, first)
    total = total + ys[c][here] * up(other, 1) + down(ys[o][here] * other, 1)
    return total + zs[c][here] * up(other, 2) + down(zs[o][here] * other, 2)


def half_sweep(v, b, c, coef, inv, start, stop, step):
    first = first_is_red((step,) + tuple(v[0].shape[1:]))

    def body(k):
        here = pl.ds(k, step)
        v[c][here] = (b[c][here] + gathered(v, c, *coef, k, step, first)) * inv[c][here]

    loop(start, stop, step, body)


def from_zero(v, b, coef, inv, start, stop, step):
    count = v[0].shape[0]
    for c in (0, 1):
        v[c][0:1] = jnp.zeros_like(v[c][0:1])
        v[c][count - 1 :] = jnp.zeros_like(v[c][0:1])

    def body(k):
        here = pl.ds(k, step)
        v[0][here] = b[0][here] * inv[0][here]

    loop(start, stop, step, body)
    half_sweep(v, b, 1, coef, inv, start, stop, step)


def put(bufs, k, rows, lanes, a, b):
    some = a if b is None else b
    a = jnp.zeros_like(some) if a is None else a
    b = jnp.zeros_like(some) if b is None else b
    first = first_is_red(some.shape)
    bufs[0][k, rows, lanes] = jnp.where(first, a, b)
    bufs[1][k, rows, lanes] = jnp.where(first, b, a)


def colours(x):
    n = x.shape[0] // 2
    first = first_is_red(x.shape[1:])
    pairs = [(x[2 * p], x[2 * p + 1]) for p in range(n)]
    return (
        jnp.stack([jnp.where(first, a, b) for a, b in pairs]),
        jnp.stack([jnp.where(first, b, a) for a, b in pairs]),
    )


def where_am_i():
    return lax.axis_index("gx"), lax.axis_index("gy"), lax.axis_index("gz")


def flags():
    gx, gy, _ = where_am_i()
    return (
        (gx > 0).astype(F32),
        (gx < lax.axis_size("gx") - 1).astype(F32),
        (gy > 0).astype(F32),
        (gy < lax.axis_size("gy") - 1).astype(F32),
    )


def fetch(pairs, sems):
    copies = [pltpu.make_async_copy(src, dst, sems.at[i]) for i, (src, dst) in enumerate(pairs)]
    for copy in copies:
        copy.start()
    return copies


def outside(shape, own_rows, k, own, has):
    row = iota(shape, len(shape) - 2)
    in_y = jnp.where(row < 8, has[2], jnp.where(row < 8 + own_rows, 1.0, has[3]))
    return in_y * jnp.where(k < H, has[0], jnp.where(k < H + own, 1.0, has[1]))


def block_of(i):
    rows, lanes = 8 * ((i % 4) // 2), 128 * (i % 2)
    return i // 4, slice(rows, rows + 8), slice(lanes, lanes + 128)


def prep_kernel(
    m_in, r_in, u_in, f_in, labels_in, own, xup, xdn, yup, ydn, m, r, u, f, labels, fold, sems
):
    copies = fetch(
        [(labels_in, labels), (m_in, m), (u_in, u), (r_in, r), (f_in, f)], sems
    )
    for copy in copies:
        copy.wait()
    spread = jnp.where(iota((BZ // 8, BZ), 1) // 8 == iota((BZ // 8, BZ), 0), 1.0, 0.0).astype(F32)
    for bx in range(BX // 8):
        wide = jnp.dot(labels[bx].astype(F32), spread, preferred_element_type=F32)
        kind = jnp.concatenate(
            [jnp.broadcast_to(wide[by : by + 1], (8, BZ)) for by in range(BY // 8)], axis=0
        )
        factor = jnp.where(kind > 1.5, 0.3, jnp.where(kind > 0.5, 1.0, 0.0)).astype(F32)
        for x in range(8 * bx, 8 * bx + 8):
            mm, rr, uu = m[x], r[x], u[x]
            inner = factor * f[x]
            own[x] = mm + uu
            own[AT_IN + x] = inner
            ionic = IONIC_GAIN * mm * (mm - IONIC_ONSET) * (mm - 1.0) + mm * rr
            own[AT_W + x] = mm - jnp.where(kind > 0.5, TIME_STEP * ionic, 0.0)
            if x % 2:
                first = first_is_red((BY, BZ))
                own[AT_U + x // 2] = jnp.where(first, uu, u[x - 1])
    sums = jnp.concatenate(
        [own[AT_IN + 2 * p] + own[AT_IN + 2 * p + 1] for p in range(BX // 2)], axis=0
    )
    mean = sum_rows(fold, dot(sums, pair_matrix(BZ, BZ // 2, 0.125)))
    for i in range(8):
        slab, rows, lanes = block_of(i)
        for ref, base in ((own, AT_MEAN), (yup, BX), (ydn, BX)):
            ref[base + slab, rows, lanes] = mean[8 * i : 8 * i + 8]
    for i in range(5):
        slab, rows, lanes = block_of(i)
        xup[16 + slab, rows, lanes] = mean[8 * (3 + i) : 8 * (4 + i)]
        xdn[16 + slab, rows, lanes] = mean[8 * i : 8 * i + 8]
    base = 0
    for start, count, depth in ((0, BX, 5), (AT_IN, BX, 5), (AT_W, BX, 4), (AT_U, BX // 2, 2)):
        xup[base : base + depth] = own[start + count - depth : start + count]
        xdn[base : base + depth] = own[start : start + depth]
        base += depth
    row = iota((8, BZ), 0)
    turn = lambda x, by: pltpu.roll(x, by % 8, 0)
    for p in range(BX // 2):
        for out, rows, keep, by, fourth in (
            (yup, slice(8, 16), row >= 3, 3, (4, 5, 6)),
            (ydn, slice(0, 8), row < 5, 5, (2, 3, 4)),
        ):
            s = [own[2 * p + i, rows] for i in (0, 1)]
            n = [own[AT_IN + 2 * p + i, rows] for i in (0, 1)]
            rest = [own[AT_W + 2 * p, rows], own[AT_W + 2 * p + 1, rows], own[AT_U + p, rows]]
            at = 0 if out is yup else 5
            last = jnp.where(
                row == at,
                turn(rest[0], fourth[0]),
                jnp.where(row == at + 1, turn(rest[1], fourth[1]), turn(rest[2], fourth[2])),
            )
            out[2 * p, 0:8] = jnp.where(keep, s[0], turn(rest[0], by))
            out[2 * p, 8:16] = jnp.where(keep, s[1], turn(rest[1], by))
            out[2 * p + 1, 0:8] = jnp.where(keep, n[0], turn(rest[2], by))
            out[2 * p + 1, 8:16] = jnp.where(keep, n[1], last)


def merge(high, a, b):
    row = iota(a.shape, 0)
    return jnp.where(row >= 4, a, pltpu.roll(b, 4, 0)) if high else jnp.where(
        row < 4, a, pltpu.roll(b, 4, 0)
    )


def corner_kernel(xlo, xhi, cup, cdn):
    for high, out in ((True, cup), (False, cdn)):
        rows = slice(8, 16) if high else slice(0, 8)
        edge = iota((8, BZ), 0) == (7 if high else 0)
        for side, src in ((0, xlo), (1, xhi)):
            at = lambda base, depth, d: src[base + (depth - d if side == 0 else d - 1), rows]
            s, n, w = (
                lambda d: at(0, 5, d),
                lambda d: at(5, 5, d),
                lambda d: at(10, 4, d),
            )
            u = lambda d: at(14, 2, d)
            tiles = [
                merge(high, s(1), s(2)),
                merge(high, s(3), s(4)),
                merge(high, n(1), n(2)),
                merge(high, n(3), n(4)),
                merge(high, w(1), w(2)),
                merge(high, jnp.where(edge, w(3), pltpu.roll(u(2), 7 if high else 1, 0)), u(1)),
            ]
            for t, tile in enumerate(tiles):
                out[8 * side + t] = tile

            def coarse(d):
                slab, block_rows, lanes = block_of(5 - d if side == 0 else d - 1)
                return src[16 + slab, block_rows, lanes]

            halves = (
                coarse(1),
                merge(high, coarse(2), coarse(3)),
                merge(high, coarse(4), coarse(5)),
            )
            for i, half in enumerate(halves):
                lanes = 128 * (i % 2)
                out[8 * side + 6 + i // 2, :, lanes : lanes + 128] = half
            out[8 * side + 7, :, 128:256] = halves[2]


def fine_kernel(*refs):
    pieces, refs = refs[:14], refs[14:]
    mnext, rhs1, rup, rdn, refs = refs[0], refs[1], refs[2], refs[3], refs[4:]
    mean1, refs = refs[0:2], refs[2:]
    v, b, near, fars, ys, zs, inv, refs = (
        refs[0:2], refs[2:4], refs[4], refs[5:7], refs[7:9], refs[9:11], refs[11:13], refs[13:],
    )
    inner, outer, s, w, refs = refs[0:2], refs[2:4], refs[4:6], refs[6:8], refs[8:]
    low_near, low_far, low_y, low_z, diag, fold, fold2 = (
        refs[0], refs[1:3], refs[3:5], refs[5:7], refs[7], refs[8], refs[9],
    )
    mout, sems = refs[10], refs[11]
    core = lax.axis_index("gz")
    has = flags()
    fields = (s, inner, w)
    for side in (0, 1):
        own, xlo, xhi, ylo, yhi, clo, chi = pieces[side::2]
        wide = BZ if side == 0 else 128
        src = pl.ds(0 if side == 0 else pl.multiple_of(core * 128, 128), wide)
        dst = pl.ds(pl.multiple_of(core * 128 if side == 0 else (1 - core) * 256, 128), wide)
        mid, low, high = slice(8, 24), slice(0, 8), slice(24, 32)

        def body(p, own=own, ylo=ylo, yhi=yhi, src=src, dst=dst):
            k = p + H
            for q, bufs in enumerate(fields):
                put(bufs, k, mid, dst, own[BX * q + 2 * p, :, src], own[BX * q + 2 * p + 1, :, src])
            v[1][k, mid, dst] = own[AT_U + p, :, src]
            row = iota((8, wide), 0)
            turn = lambda x, by: pltpu.roll(x, by, 0)
            for rows, ref, flag, keep, deep, by, fourth in (
                (low, ylo, has[2], row >= 3, row >= 5, 5, (4, 3, 2)),
                (high, yhi, has[3], row < 5, row < 3, 3, (6, 5, 4)),
            ):
                t = [
                    ref[2 * p + i // 2, 8 * (i % 2) : 8 * (i % 2) + 8, src] * flag for i in range(4)
                ]
                put(s, k, rows, dst, t[0], t[1])
                put(inner, k, rows, dst, jnp.where(keep, t[2], 0.0), jnp.where(keep, t[3], 0.0))
                rest = [
                    jnp.where(deep, turn(t[i], by), turn(t[3], fourth[i])) for i in (0, 1, 2)
                ]
                put(w, k, rows, dst, rest[0], rest[1])
                v[1][k, rows, dst] = rest[2]

        loop(0, BX // 2, 1, body)
        for x_side, ref, flag in ((0, xlo, has[0]), (1, xhi, has[1])):
            base = 0
            order = (5, 4, 3, 2, 1) if x_side == 0 else (1, 2, 3, 4, 5)
            for q, depth in enumerate((5, 5, 4)):
                slabs = {d: ref[base + i, :, src] * flag for i, d in enumerate(
                    [d for d in order if d <= depth])}
                base += depth
                for j in range(H):
                    near_d, far_d = 2 * j + 1, 2 * j + 2
                    pair = (slabs.get(near_d), slabs.get(far_d))
                    k = H - 1 - j if x_side == 0 else K0 - H + j
                    if x_side == 0:
                        pair = pair[::-1]
                    if pair[0] is None and pair[1] is None:
                        pair = (jnp.zeros((16, wide), F32), None)
                    put(fields[q], k, mid, dst, *pair)
            black = [ref[14, :, src] * flag, ref[15, :, src] * flag, jnp.zeros((16, wide), F32)]
            if x_side == 0:
                black[0], black[1] = black[1], black[0]
            for j in range(H):
                v[1][H - 1 - j if x_side == 0 else K0 - H + j, mid, dst] = black[j]
            for rows, cref, yflag in ((low, clo, has[2]), (high, chi, has[3])):
                both = flag * yflag
                tile = [cref[8 * x_side + t, :, src] * both for t in range(6)]
                turned = [pltpu.roll(t, 4, 0) for t in tile]
                zero = jnp.zeros((8, wide), F32)
                by_field = (
                    (tile[0], turned[0], tile[1], turned[1]),
                    (tile[2], turned[2], tile[3], turned[3]),
                    (tile[4], turned[4], tile[5], zero),
                )
                last = pltpu.roll(tile[5], 1 if cref is clo else 7, 0)
                black = (turned[5], last, zero)
                for j in range(H):
                    v[1][H - 1 - j if x_side == 0 else K0 - H + j, rows, dst] = black[j]
                for q in range(3):
                    slabs = by_field[q] + (zero, zero)
                    for j in range(H):
                        pair = (slabs[2 * j], slabs[2 * j + 1])
                        k = H - 1 - j if x_side == 0 else K0 - H + j
                        put(fields[q], k, rows, dst, *(pair[::-1] if x_side == 0 else pair))
        dst = pl.ds(pl.multiple_of((core if side == 0 else 1 - core) * 128, 128), 128)
        for p in range(4):
            def of_own(i):
                slab, rows, lanes = block_of(i)
                return own[AT_MEAN + slab, rows, lanes]

            put(mean1, p + H, slice(8, 16), dst, of_own(2 * p), of_own(2 * p + 1))
            for rows, ref, flag in ((slice(0, 8), ylo, has[2]), (slice(16, 24), yhi, has[3])):
                def of_y(i):
                    slab, part, lanes = block_of(i)
                    return ref[BX + slab, part, lanes] * flag

                put(mean1, p + H, rows, dst, of_y(2 * p), of_y(2 * p + 1))
        for x_side, ref, flag in ((0, xlo, has[0]), (1, xhi, has[1])):
            def of_x(d):
                slab, part, lanes = block_of(5 - d if x_side == 0 else d - 1)
                return ref[16 + slab, part, lanes] * flag

            zero = jnp.zeros((8, 128), F32)
            mids = [of_x(d) for d in (1, 2, 3, 4, 5)] + [zero]
            columns_of = [(slice(8, 16), mids)]
            for rows, cref, yflag in ((slice(0, 8), clo, has[2]), (slice(16, 24), chi, has[3])):
                h = [
                    cref[8 * x_side + 6 + i // 2, :, 128 * (i % 2) : 128 * (i % 2) + 128]
                    * (flag * yflag)
                    for i in range(3)
                ]
                t = [h[0], h[1], pltpu.roll(h[1], 4, 0), h[2], pltpu.roll(h[2], 4, 0)]
                columns_of.append((rows, t + [zero]))
            for rows, slabs in columns_of:
                for j in range(H):
                    pair = (slabs[2 * j], slabs[2 * j + 1])
                    k = H - 1 - j if x_side == 0 else K1 - H + j
                    put(mean1, k, rows, dst, *(pair[::-1] if x_side == 0 else pair))

    def body(k):
        here = pl.ds(k, 1)
        inside = outside((1, Y0, Z0), 16, k, BX // 2, has)
        for c in (0, 1):
            outer[c][here] = jnp.where(inner[c][here] > 0.0, 1.0, 3.0 * inside)

    loop(0, K0, 1, body)
    faces(
        inner, outer, near, fars, ys, zs, diag, inv, (low_near, low_far, low_y, low_z), 1, K0 - 1, SF
    )
    first = first_is_red((SI, Y0, Z0))

    def intra(x, k):
        here = pl.ds(k, SI)
        a = [x[0][here], x[1][here]]
        flow = low_near[here] * (a[1] - a[0])
        total = [flow, -flow]
        for c in (0, 1):
            total[c] = total[c] + low_far[c][here] * (far(x[1 - c], k, SI, c == 0, first) - a[c])
        for axis, low in ((1, low_y), (2, low_z)):
            flows = [low[c][here] * (up(a[1 - c], axis) - a[c]) for c in (0, 1)]
            for c in (0, 1):
                total[c] = total[c] + flows[c] - down(flows[1 - c], axis)
        return total

    def body(k):
        here = pl.ds(k, SI)
        drive = intra(s, k)
        for c in (0, 1):
            w[c][here] = w[c][here] + TIME_STEP * drive[c]

    loop(1, K0 - 1, SI, body)
    lanes = pl.ds(pl.multiple_of(core * 128, 128), BZ)
    half_first = first_is_red((BY, BZ))

    def body(p):
        a, c = w[0][p + H, 8:24, lanes], w[1][p + H, 8:24, lanes]
        mout[2 * p] = jnp.where(half_first, a, c)
        mout[2 * p + 1] = jnp.where(half_first, c, a)

    loop(0, BX // 2, 1, body)
    copies = fetch([(mout, mnext)], sems)

    def body(k):
        here = pl.ds(k, SI)
        both = intra(w, k)
        for c in (0, 1):
            b[c][here] = both[c]

    loop(1, K0 - 1, SI, body)
    coef = (near, fars, ys, zs)
    half_sweep(v, b, 0, coef, inv, 1, K0 - 1, SH)
    half_sweep(v, b, 1, coef, inv, 2, K0 - 2, SHB)
    first = first_is_red((SH, Y0, Z0))

    def body(p):
        here = pl.ds(p + H, SH)
        res = b[0][here] - (diag[here] * v[0][here] - gathered(v, 0, *coef, p + H, SH, first))
        fold[pl.ds(p, SH)] = res[:, 8:24, :]

    loop(0, BX // 2, SH, body)
    half = BX // 2 * BY
    pairs = pair_matrix(Z0, Z1, 0.5, core * 64)
    coarse = sum_rows(fold2, dot(fold[...].reshape(half, Z0), pairs)).reshape(8, 8, Z1)
    red, black = colours(coarse)
    for c, pairs in ((0, red), (1, black)):
        rhs1[c] = pairs
        for j in (0, 1):
            rup[c, j] = merge(True, pairs[2 * j], pairs[2 * j + 1])
            rdn[c, j] = merge(False, pairs[2 * j], pairs[2 * j + 1])
    copies[0].wait()


def middle_faces_kernel(m_in, r_in, *refs):
    inner, refs = refs[0:2], refs[2:]
    rnext, near, fars, ys, zs, diag, inv, outer = (
        refs[0], refs[1], refs[2:4], refs[4:6], refs[6:8], refs[8], refs[9:11], refs[11:13],
    )
    m, r, sems = refs[13:]
    copies = fetch([(m_in, m), (r_in, r)], sems)
    has = flags()
    for k in range(K1):
        inside = outside((Y1, Z1), 8, k, 4, has)
        for c in (0, 1):
            outer[c][k] = jnp.where(inner[c][k] > 0.0, 1.0, 3.0 * inside)
    for copy in copies:
        copy.wait()
    for x in range(BX):
        mm, rr = m[x], r[x]
        r[x] = rr + TIME_STEP * RECOVERY_RATE * (
            -rr - IONIC_GAIN * mm * (mm - IONIC_ONSET - 1.0)
        )
    copies = fetch([(r, rnext)], sems)
    faces(inner, outer, near, fars, ys, zs, diag, inv, None, 1, K1 - 1, S1)
    copies[0].wait()


def join_kernel(low, own, high, wide, xup, xdn):
    row = iota((8, Z1), 0)
    for c in (0, 1):
        for p in range(4):
            a, b = low[c, p // 2], high[c, p // 2]
            edge = jnp.where(row >= 4, a, b) if p % 2 == 0 else pltpu.roll(
                jnp.where(row < 4, a, b), 4, 0
            )
            for ref, q in ((wide, p), (xdn, p) if p < 2 else (xup, p - 2)):
                ref[c, q, 0:8] = edge
                ref[c, q, 8:16] = own[c, p]


def spread_kernel(got, send):
    whole = got[...]
    for d in range(send.shape[0]):
        send[d] = whole


def middle_kernel(low, own, high, seed, *refs):
    near, fars, ys, zs, diag, inv, refs = (
        refs[0], refs[1:3], refs[3:5], refs[5:7], refs[7], refs[8:10], refs[10:],
    )
    v, b, send, fold, fold2 = refs[0:2], refs[2:4], refs[4], refs[5], refs[6]
    core = lax.axis_index("gz")
    has = flags()
    for c in (0, 1):
        b[c][0:1] = jnp.zeros((1, Y1, Z1), F32)
        b[c][K1 - 1 :] = jnp.zeros((1, Y1, Z1), F32)
        for k in range(1, K1 - 1):
            src = low[c, k - 1] if k < H else (own[c, k - H] if k < H + 4 else high[c, k - H - 4])
            inside = outside((Y1, Z1), 8, k, 4, has)
            for rows, part in ((slice(0, 8), src[0:8]), (slice(8, 16), src[8:16]), (slice(16, 24), src[0:8])):
                b[c][k, rows] = part * inside[rows]
    coef = (near, fars, ys, zs)
    from_zero(v, b, coef, inv, 1, K1 - 1, S1)
    first = first_is_red((2, Y1, Z1))
    for p in (0, 2):
        here = slice(p + H, p + H + 2)
        res = b[0][here] - (diag[here] * v[0][here] - gathered(v, 0, *coef, p + H, 2, first))
        fold[8 * p : 8 * p + 16] = res[:, 8:16, :].reshape(16, Z1)
    both = sum_rows(fold2, dot(fold[...], pair_matrix(Z1, Z2, 0.5)))
    red, black = colours(both.reshape(4, 4, Z2))
    red, black = red.reshape(8, Z2), black.reshape(8, Z2)
    mine = (iota((8, Z2), 1) < 64) == (core == 0)
    piece = in_order(jnp.where(mine, red, pltpu.roll(black, 64, 1)))
    for d in range(send.shape[0]):
        send[d, 0:8] = piece
        send[d, 8:16] = seed[...]


def in_order(piece):
    odd = (iota(piece.shape, 0) * 0 + lax.axis_index("gy")) & 1
    return jnp.where(odd == 1, pltpu.roll(piece, 4, 0), piece)


def seed_kernel(own, send, fold):
    sums = []
    for p in range(4):
        total = None
        for i in (2 * p, 2 * p + 1):
            slab, rows, lanes = block_of(i)
            block = own[AT_MEAN + slab, rows, lanes]
            total = block if total is None else total + block
        sums.append(total)
    both = sum_rows(fold, dot(jnp.concatenate(sums, axis=0), pair_matrix(Z2, Z2, 0.125)))
    red, black = colours(both.reshape(4, 4, Z2))
    red, black = red.reshape(8, Z2), black.reshape(8, Z2)
    core = lax.axis_index("gz")
    lane = iota((8, Z2), 1) + core * 0
    lower = jnp.where(lane < 64, red, pltpu.roll(black, 64, 1))
    upper = jnp.where(lane < 64, black, pltpu.roll(red, 64, 1))
    send[...] = in_order(jnp.where(core == 0, lower, upper))


def unpack(got, got_z, part, bufs, nx, ny):
    core = lax.axis_index("gz")
    mine = (iota((8, Z2), 1) < 64) == (core == 0)
    upper = iota((8, Z2), 0) < 4

    def body(start):
      for gx in [start + i for i in range(min(SU, nx))]:
        for t in range(ny // 2):
            d = gx * ny + 2 * t
            tiles = []
            for src in (got, got_z):
                even, odd = src[d, part : part + 8], src[d + 1, part : part + 8]
                tiles.append(
                    (
                        jnp.where(upper, even, odd),
                        pltpu.roll(jnp.where(upper, odd, even), 4, 0),
                    )
                )
            for p in (0, 1):
                a, c = tiles[0][p], tiles[1][p]
                rows = slice(8 * t, 8 * t + 8)
                bufs[0][1 + 2 * gx + p, rows, :] = jnp.where(mine, a, c)
                bufs[1][1 + 2 * gx + p, rows, :] = pltpu.roll(jnp.where(mine, c, a), 64, 1)

    loop(0, nx, min(SU, nx), body)


def coarse_kernel(got, got_z, *refs, nx, ny):
    n2, y2, n3, y3 = 2 * nx, 4 * ny, nx, 2 * ny
    coef2, refs = (refs[0], refs[1:3], refs[3:5], refs[5:7], refs[7], refs[8:10]), refs[10:]
    coef3, refs = (refs[0], refs[1:3], refs[3:5], refs[5:7], None, refs[7:9]), refs[9:]
    in2, out2, in3, out3, fold2, fold1 = (
        refs[0:2], refs[2:4], refs[4:6], refs[6:8], refs[8], refs[9],
    )
    unpack(got, got_z, 8, in2, nx, ny)

    def body(k):
        here = pl.ds(k, 4)
        for c in (0, 1):
            out2[c][here] = jnp.where(in2[c][here] > 0.0, 1.0, 3.0)
        total = 0.25 * (in2[0][here] + in2[1][here])
        fold2[pl.ds(pl.multiple_of((k - 1) * y2, 4 * y2), 4 * y2), :] = total.reshape(4 * y2, Z2)

    loop(1, n2 + 1, 4, body)
    for bufs, count in ((in2, n2), (out2, n2), (in3, n3), (out3, n3)):
        for c in (0, 1):
            bufs[c][0:1] = jnp.zeros_like(bufs[c][0:1])
            bufs[c][count + 1 :] = jnp.zeros_like(bufs[c][0:1])
    faces(in2, out2, *coef2, None, 1, n2 + 1, min(S2, n2))
    restrict(fold2, fold1, in3, n3, y3)
    lane = iota((n3, y3, Z2), 2)
    for c in (0, 1):
        value = jnp.where(in3[c][1 : n3 + 1] > 0.0, 1.0, 3.0)
        out3[c][1 : n3 + 1] = jnp.where(lane < Z2 // 2, value, 0.0)
    faces(in3, out3, *coef3, None, 1, n3 + 1, min(S3, n3))


def restrict(fold2, fold1, bufs, n3, y3):
    rows = 2 * n3 * y3
    sums = fold2[pl.ds(0, rows, 2), :] + fold2[pl.ds(1, rows, 2), :]
    fold1[0, 0:rows, :] = dot(sums, pair_matrix(Z2, Z2, 0.5))
    first = first_is_red((1, y3, Z2))

    def body(p):
        a = fold1[0, pl.ds(pl.multiple_of(2 * p * y3, y3), y3), :][None]
        c = fold1[0, pl.ds(pl.multiple_of((2 * p + 1) * y3, y3), y3), :][None]
        here = pl.ds(p + 1, 1)
        bufs[0][here] = jnp.where(first, a, c)
        bufs[1][here] = jnp.where(first, c, a)

    loop(0, n3, 1, body)


def up_kernel(got, got_z, *refs, nx, ny):
    level1, refs = refs[:13], refs[13:]
    level0, refs = refs[:13], refs[13:]
    coef2, diag2, inv2, refs = (
        (refs[0], refs[1:3], refs[3:5], refs[5:7]), refs[7], refs[8:10], refs[10:],
    )
    coef3, inv3, refs = (refs[0], refs[1:3], refs[3:5], refs[5:7]), refs[7:9], refs[9:]
    out, refs = refs[0], refs[1:]

    def split(r):
        return r[0:2], r[2:4], (r[4], r[5:7], r[7:9], r[9:11]), r[11:13]

    v1, b1, coef1, inv1 = split(level1)
    v0, b0, coef0, inv0 = split(level0)
    n2, y2 = 2 * nx, 4 * ny
    n3, y3 = nx, 2 * ny
    v2, b2, v3, b3 = refs[0:2], refs[2:4], refs[4:6], refs[6:8]
    fold2, fold1, fold0 = refs[8], refs[9], refs[10]
    gx_me, gy_me, core = where_am_i()
    unpack(got, got_z, 0, b2, nx, ny)
    step2 = min(S22, n2)
    from_zero(v2, b2, coef2, inv2, 1, n2 + 1, step2)
    first = first_is_red((step2, y2, Z2))

    def body(k):
        here = pl.ds(k, step2)
        res = b2[0][here] - (diag2[here] * v2[0][here] - gathered(v2, 0, *coef2, k, step2, first))
        start = pl.multiple_of((k - 1) * y2, step2 * y2)
        fold2[pl.ds(start, step2 * y2), :] = res.reshape(step2 * y2, Z2)

    loop(1, n2 + 1, step2, body)
    restrict(fold2, fold1, b3, n3, y3)
    from_zero(v3, b3, coef3, inv3, 1, n3 + 1, n3)

    def sweep(i):
        half_sweep(v3, b3, 0, coef3, inv3, 1, n3 + 1, n3)
        half_sweep(v3, b3, 1, coef3, inv3, 1, n3 + 1, n3)

    loop(0, COARSE_SWEEPS - 1, 1, sweep)
    near2 = min(8, n2)
    base = jnp.clip(2 * gx_me - 2, 0, n2 - near2)
    first3 = first_is_red((y3, Z2))
    for p in range(near2 // 2):
        a, c = v3[0][base // 2 + p + 1], v3[1][base // 2 + p + 1]
        fold2[2 * p * y3 : (2 * p + 1) * y3, :] = jnp.where(first3, a, c)
        fold2[(2 * p + 1) * y3 : (2 * p + 2) * y3, :] = jnp.where(first3, c, a)
    twice_rows(fold1, dot(fold2[0 : near2 * y3, :], copy_matrix(Z2, Z2)))
    for k in range(0, near2, 4):
        e = fold1[0, k * y2 : (k + 4) * y2, :].reshape(4, y2, Z2)
        here = pl.ds(base + 1 + k, 4)
        v2[1][here] = v2[1][here] + e
    half_sweep(v2, b2, 0, coef2, inv2, base + 1, base + 1 + near2, near2)
    half_sweep(v2, b2, 1, coef2, inv2, base + 1, base + 1 + near2, near2)
    shift = lax.rem(4 - 4 * gy_me + 2 * y2, y2)
    first1 = first_is_red((y2, Z2))
    cells = []
    for j in range(4):
        a, c = v2[0][2 * gx_me + j], v2[1][2 * gx_me + j]
        for cell in (jnp.where(first1, a, c), jnp.where(first1, c, a)):
            cells.append(pltpu.roll(cell, shift, 0)[0:16])
    twice_rows(fold1, dot(jnp.concatenate(cells, axis=0), copy_matrix(Z2, Z1)))
    for k in range(1, K1 - 1):
        e = columns(fold1, 32 * (k - 1), Y1, Z1)
        v1[1][k] = jnp.where(inv1[1][k] > 0.0, v1[1][k] + e, 0.0)
    half_sweep(v1, b1, 0, coef1, inv1, 1, K1 - 1, S1)
    half_sweep(v1, b1, 1, coef1, inv1, 1, K1 - 1, S1)
    first0 = first_is_red((Y1, Z1))
    cells = []
    for k in range(H - 1, K1 - H + 1):
        a, c = v1[0][k], v1[1][k]
        cells += [jnp.where(first0, a, c), jnp.where(first0, c, a)]
    cells = [cell[4:20] for cell in cells[1:-1]]
    twice_rows(fold0, dot(jnp.concatenate(cells, axis=0), copy_matrix(Z1, Z0, core * 64)))

    def body(p):
        e = columns(fold0, pl.multiple_of(p * 32, 32), 32, Z0)[None]
        here = pl.ds(p + H - 1, 1)
        v0[1][here] = jnp.where(inv0[1][here] > 0.0, v0[1][here] + e, 0.0)

    loop(0, BX // 2 + 2, 1, body)
    half_sweep(v0, b0, 0, coef0, inv0, H - 1, K0 - H + 1, SHB)
    half_sweep(v0, b0, 1, coef0, inv0, H, K0 - H, SH)
    lanes = pl.ds(pl.multiple_of(core * 128, 128), BZ)
    half_first = first_is_red((BY, BZ))

    def body(p):
        a, c = v0[0][p + H, 8:24, lanes], v0[1][p + H, 8:24, lanes]
        out[2 * p] = jnp.where(half_first, a, c)
        out[2 * p + 1] = jnp.where(half_first, c, a)

    loop(0, BX // 2, 1, body)


def shape(*dims):
    return jax.ShapeDtypeStruct(dims, F32)


def scratch(*dims):
    return pltpu.VMEM(dims, F32)


def ring(x, axis, step):
    n = lax.axis_size(axis)
    return lax.ppermute(x, axis, [(i, (i + step) % n) for i in range(n)])


def swap(x):
    return lax.ppermute(x, "gz", [(0, 1), (1, 0)])


def gather(send, nx, ny):
    got = lax.all_to_all(send, "gy", 0, 0, tiled=True)
    (send,) = call(spread_kernel, "spread", 4, [(nx,) + got.shape], [], got)
    return lax.all_to_all(send, "gx", 0, 0, tiled=True).reshape((nx * ny,) + got.shape[1:])


def call(kernel, name, mib, outs, scratches, *args, hbm_in=0, hbm_out=0):
    return pl.pallas_call(
        kernel,
        out_shape=tuple(shape(*o) for o in outs),
        in_specs=[HBM] * hbm_in + [VMEM] * (len(args) - hbm_in),
        out_specs=(HBM,) * hbm_out + (VMEM,) * (len(outs) - hbm_out),
        scratch_shapes=[scratch(*s) if isinstance(s, tuple) else s for s in scratches],
        compiler_params=params(mib),
        name=name,
    )(*args)


def on_device(membrane, recovery, extracellular, fiber_scale, labels):
    nx, ny = lax.axis_size("gx"), lax.axis_size("gy")
    block = (BX, BY, BZ)
    held = [
        pltpu.with_memory_space_constraint(x, pltpu.HBM)
        for x in (membrane, recovery, extracellular, fiber_scale, labels)
    ]
    own, xup, xdn, yup, ydn = call(
        prep_kernel, "prep", 6,
        [(AT_MEAN + 2, BY, BZ)] + [(18, BY, BZ)] * 4,
        [block] * 4
        + [pltpu.VMEM(labels.shape, jnp.int32), (1, 128, 128), pltpu.SemaphoreType.DMA((5,))],
        *held, hbm_in=5,
    )
    xlo, xhi = ring(xup, "gx", 1), ring(xdn, "gx", -1)
    ylo, yhi = ring(yup, "gy", 1), ring(ydn, "gy", -1)
    cup, cdn = call(corner_kernel, "corner", 4, [(16, 8, BZ)] * 2, [], xlo, xhi)
    clo, chi = lax.optimization_barrier((ring(cup, "gy", 1), ring(cdn, "gy", -1)))
    halos = []
    for piece in (own, xlo, xhi, ylo, yhi, clo, chi):
        halos += [piece, swap(piece)]
    (seed,) = call(seed_kernel, "seed", 4, [(8, Z2)], [(1, 32, 128)], own)
    fine = (K0, Y0, Z0)
    mid = (K1, Y1, Z1)
    grid2, grid3 = (2 * nx + 2, 4 * ny, Z2), (nx + 2, 2 * ny, Z2)
    mnext, rhs1, rup, rdn, in1r, in1b, *level0 = call(
        fine_kernel, "fine", 20,
        [block, (2, 4, 8, Z1), (2, 2, 8, Z1), (2, 2, 8, Z1)] + [mid] * 2 + [fine] * 13,
        [fine] * 16
        + [(8, BY, Z0), (2, 128, 128), block, pltpu.SemaphoreType.DMA((1,))],
        *halos, hbm_out=1,
    )
    rnext, *coef1 = call(
        middle_faces_kernel, "middle_faces", 4, [block] + [mid] * 10,
        [mid] * 2 + [block] * 2 + [pltpu.SemaphoreType.DMA((2,))],
        held[0], held[1], in1r, in1b, hbm_in=2, hbm_out=1,
    )
    part = (2, 2, 16, Z1)
    wide, xup, xdn = call(
        join_kernel, "join", 4, [(2, 4, 16, Z1), part, part], [],
        ring(rup, "gy", 1), rhs1, ring(rdn, "gy", -1),
    )
    low, high = ring(xup, "gx", 1), ring(xdn, "gx", -1)
    v1r, v1b, b1r, b1b, send = call(
        middle_kernel, "middle", 4,
        [mid] * 4 + [(ny, 16, Z2)],
        [(32, Z1), (1, 32, 128)],
        low, wide, high, seed, *coef1,
    )
    got = gather(send, nx, ny)
    got_z = swap(got)
    coarse = call(
        lambda *refs: coarse_kernel(*refs, nx=nx, ny=ny), "coarse", 8,
        [grid2] * 10 + [grid3] * 9,
        [grid2] * 4 + [grid3] * 4 + [(8 * nx * ny, Z2), (1, 4 * nx * ny, Z2)],
        got, got_z,
    )
    level1 = [v1r, v1b, b1r, b1b, *coef1[:7], *coef1[8:]]
    (enext,) = call(
        lambda *refs: up_kernel(*refs, nx=nx, ny=ny), "up", 10,
        [block],
        [grid2] * 4 + [grid3] * 4
        + [(8 * nx * ny, Z2), (2, max(4 * nx * ny, 256), Z2), (3, 320, 128)],
        got, got_z, *level1, *level0, *coarse,
    )
    return mnext, rnext, enext


def solution(mesh):
    spec = P("gx", "gy", "gz")
    return jax.shard_map(
        on_device, mesh=mesh, in_specs=(spec,) * 5, out_specs=(spec,) * 3, check_vma=False
    )
```

```python
import jax
import jax.numpy as jnp
from jax import lax
from jax.experimental import pallas as pl
from jax.experimental.pallas import tpu as pltpu
from jax.sharding import PartitionSpec as P

TIME_STEP = 0.05
IONIC_GAIN = 8.0
IONIC_ONSET = 0.15
RECOVERY_RATE = 0.01
COARSE_SWEEPS = 8

F32 = jnp.float32
BX, BY, BZ = 16, 16, 256
H = 3
SF, SI, SH, SHB, S1, S2, SU, S22, S3 = 3, 4, 4, 5, 8, 8, 8, 16, 16
AT_IN, AT_W, AT_U, AT_MEAN = BX, 2 * BX, 3 * BX, 3 * BX + BX // 2
K0, Y0, Z0 = BX // 2 + 2 * H, 32, 384
K1, Y1, Z1 = BX // 4 + 2 * H, 24, BZ
Z2 = BZ // 2
VMEM = pl.BlockSpec(memory_space=pltpu.VMEM)
HBM = pl.BlockSpec(memory_space=pltpu.HBM)


def params(mib):
    return pltpu.CompilerParams(vmem_limit_bytes=mib * 1024 * 1024)


def iota(shape, dim):
    return lax.broadcasted_iota(jnp.int32, shape, dim)


def first_is_red(shape):
    return ((iota(shape, len(shape) - 2) + iota(shape, len(shape) - 1)) & 1) == 0


def up(x, axis):
    return pltpu.roll(x, x.shape[axis] - 1, axis)


def down(x, axis):
    return pltpu.roll(x, 1, axis)


def pair_matrix(rows, cols, value, shift=0):
    return jnp.where(
        iota((rows, cols), 0) // 2 + shift == iota((rows, cols), 1), value, 0.0
    ).astype(F32)


def copy_matrix(rows, cols, shift=0):
    return jnp.where(
        iota((rows, cols), 1) // 2 + shift == iota((rows, cols), 0), 1.0, 0.0
    ).astype(F32)


def dot(a, b):
    b = b.astype(jnp.bfloat16)
    high = a.astype(jnp.bfloat16)
    rest = a - high.astype(F32)
    mid = rest.astype(jnp.bfloat16)
    low = (rest - mid.astype(F32)).astype(jnp.bfloat16)
    parts = [jnp.dot(p, b, preferred_element_type=F32) for p in (low, mid, high)]
    return parts[0] + parts[1] + parts[2]


def sum_rows(buf, x):
    rows, cols = x.shape
    sums = []
    for c in range(cols // 128):
        buf[c, 0:rows, :] = x[:, 128 * c : 128 * c + 128]
        sums.append(buf[c, pl.ds(0, rows // 2, 2), :] + buf[c, pl.ds(1, rows // 2, 2), :])
    return sums[0] if len(sums) == 1 else jnp.concatenate(sums, axis=1)


def twice_rows(buf, x):
    rows, cols = x.shape
    for c in range(cols // 128):
        for k in (0, 1):
            buf[c, pl.ds(k, rows, 2), :] = x[:, 128 * c : 128 * c + 128]


def columns(buf, start, rows, cols):
    parts = [buf[c, pl.ds(start, rows), :] for c in range(cols // 128)]
    return parts[0] if len(parts) == 1 else jnp.concatenate(parts, axis=1)


def loop(start, stop, step, body):
    if not isinstance(start, int) or stop - start == step:
        body(start)
        return

    def run(index, carry):
        body(start + index * step)
        return carry

    lax.fori_loop(0, (stop - start) // step, run, 0)


def far(other, k, step, red, first):
    before, after = other[pl.ds(k - 1, step)], other[pl.ds(k + 1, step)]
    return jnp.where(first, before, after) if red else jnp.where(first, after, before)


def faces(inner, outer, near, fars, ys, zs, diag, inv, least, start, stop, step):
    rows, lanes = inner[0].shape[1:]
    shape = (step, rows, lanes)
    row, lane = iota(shape, 1), iota(shape, 2)
    first = first_is_red(shape)

    def body(k):
        here = pl.ds(k, step)
        low = jnp.minimum(inner[0][here], inner[1][here])
        if least is not None:
            least[0][here] = low
        halves = [0.5 * outer[c][here] for c in (0, 1)]
        pair = low + halves[0] + halves[1]
        near[here] = pair
        totals = [pair, pair]
        for axis, out, keep, place, size in (
            (1, ys, None if least is None else least[2], row, rows),
            (2, zs, None if least is None else least[3], lane, lanes),
        ):
            full = []
            for c in (0, 1):
                o = 1 - c
                mine = inner[c][here]
                low = jnp.where(place < size - 1, jnp.minimum(mine, up(inner[o][here], axis)), 0.0)
                if keep is not None:
                    keep[c][here] = low
                both = low + halves[c] + jnp.where(place < size - 1, up(halves[o], axis), 0.0)
                full.append(both)
                out[c][here] = jnp.where(place < size - 1, both, 0.0)
            for c in (0, 1):
                below = jnp.where(place > 0, down(full[1 - c], axis), halves[c])
                totals[c] = totals[c] + full[c] + below
        for c in (0, 1):
            o = 1 - c
            low = jnp.minimum(inner[c][here], far(inner[o], k, step, c == 0, first))
            if least is not None:
                least[1][c][here] = low
            both = low + halves[c] + 0.5 * far(outer[o], k, step, c == 0, first)
            fars[c][here] = both
            total = totals[c] + both
            if c == 0 and diag is not None:
                diag[here] = total
            inside = outer[c][here] > 0.0
            inv[c][here] = jnp.where(inside, 1.0 / jnp.where(inside, total, 1.0), 0.0)

    loop(start, stop, step, body)


def gathered(v, c, near, fars, ys, zs, k, step, first):
    here = pl.ds(k, step)
    o = 1 - c
    other = v[o][here]
    total = near[here] * other + fars[c][here] * far(v[o], k, step, c == 0, first)
    total = total + ys[c][here] * up(other, 1) + down(ys[o][here] * other, 1)
    return total + zs[c][here] * up(other, 2) + down(zs[o][here] * other, 2)


def half_sweep(v, b, c, coef, inv, start, stop, step):
    first = first_is_red((step,) + tuple(v[0].shape[1:]))

    def body(k):
        here = pl.ds(k, step)
        v[c][here] = (b[c][here] + gathered(v, c, *coef, k, step, first)) * inv[c][here]

    loop(start, stop, step, body)


def from_zero(v, b, coef, inv, start, stop, step):
    count = v[0].shape[0]
    for c in (0, 1):
        v[c][0:1] = jnp.zeros_like(v[c][0:1])
        v[c][count - 1 :] = jnp.zeros_like(v[c][0:1])

    def body(k):
        here = pl.ds(k, step)
        v[0][here] = b[0][here] * inv[0][here]

    loop(start, stop, step, body)
    half_sweep(v, b, 1, coef, inv, start, stop, step)


def put(bufs, k, rows, lanes, a, b):
    some = a if b is None else b
    a = jnp.zeros_like(some) if a is None else a
    b = jnp.zeros_like(some) if b is None else b
    first = first_is_red(some.shape)
    bufs[0][k, rows, lanes] = jnp.where(first, a, b)
    bufs[1][k, rows, lanes] = jnp.where(first, b, a)


def colours(x):
    n = x.shape[0] // 2
    first = first_is_red(x.shape[1:])
    pairs = [(x[2 * p], x[2 * p + 1]) for p in range(n)]
    return (
        jnp.stack([jnp.where(first, a, b) for a, b in pairs]),
        jnp.stack([jnp.where(first, b, a) for a, b in pairs]),
    )


def where_am_i():
    return lax.axis_index("gx"), lax.axis_index("gy"), lax.axis_index("gz")


def flags():
    gx, gy, _ = where_am_i()
    return (
        (gx > 0).astype(F32),
        (gx < lax.axis_size("gx") - 1).astype(F32),
        (gy > 0).astype(F32),
        (gy < lax.axis_size("gy") - 1).astype(F32),
    )


def fetch(pairs, sems):
    copies = [pltpu.make_async_copy(src, dst, sems.at[i]) for i, (src, dst) in enumerate(pairs)]
    for copy in copies:
        copy.start()
    return copies


def outside(shape, own_rows, k, own, has):
    row = iota(shape, len(shape) - 2)
    in_y = jnp.where(row < 8, has[2], jnp.where(row < 8 + own_rows, 1.0, has[3]))
    return in_y * jnp.where(k < H, has[0], jnp.where(k < H + own, 1.0, has[1]))


def block_of(i):
    rows, lanes = 8 * ((i % 4) // 2), 128 * (i % 2)
    return i // 4, slice(rows, rows + 8), slice(lanes, lanes + 128)


def prep_kernel(
    m_in, r_in, u_in, f_in, labels_in, own, xup, xdn, yup, ydn, m, r, u, f, labels, fold, sems
):
    copies = fetch(
        [(labels_in, labels), (m_in, m), (u_in, u), (r_in, r), (f_in, f)], sems
    )
    for copy in copies:
        copy.wait()
    spread = jnp.where(iota((BZ // 8, BZ), 1) // 8 == iota((BZ // 8, BZ), 0), 1.0, 0.0).astype(F32)
    for bx in range(BX // 8):
        wide = jnp.dot(labels[bx].astype(F32), spread, preferred_element_type=F32)
        kind = jnp.concatenate(
            [jnp.broadcast_to(wide[by : by + 1], (8, BZ)) for by in range(BY // 8)], axis=0
        )
        factor = jnp.where(kind > 1.5, 0.3, jnp.where(kind > 0.5, 1.0, 0.0)).astype(F32)
        for x in range(8 * bx, 8 * bx + 8):
            mm, rr, uu = m[x], r[x], u[x]
            inner = factor * f[x]
            own[x] = mm + uu
            own[AT_IN + x] = inner
            ionic = IONIC_GAIN * mm * (mm - IONIC_ONSET) * (mm - 1.0) + mm * rr
            own[AT_W + x] = mm - jnp.where(kind > 0.5, TIME_STEP * ionic, 0.0)
            if x % 2:
                first = first_is_red((BY, BZ))
                own[AT_U + x // 2] = jnp.where(first, uu, u[x - 1])
    sums = jnp.concatenate(
        [own[AT_IN + 2 * p] + own[AT_IN + 2 * p + 1] for p in range(BX // 2)], axis=0
    )
    mean = sum_rows(fold, dot(sums, pair_matrix(BZ, BZ // 2, 0.125)))
    for i in range(8):
        slab, rows, lanes = block_of(i)
        for ref, base in ((own, AT_MEAN), (yup, BX), (ydn, BX)):
            ref[base + slab, rows, lanes] = mean[8 * i : 8 * i + 8]
    for i in range(5):
        slab, rows, lanes = block_of(i)
        xup[16 + slab, rows, lanes] = mean[8 * (3 + i) : 8 * (4 + i)]
        xdn[16 + slab, rows, lanes] = mean[8 * i : 8 * i + 8]
    base = 0
    for start, count, depth in ((0, BX, 5), (AT_IN, BX, 5), (AT_W, BX, 4), (AT_U, BX // 2, 2)):
        xup[base : base + depth] = own[start + count - depth : start + count]
        xdn[base : base + depth] = own[start : start + depth]
        base += depth
    row = iota((8, BZ), 0)
    turn = lambda x, by: pltpu.roll(x, by % 8, 0)
    for p in range(BX // 2):
        for out, rows, keep, by, fourth in (
            (yup, slice(8, 16), row >= 3, 3, (4, 5, 6)),
            (ydn, slice(0, 8), row < 5, 5, (2, 3, 4)),
        ):
            s = [own[2 * p + i, rows] for i in (0, 1)]
            n = [own[AT_IN + 2 * p + i, rows] for i in (0, 1)]
            rest = [own[AT_W + 2 * p, rows], own[AT_W + 2 * p + 1, rows], own[AT_U + p, rows]]
            at = 0 if out is yup else 5
            last = jnp.where(
                row == at,
                turn(rest[0], fourth[0]),
                jnp.where(row == at + 1, turn(rest[1], fourth[1]), turn(rest[2], fourth[2])),
            )
            out[2 * p, 0:8] = jnp.where(keep, s[0], turn(rest[0], by))
            out[2 * p, 8:16] = jnp.where(keep, s[1], turn(rest[1], by))
            out[2 * p + 1, 0:8] = jnp.where(keep, n[0], turn(rest[2], by))
            out[2 * p + 1, 8:16] = jnp.where(keep, n[1], last)


def merge(high, a, b):
    row = iota(a.shape, 0)
    return jnp.where(row >= 4, a, pltpu.roll(b, 4, 0)) if high else jnp.where(
        row < 4, a, pltpu.roll(b, 4, 0)
    )


def corner_kernel(xlo, xhi, cup, cdn):
    for high, out in ((True, cup), (False, cdn)):
        rows = slice(8, 16) if high else slice(0, 8)
        edge = iota((8, BZ), 0) == (7 if high else 0)
        for side, src in ((0, xlo), (1, xhi)):
            at = lambda base, depth, d: src[base + (depth - d if side == 0 else d - 1), rows]
            s, n, w = (
                lambda d: at(0, 5, d),
                lambda d: at(5, 5, d),
                lambda d: at(10, 4, d),
            )
            u = lambda d: at(14, 2, d)
            tiles = [
                merge(high, s(1), s(2)),
                merge(high, s(3), s(4)),
                merge(high, n(1), n(2)),
                merge(high, n(3), n(4)),
                merge(high, w(1), w(2)),
                merge(high, jnp.where(edge, w(3), pltpu.roll(u(2), 7 if high else 1, 0)), u(1)),
            ]
            for t, tile in enumerate(tiles):
                out[8 * side + t] = tile

            def coarse(d):
                slab, block_rows, lanes = block_of(5 - d if side == 0 else d - 1)
                return src[16 + slab, block_rows, lanes]

            halves = (
                coarse(1),
                merge(high, coarse(2), coarse(3)),
                merge(high, coarse(4), coarse(5)),
            )
            for i, half in enumerate(halves):
                lanes = 128 * (i % 2)
                out[8 * side + 6 + i // 2, :, lanes : lanes + 128] = half
            out[8 * side + 7, :, 128:256] = halves[2]


def fine_kernel(*refs):
    pieces, refs = refs[:14], refs[14:]
    mnext, rhs1, rup, rdn, refs = refs[0], refs[1], refs[2], refs[3], refs[4:]
    mean1, refs = refs[0:2], refs[2:]
    v, b, near, fars, ys, zs, inv, refs = (
        refs[0:2], refs[2:4], refs[4], refs[5:7], refs[7:9], refs[9:11], refs[11:13], refs[13:],
    )
    inner, outer, s, w, refs = refs[0:2], refs[2:4], refs[4:6], refs[6:8], refs[8:]
    low_near, low_far, low_y, low_z, diag, fold, fold2 = (
        refs[0], refs[1:3], refs[3:5], refs[5:7], refs[7], refs[8], refs[9],
    )
    mout, sems = refs[10], refs[11]
    core = lax.axis_index("gz")
    has = flags()
    fields = (s, inner, w)
    for side in (0, 1):
        own, xlo, xhi, ylo, yhi, clo, chi = pieces[side::2]
        wide = BZ if side == 0 else 128
        src = pl.ds(0 if side == 0 else pl.multiple_of(core * 128, 128), wide)
        dst = pl.ds(pl.multiple_of(core * 128 if side == 0 else (1 - core) * 256, 128), wide)
        mid, low, high = slice(8, 24), slice(0, 8), slice(24, 32)

        def body(p, own=own, ylo=ylo, yhi=yhi, src=src, dst=dst):
            k = p + H
            for q, bufs in enumerate(fields):
                put(bufs, k, mid, dst, own[BX * q + 2 * p, :, src], own[BX * q + 2 * p + 1, :, src])
            v[1][k, mid, dst] = own[AT_U + p, :, src]
            row = iota((8, wide), 0)
            turn = lambda x, by: pltpu.roll(x, by, 0)
            for rows, ref, flag, keep, deep, by, fourth in (
                (low, ylo, has[2], row >= 3, row >= 5, 5, (4, 3, 2)),
                (high, yhi, has[3], row < 5, row < 3, 3, (6, 5, 4)),
            ):
                t = [
                    ref[2 * p + i // 2, 8 * (i % 2) : 8 * (i % 2) + 8, src] * flag for i in range(4)
                ]
                put(s, k, rows, dst, t[0], t[1])
                put(inner, k, rows, dst, jnp.where(keep, t[2], 0.0), jnp.where(keep, t[3], 0.0))
                rest = [
                    jnp.where(deep, turn(t[i], by), turn(t[3], fourth[i])) for i in (0, 1, 2)
                ]
                put(w, k, rows, dst, rest[0], rest[1])
                v[1][k, rows, dst] = rest[2]

        loop(0, BX // 2, 1, body)
        for x_side, ref, flag in ((0, xlo, has[0]), (1, xhi, has[1])):
            base = 0
            order = (5, 4, 3, 2, 1) if x_side == 0 else (1, 2, 3, 4, 5)
            for q, depth in enumerate((5, 5, 4)):
                slabs = {d: ref[base + i, :, src] * flag for i, d in enumerate(
                    [d for d in order if d <= depth])}
                base += depth
                for j in range(H):
                    near_d, far_d = 2 * j + 1, 2 * j + 2
                    pair = (slabs.get(near_d), slabs.get(far_d))
                    k = H - 1 - j if x_side == 0 else K0 - H + j
                    if x_side == 0:
                        pair = pair[::-1]
                    if pair[0] is None and pair[1] is None:
                        pair = (jnp.zeros((16, wide), F32), None)
                    put(fields[q], k, mid, dst, *pair)
            black = [ref[14, :, src] * flag, ref[15, :, src] * flag, jnp.zeros((16, wide), F32)]
            if x_side == 0:
                black[0], black[1] = black[1], black[0]
            for j in range(H):
                v[1][H - 1 - j if x_side == 0 else K0 - H + j, mid, dst] = black[j]
            for rows, cref, yflag in ((low, clo, has[2]), (high, chi, has[3])):
                both = flag * yflag
                tile = [cref[8 * x_side + t, :, src] * both for t in range(6)]
                turned = [pltpu.roll(t, 4, 0) for t in tile]
                zero = jnp.zeros((8, wide), F32)
                by_field = (
                    (tile[0], turned[0], tile[1], turned[1]),
                    (tile[2], turned[2], tile[3], turned[3]),
                    (tile[4], turned[4], tile[5], zero),
                )
                last = pltpu.roll(tile[5], 1 if cref is clo else 7, 0)
                black = (turned[5], last, zero)
                for j in range(H):
                    v[1][H - 1 - j if x_side == 0 else K0 - H + j, rows, dst] = black[j]
                for q in range(3):
                    slabs = by_field[q] + (zero, zero)
                    for j in range(H):
                        pair = (slabs[2 * j], slabs[2 * j + 1])
                        k = H - 1 - j if x_side == 0 else K0 - H + j
                        put(fields[q], k, rows, dst, *(pair[::-1] if x_side == 0 else pair))
        dst = pl.ds(pl.multiple_of((core if side == 0 else 1 - core) * 128, 128), 128)
        for p in range(4):
            def of_own(i):
                slab, rows, lanes = block_of(i)
                return own[AT_MEAN + slab, rows, lanes]

            put(mean1, p + H, slice(8, 16), dst, of_own(2 * p), of_own(2 * p + 1))
            for rows, ref, flag in ((slice(0, 8), ylo, has[2]), (slice(16, 24), yhi, has[3])):
                def of_y(i):
                    slab, part, lanes = block_of(i)
                    return ref[BX + slab, part, lanes] * flag

                put(mean1, p + H, rows, dst, of_y(2 * p), of_y(2 * p + 1))
        for x_side, ref, flag in ((0, xlo, has[0]), (1, xhi, has[1])):
            def of_x(d):
                slab, part, lanes = block_of(5 - d if x_side == 0 else d - 1)
                return ref[16 + slab, part, lanes] * flag

            zero = jnp.zeros((8, 128), F32)
            mids = [of_x(d) for d in (1, 2, 3, 4, 5)] + [zero]
            columns_of = [(slice(8, 16), mids)]
            for rows, cref, yflag in ((slice(0, 8), clo, has[2]), (slice(16, 24), chi, has[3])):
                h = [
                    cref[8 * x_side + 6 + i // 2, :, 128 * (i % 2) : 128 * (i % 2) + 128]
                    * (flag * yflag)
                    for i in range(3)
                ]
                t = [h[0], h[1], pltpu.roll(h[1], 4, 0), h[2], pltpu.roll(h[2], 4, 0)]
                columns_of.append((rows, t + [zero]))
            for rows, slabs in columns_of:
                for j in range(H):
                    pair = (slabs[2 * j], slabs[2 * j + 1])
                    k = H - 1 - j if x_side == 0 else K1 - H + j
                    put(mean1, k, rows, dst, *(pair[::-1] if x_side == 0 else pair))

    def body(k):
        here = pl.ds(k, 1)
        inside = outside((1, Y0, Z0), 16, k, BX // 2, has)
        for c in (0, 1):
            outer[c][here] = jnp.where(inner[c][here] > 0.0, 1.0, 3.0 * inside)

    loop(0, K0, 1, body)
    faces(
        inner, outer, near, fars, ys, zs, diag, inv, (low_near, low_far, low_y, low_z), 1, K0 - 1, SF
    )
    first = first_is_red((SI, Y0, Z0))

    def intra(x, k):
        here = pl.ds(k, SI)
        a = [x[0][here], x[1][here]]
        flow = low_near[here] * (a[1] - a[0])
        total = [flow, -flow]
        for c in (0, 1):
            total[c] = total[c] + low_far[c][here] * (far(x[1 - c], k, SI, c == 0, first) - a[c])
        for axis, low in ((1, low_y), (2, low_z)):
            flows = [low[c][here] * (up(a[1 - c], axis) - a[c]) for c in (0, 1)]
            for c in (0, 1):
                total[c] = total[c] + flows[c] - down(flows[1 - c], axis)
        return total

    def body(k):
        here = pl.ds(k, SI)
        drive = intra(s, k)
        for c in (0, 1):
            w[c][here] = w[c][here] + TIME_STEP * drive[c]

    loop(1, K0 - 1, SI, body)
    lanes = pl.ds(pl.multiple_of(core * 128, 128), BZ)
    half_first = first_is_red((BY, BZ))

    def body(p):
        a, c = w[0][p + H, 8:24, lanes], w[1][p + H, 8:24, lanes]
        mout[2 * p] = jnp.where(half_first, a, c)
        mout[2 * p + 1] = jnp.where(half_first, c, a)

    loop(0, BX // 2, 1, body)
    copies = fetch([(mout, mnext)], sems)

    def body(k):
        here = pl.ds(k, SI)
        both = intra(w, k)
        for c in (0, 1):
            b[c][here] = both[c]

    loop(1, K0 - 1, SI, body)
    coef = (near, fars, ys, zs)
    half_sweep(v, b, 0, coef, inv, 1, K0 - 1, SH)
    half_sweep(v, b, 1, coef, inv, 2, K0 - 2, SHB)
    first = first_is_red((SH, Y0, Z0))

    def body(p):
        here = pl.ds(p + H, SH)
        res = b[0][here] - (diag[here] * v[0][here] - gathered(v, 0, *coef, p + H, SH, first))
        fold[pl.ds(p, SH)] = res[:, 8:24, :]

    loop(0, BX // 2, SH, body)
    half = BX // 2 * BY
    pairs = pair_matrix(Z0, Z1, 0.5, core * 64)
    coarse = sum_rows(fold2, dot(fold[...].reshape(half, Z0), pairs)).reshape(8, 8, Z1)
    red, black = colours(coarse)
    for c, pairs in ((0, red), (1, black)):
        rhs1[c] = pairs
        for j in (0, 1):
            rup[c, j] = merge(True, pairs[2 * j], pairs[2 * j + 1])
            rdn[c, j] = merge(False, pairs[2 * j], pairs[2 * j + 1])
    copies[0].wait()


def middle_faces_kernel(m_in, r_in, *refs):
    inner, refs = refs[0:2], refs[2:]
    rnext, near, fars, ys, zs, diag, inv, outer = (
        refs[0], refs[1], refs[2:4], refs[4:6], refs[6:8], refs[8], refs[9:11], refs[11:13],
    )
    m, r, sems = refs[13:]
    copies = fetch([(m_in, m), (r_in, r)], sems)
    has = flags()
    for k in range(K1):
        inside = outside((Y1, Z1), 8, k, 4, has)
        for c in (0, 1):
            outer[c][k] = jnp.where(inner[c][k] > 0.0, 1.0, 3.0 * inside)
    for copy in copies:
        copy.wait()
    for x in range(BX):
        mm, rr = m[x], r[x]
        r[x] = rr + TIME_STEP * RECOVERY_RATE * (
            -rr - IONIC_GAIN * mm * (mm - IONIC_ONSET - 1.0)
        )
    copies = fetch([(r, rnext)], sems)
    faces(inner, outer, near, fars, ys, zs, diag, inv, None, 1, K1 - 1, S1)
    copies[0].wait()


def join_kernel(low, own, high, wide, xup, xdn):
    row = iota((8, Z1), 0)
    for c in (0, 1):
        for p in range(4):
            a, b = low[c, p // 2], high[c, p // 2]
            edge = jnp.where(row >= 4, a, b) if p % 2 == 0 else pltpu.roll(
                jnp.where(row < 4, a, b), 4, 0
            )
            for ref, q in ((wide, p), (xdn, p) if p < 2 else (xup, p - 2)):
                ref[c, q, 0:8] = edge
                ref[c, q, 8:16] = own[c, p]


def spread_kernel(got, send):
    whole = got[...]
    for d in range(send.shape[0]):
        send[d] = whole


def middle_kernel(low, own, high, seed, *refs):
    near, fars, ys, zs, diag, inv, refs = (
        refs[0], refs[1:3], refs[3:5], refs[5:7], refs[7], refs[8:10], refs[10:],
    )
    v, b, send, fold, fold2 = refs[0:2], refs[2:4], refs[4], refs[5], refs[6]
    core = lax.axis_index("gz")
    has = flags()
    for c in (0, 1):
        b[c][0:1] = jnp.zeros((1, Y1, Z1), F32)
        b[c][K1 - 1 :] = jnp.zeros((1, Y1, Z1), F32)
        for k in range(1, K1 - 1):
            src = low[c, k - 1] if k < H else (own[c, k - H] if k < H + 4 else high[c, k - H - 4])
            inside = outside((Y1, Z1), 8, k, 4, has)
            for rows, part in ((slice(0, 8), src[0:8]), (slice(8, 16), src[8:16]), (slice(16, 24), src[0:8])):
                b[c][k, rows] = part * inside[rows]
    coef = (near, fars, ys, zs)
    from_zero(v, b, coef, inv, 1, K1 - 1, S1)
    first = first_is_red((2, Y1, Z1))
    for p in (0, 2):
        here = slice(p + H, p + H + 2)
        res = b[0][here] - (diag[here] * v[0][here] - gathered(v, 0, *coef, p + H, 2, first))
        fold[8 * p : 8 * p + 16] = res[:, 8:16, :].reshape(16, Z1)
    both = sum_rows(fold2, dot(fold[...], pair_matrix(Z1, Z2, 0.5)))
    red, black = colours(both.reshape(4, 4, Z2))
    red, black = red.reshape(8, Z2), black.reshape(8, Z2)
    mine = (iota((8, Z2), 1) < 64) == (core == 0)
    piece = in_order(jnp.where(mine, red, pltpu.roll(black, 64, 1)))
    for d in range(send.shape[0]):
        send[d, 0:8] = piece
        send[d, 8:16] = seed[...]


def in_order(piece):
    odd = (iota(piece.shape, 0) * 0 + lax.axis_index("gy")) & 1
    return jnp.where(odd == 1, pltpu.roll(piece, 4, 0), piece)


def seed_kernel(own, send, fold):
    sums = []
    for p in range(4):
        total = None
        for i in (2 * p, 2 * p + 1):
            slab, rows, lanes = block_of(i)
            block = own[AT_MEAN + slab, rows, lanes]
            total = block if total is None else total + block
        sums.append(total)
    both = sum_rows(fold, dot(jnp.concatenate(sums, axis=0), pair_matrix(Z2, Z2, 0.125)))
    red, black = colours(both.reshape(4, 4, Z2))
    red, black = red.reshape(8, Z2), black.reshape(8, Z2)
    core = lax.axis_index("gz")
    lane = iota((8, Z2), 1) + core * 0
    lower = jnp.where(lane < 64, red, pltpu.roll(black, 64, 1))
    upper = jnp.where(lane < 64, black, pltpu.roll(red, 64, 1))
    send[...] = in_order(jnp.where(core == 0, lower, upper))


def unpack(got, got_z, part, bufs, nx, ny):
    core = lax.axis_index("gz")
    mine = (iota((8, Z2), 1) < 64) == (core == 0)
    upper = iota((8, Z2), 0) < 4

    def body(start):
      for gx in [start + i for i in range(min(SU, nx))]:
        for t in range(ny // 2):
            d = gx * ny + 2 * t
            tiles = []
            for src in (got, got_z):
                even, odd = src[d, part : part + 8], src[d + 1, part : part + 8]
                tiles.append(
                    (
                        jnp.where(upper, even, odd),
                        pltpu.roll(jnp.where(upper, odd, even), 4, 0),
                    )
                )
            for p in (0, 1):
                a, c = tiles[0][p], tiles[1][p]
                rows = slice(8 * t, 8 * t + 8)
                bufs[0][1 + 2 * gx + p, rows, :] = jnp.where(mine, a, c)
                bufs[1][1 + 2 * gx + p, rows, :] = pltpu.roll(jnp.where(mine, c, a), 64, 1)

    loop(0, nx, min(SU, nx), body)


def coarse_kernel(got, got_z, *refs, nx, ny):
    n2, y2, n3, y3 = 2 * nx, 4 * ny, nx, 2 * ny
    coef2, refs = (refs[0], refs[1:3], refs[3:5], refs[5:7], refs[7], refs[8:10]), refs[10:]
    coef3, refs = (refs[0], refs[1:3], refs[3:5], refs[5:7], None, refs[7:9]), refs[9:]
    in2, out2, in3, out3, fold2, fold1 = (
        refs[0:2], refs[2:4], refs[4:6], refs[6:8], refs[8], refs[9],
    )
    unpack(got, got_z, 8, in2, nx, ny)

    def body(k):
        here = pl.ds(k, 4)
        for c in (0, 1):
            out2[c][here] = jnp.where(in2[c][here] > 0.0, 1.0, 3.0)
        total = 0.25 * (in2[0][here] + in2[1][here])
        fold2[pl.ds(pl.multiple_of((k - 1) * y2, 4 * y2), 4 * y2), :] = total.reshape(4 * y2, Z2)

    loop(1, n2 + 1, 4, body)
    for bufs, count in ((in2, n2), (out2, n2), (in3, n3), (out3, n3)):
        for c in (0, 1):
            bufs[c][0:1] = jnp.zeros_like(bufs[c][0:1])
            bufs[c][count + 1 :] = jnp.zeros_like(bufs[c][0:1])
    faces(in2, out2, *coef2, None, 1, n2 + 1, min(S2, n2))
    restrict(fold2, fold1, in3, n3, y3)
    lane = iota((n3, y3, Z2), 2)
    for c in (0, 1):
        value = jnp.where(in3[c][1 : n3 + 1] > 0.0, 1.0, 3.0)
        out3[c][1 : n3 + 1] = jnp.where(lane < Z2 // 2, value, 0.0)
    faces(in3, out3, *coef3, None, 1, n3 + 1, min(S3, n3))


def restrict(fold2, fold1, bufs, n3, y3):
    rows = 2 * n3 * y3
    sums = fold2[pl.ds(0, rows, 2), :] + fold2[pl.ds(1, rows, 2), :]
    fold1[0, 0:rows, :] = dot(sums, pair_matrix(Z2, Z2, 0.5))
    first = first_is_red((1, y3, Z2))

    def body(p):
        a = fold1[0, pl.ds(pl.multiple_of(2 * p * y3, y3), y3), :][None]
        c = fold1[0, pl.ds(pl.multiple_of((2 * p + 1) * y3, y3), y3), :][None]
        here = pl.ds(p + 1, 1)
        bufs[0][here] = jnp.where(first, a, c)
        bufs[1][here] = jnp.where(first, c, a)

    loop(0, n3, 1, body)


def up_kernel(got, got_z, *refs, nx, ny):
    level1, refs = refs[:13], refs[13:]
    level0, refs = refs[:13], refs[13:]
    coef2, diag2, inv2, refs = (
        (refs[0], refs[1:3], refs[3:5], refs[5:7]), refs[7], refs[8:10], refs[10:],
    )
    coef3, inv3, refs = (refs[0], refs[1:3], refs[3:5], refs[5:7]), refs[7:9], refs[9:]
    out, refs = refs[0], refs[1:]

    def split(r):
        return r[0:2], r[2:4], (r[4], r[5:7], r[7:9], r[9:11]), r[11:13]

    v1, b1, coef1, inv1 = split(level1)
    v0, b0, coef0, inv0 = split(level0)
    n2, y2 = 2 * nx, 4 * ny
    n3, y3 = nx, 2 * ny
    v2, b2, v3, b3 = refs[0:2], refs[2:4], refs[4:6], refs[6:8]
    fold2, fold1, fold0, result, sems = refs[8:]
    gx_me, gy_me, core = where_am_i()
    unpack(got, got_z, 0, b2, nx, ny)
    step2 = min(S22, n2)
    from_zero(v2, b2, coef2, inv2, 1, n2 + 1, step2)
    first = first_is_red((step2, y2, Z2))

    def body(k):
        here = pl.ds(k, step2)
        res = b2[0][here] - (diag2[here] * v2[0][here] - gathered(v2, 0, *coef2, k, step2, first))
        start = pl.multiple_of((k - 1) * y2, step2 * y2)
        fold2[pl.ds(start, step2 * y2), :] = res.reshape(step2 * y2, Z2)

    loop(1, n2 + 1, step2, body)
    restrict(fold2, fold1, b3, n3, y3)
    from_zero(v3, b3, coef3, inv3, 1, n3 + 1, n3)

    def sweep(i):
        half_sweep(v3, b3, 0, coef3, inv3, 1, n3 + 1, n3)
        half_sweep(v3, b3, 1, coef3, inv3, 1, n3 + 1, n3)

    loop(0, COARSE_SWEEPS - 1, 1, sweep)
    near2 = min(8, n2)
    base = jnp.clip(2 * gx_me - 2, 0, n2 - near2)
    first3 = first_is_red((y3, Z2))
    for p in range(near2 // 2):
        a, c = v3[0][base // 2 + p + 1], v3[1][base // 2 + p + 1]
        fold2[2 * p * y3 : (2 * p + 1) * y3, :] = jnp.where(first3, a, c)
        fold2[(2 * p + 1) * y3 : (2 * p + 2) * y3, :] = jnp.where(first3, c, a)
    twice_rows(fold1, dot(fold2[0 : near2 * y3, :], copy_matrix(Z2, Z2)))
    for k in range(0, near2, 4):
        e = fold1[0, k * y2 : (k + 4) * y2, :].reshape(4, y2, Z2)
        here = pl.ds(base + 1 + k, 4)
        v2[1][here] = v2[1][here] + e
    half_sweep(v2, b2, 0, coef2, inv2, base + 1, base + 1 + near2, near2)
    half_sweep(v2, b2, 1, coef2, inv2, base + 1, base + 1 + near2, near2)
    shift = lax.rem(4 - 4 * gy_me + 2 * y2, y2)
    first1 = first_is_red((y2, Z2))
    cells = []
    for j in range(4):
        a, c = v2[0][2 * gx_me + j], v2[1][2 * gx_me + j]
        for cell in (jnp.where(first1, a, c), jnp.where(first1, c, a)):
            cells.append(pltpu.roll(cell, shift, 0)[0:16])
    twice_rows(fold1, dot(jnp.concatenate(cells, axis=0), copy_matrix(Z2, Z1)))
    for k in range(1, K1 - 1):
        e = columns(fold1, 32 * (k - 1), Y1, Z1)
        v1[1][k] = jnp.where(inv1[1][k] > 0.0, v1[1][k] + e, 0.0)
    half_sweep(v1, b1, 0, coef1, inv1, 1, K1 - 1, S1)
    half_sweep(v1, b1, 1, coef1, inv1, 1, K1 - 1, S1)
    first0 = first_is_red((Y1, Z1))
    cells = []
    for k in range(H - 1, K1 - H + 1):
        a, c = v1[0][k], v1[1][k]
        cells += [jnp.where(first0, a, c), jnp.where(first0, c, a)]
    cells = [cell[4:20] for cell in cells[1:-1]]
    twice_rows(fold0, dot(jnp.concatenate(cells, axis=0), copy_matrix(Z1, Z0, core * 64)))

    def body(p):
        e = columns(fold0, pl.multiple_of(p * 32, 32), 32, Z0)[None]
        here = pl.ds(p + H - 1, 1)
        v0[1][here] = jnp.where(inv0[1][here] > 0.0, v0[1][here] + e, 0.0)

    loop(0, BX // 2 + 2, 1, body)
    half_sweep(v0, b0, 0, coef0, inv0, H - 1, K0 - H + 1, SHB)
    lanes = pl.ds(pl.multiple_of(core * 128, 128), BZ)
    half_first = first_is_red((BY, BZ))

    copies = []
    for i, start in enumerate(range(0, BX // 2, SH)):
        half_sweep(v0, b0, 1, coef0, inv0, H + start, H + start + SH, SH)
        for p in range(start, start + SH):
            a, c = v0[0][p + H, 8:24, lanes], v0[1][p + H, 8:24, lanes]
            result[2 * p] = jnp.where(half_first, a, c)
            result[2 * p + 1] = jnp.where(half_first, c, a)
        part = pl.ds(2 * start, 2 * SH)
        copies.append(pltpu.make_async_copy(result.at[part], out.at[part], sems.at[i]))
        copies[-1].start()
    for copy in copies:
        copy.wait()


def shape(*dims):
    return jax.ShapeDtypeStruct(dims, F32)


def scratch(*dims):
    return pltpu.VMEM(dims, F32)


def ring(x, axis, step):
    n = lax.axis_size(axis)
    return lax.ppermute(x, axis, [(i, (i + step) % n) for i in range(n)])


def swap(x):
    return lax.ppermute(x, "gz", [(0, 1), (1, 0)])


def gather(send, nx, ny):
    got = lax.all_to_all(send, "gy", 0, 0, tiled=True)
    (send,) = call(spread_kernel, "spread", 4, [(nx,) + got.shape], [], got)
    return lax.all_to_all(send, "gx", 0, 0, tiled=True).reshape((nx * ny,) + got.shape[1:])


def call(kernel, name, mib, outs, scratches, *args, hbm_in=0, hbm_out=0):
    return pl.pallas_call(
        kernel,
        out_shape=tuple(shape(*o) for o in outs),
        in_specs=[HBM] * hbm_in + [VMEM] * (len(args) - hbm_in),
        out_specs=(HBM,) * hbm_out + (VMEM,) * (len(outs) - hbm_out),
        scratch_shapes=[scratch(*s) if isinstance(s, tuple) else s for s in scratches],
        compiler_params=params(mib),
        name=name,
    )(*args)


def on_device(membrane, recovery, extracellular, fiber_scale, labels):
    nx, ny = lax.axis_size("gx"), lax.axis_size("gy")
    block = (BX, BY, BZ)
    held = [
        pltpu.with_memory_space_constraint(x, pltpu.HBM)
        for x in (membrane, recovery, extracellular, fiber_scale, labels)
    ]
    own, xup, xdn, yup, ydn = call(
        prep_kernel, "prep", 6,
        [(AT_MEAN + 2, BY, BZ)] + [(18, BY, BZ)] * 4,
        [block] * 4
        + [pltpu.VMEM(labels.shape, jnp.int32), (1, 128, 128), pltpu.SemaphoreType.DMA((5,))],
        *held, hbm_in=5,
    )
    xlo, xhi = ring(xup, "gx", 1), ring(xdn, "gx", -1)
    ylo, yhi = ring(yup, "gy", 1), ring(ydn, "gy", -1)
    cup, cdn = call(corner_kernel, "corner", 4, [(16, 8, BZ)] * 2, [], xlo, xhi)
    clo, chi = lax.optimization_barrier((ring(cup, "gy", 1), ring(cdn, "gy", -1)))
    halos = []
    for piece in (own, xlo, xhi, ylo, yhi, clo, chi):
        halos += [piece, swap(piece)]
    (seed,) = call(seed_kernel, "seed", 4, [(8, Z2)], [(1, 32, 128)], own)
    fine = (K0, Y0, Z0)
    mid = (K1, Y1, Z1)
    grid2, grid3 = (2 * nx + 2, 4 * ny, Z2), (nx + 2, 2 * ny, Z2)
    mnext, rhs1, rup, rdn, in1r, in1b, *level0 = call(
        fine_kernel, "fine", 20,
        [block, (2, 4, 8, Z1), (2, 2, 8, Z1), (2, 2, 8, Z1)] + [mid] * 2 + [fine] * 13,
        [fine] * 16
        + [(8, BY, Z0), (2, 128, 128), block, pltpu.SemaphoreType.DMA((1,))],
        *halos, hbm_out=1,
    )
    rnext, *coef1 = call(
        middle_faces_kernel, "middle_faces", 4, [block] + [mid] * 10,
        [mid] * 2 + [block] * 2 + [pltpu.SemaphoreType.DMA((2,))],
        held[0], held[1], in1r, in1b, hbm_in=2, hbm_out=1,
    )
    part = (2, 2, 16, Z1)
    wide, xup, xdn = call(
        join_kernel, "join", 4, [(2, 4, 16, Z1), part, part], [],
        ring(rup, "gy", 1), rhs1, ring(rdn, "gy", -1),
    )
    low, high = ring(xup, "gx", 1), ring(xdn, "gx", -1)
    v1r, v1b, b1r, b1b, send = call(
        middle_kernel, "middle", 4,
        [mid] * 4 + [(ny, 16, Z2)],
        [(32, Z1), (1, 32, 128)],
        low, wide, high, seed, *coef1,
    )
    got = gather(send, nx, ny)
    got_z = swap(got)
    coarse = call(
        lambda *refs: coarse_kernel(*refs, nx=nx, ny=ny), "coarse", 8,
        [grid2] * 10 + [grid3] * 9,
        [grid2] * 4 + [grid3] * 4 + [(8 * nx * ny, Z2), (1, 4 * nx * ny, Z2)],
        got, got_z,
    )
    level1 = [v1r, v1b, b1r, b1b, *coef1[:7], *coef1[8:]]
    (enext,) = call(
        lambda *refs: up_kernel(*refs, nx=nx, ny=ny), "up", 10,
        [block],
        [grid2] * 4 + [grid3] * 4
        + [(8 * nx * ny, Z2), (2, max(4 * nx * ny, 256), Z2), (3, 320, 128)]
        + [block, pltpu.SemaphoreType.DMA((2,))],
        got, got_z, *level1, *level0, *coarse, hbm_out=1,
    )
    return mnext, rnext, enext


def solution(mesh):
    spec = P("gx", "gy", "gz")
    return jax.shard_map(
        on_device, mesh=mesh, in_specs=(spec,) * 5, out_specs=(spec,) * 3, check_vma=False
    )
```
